32 devices in a mesh: prob: 2 (over x), row: 4 (over z), col: 4 (over y, core).
Axes of the slice: x: 2, y: 2, z: 4, core: 2. Of those that a mesh axis runs over, the one named last changes fastest.
Arguments:
- kernel: bfloat16 [9216, 9216], P('row', 'col')
- cost_mat: bfloat16 [9216, 9216], P('row', 'col')
- src_mass: float32 [9216, 128], P('row', 'prob'), parts along dimension 1
- tgt_mass: float32 [9216, 128], P('col', 'prob'), parts along dimension 1
Outputs:
- output 1: float32 [9216, 128], P('row', 'prob'), parts along dimension 1
- output 2: float32 [9216, 128], P('col', 'prob'), parts along dimension 1
- output 3: float32 [128], P('prob'), parts along dimension 0
There are 2 independent parts. The reference program is written for one: setup_inputs(seed, part) draws one part's arguments, and reference() takes and returns one part's arrays. A program takes and returns all parts, laid end to end along the dimension named above; an argument that names none is the same for every part.
All inputs are finite; a program needn't handle non-finite values.
Results may differ from the reference program's by a relative error of at most 0.001.
Values are sent between devices in bfloat16 or wider.
A program may use at most 1 GiB of HBM per device.

```python
import jax
import jax.numpy as jnp
from jax import lax

N_SRC = 9216
N_TGT = 9216
BATCH = 64
SWEEPS = 6
EPSILON = 0.1


def setup_inputs(seed: int = 0, part: int = 0) -> dict:
    base_key = jax.random.key(seed)
    key_src, key_tgt = jax.random.split(base_key, 2)
    src_pts = jax.random.uniform(key_src, (N_SRC, 3), jnp.float32)
    tgt_pts = jax.random.uniform(key_tgt, (N_TGT, 3), jnp.float32)
    cross_dot = jnp.dot(src_pts, tgt_pts.T)
    dist_sq = jnp.sum(src_pts * src_pts, axis=1)[:, None] + jnp.sum(tgt_pts * tgt_pts, axis=1)[None, :] - 2.0 * cross_dot
    cost_full = jnp.clip(dist_sq / 3.0, 0.0, 1.0)
    part_key = jax.random.fold_in(jax.random.key(seed + 1), part)
    key_a, key_b = jax.random.split(part_key, 2)
    src_mass = N_TGT * jax.random.uniform(key_a, (N_SRC, BATCH), jnp.float32, 0.25, 1.75)
    tgt_mass = N_SRC * jax.random.uniform(key_b, (N_TGT, BATCH), jnp.float32, 0.25, 1.75)
    return {"kernel": jnp.exp(-cost_full / EPSILON).astype(jnp.bfloat16), "cost_mat": cost_full.astype(jnp.bfloat16), "src_mass": src_mass, "tgt_mass": tgt_mass}


def reference(kernel, cost_mat, src_mass, tgt_mass):
    def sweep(carry, unused):
        tgt_scale = carry[1]
        row_sum = jnp.dot(kernel, tgt_scale.astype(jnp.bfloat16), preferred_element_type=jnp.float32)
        src_scale = src_mass / row_sum
        col_sum = lax.dot_general(kernel, src_scale.astype(jnp.bfloat16), (((0,), (0,)), ((), ())), preferred_element_type=jnp.float32)
        return (src_scale, tgt_mass / col_sum), None
    start = (jnp.zeros((N_SRC, BATCH), jnp.float32), jnp.ones((N_TGT, BATCH), jnp.float32))
    final, unused_hist = lax.scan(sweep, start, None, length=SWEEPS)
    src_scale, tgt_scale = final
    kern_cost = kernel * cost_mat
    weighted = jnp.dot(kern_cost, tgt_scale.astype(jnp.bfloat16), preferred_element_type=jnp.float32)
    transport = jnp.sum(src_scale * weighted, axis=0) / (N_SRC * N_TGT)
    return (src_scale, tgt_scale, transport)
```

```python
import functools

import jax
import jax.numpy as jnp
from jax import lax
from jax.experimental import pallas as pl
from jax.experimental.pallas import tpu as pltpu
from jax.sharding import PartitionSpec as P

SWEEPS = 6
MESH = pl.DeviceIdType.MESH
F32 = jnp.float32
BF16 = jnp.bfloat16
NB = 2
NT = 3


def dot_nn(x, y):
    return jnp.dot(x, y, preferred_element_type=F32)


def dot_nt(x, y):
    return lax.dot_general(x, y, (((1,), (1,)), ((), ())), preferred_element_type=F32)


def tiles(size, tile=256):
    return [(o, min(tile, size - o)) for o in range(0, size, tile)]


def kernel(n_row, n_col, norm,
           k_hbm, c_hbm, a_hbm, b_hbm, u_hbm, v_hbm, cost_ref,
           K, C, A, B, UB, VB, UF, VF, DS, DR, SP, YR, TP, EI, XR, R0, ACC, CPS, CPR,
           k_sem, in_sem, out_sem, r0_sem,
           d_sem, y_sem, u_sem, uf_sem, e_sem, x_sem, v_sem, vf_sem, cp_sem):
    row = lax.axis_index("row")
    col = lax.axis_index("col")
    core = lax.rem(col, 2)
    n = K.shape[0]
    half = n // 2
    m = UB.shape[1]
    width = n // NT
    sib = {"col": col + 1 - 2 * core}
    ypeer = {"col": lax.rem(col + 2, n_col)}
    inner = jnp.logical_or(row == 1, row == 2)
    edge = jnp.logical_not(inner)
    zpair = {"row": row + 1 - 2 * lax.rem(row, 2)}
    zmid = {"row": n_row - 1 - row}
    own0 = pl.multiple_of(core * half, 128)
    sib0 = pl.multiple_of((1 - core) * half, 128)
    subs = [(0, 512), (512, half - 512)]

    def rcopy(src, dst, sem, dev):
        return pltpu.make_async_remote_copy(src_ref=src, dst_ref=dst, send_sem=sem.at[0], recv_sem=sem.at[1],
                                            device_id=dev, device_id_type=MESH)

    rows_per = 384
    k_loads = []
    for h0 in (sib0, own0):
        for j in range(half // rows_per):
            sl = pl.ds(pl.multiple_of(h0 + j * rows_per, 128), rows_per)
            cp = pltpu.make_async_copy(k_hbm.at[sl, :], K.at[sl, :], k_sem.at[len(k_loads)])
            cp.start()
            k_loads.append((sl, cp))
    a_load = pltpu.make_async_copy(a_hbm, A, in_sem.at[0])
    b_load = pltpu.make_async_copy(b_hbm, B, in_sem.at[1])
    c_load = pltpu.make_async_copy(c_hbm, C, in_sem.at[2])
    a_load.start()
    b_load.start()
    c_load.start()

    barrier = pltpu.get_barrier_semaphore()
    rel = [(dr, dc) for dr in range(n_row) for dc in range(n_col) if (dr, dc) != (0, 0)]
    peers = [{"row": lax.rem(row + dr, n_row), "col": lax.rem(col + dc, n_col)} for dr, dc in rel]
    for dev in peers:
        pl.semaphore_signal(barrier, inc=1, device_id=dev, device_id_type=MESH)

    ACC[...] = jnp.zeros_like(ACC)

    ones = jnp.ones((16, n), BF16)
    per_half = half // rows_per
    for h in range(2):
        for j in range(per_half):
            sl, cp = k_loads[h * per_half + j]
            cp.wait()
            R0[h, :, j * rows_per:(j + 1) * rows_per] = dot_nt(ones, K[sl, :])[:8]
        if h == 0:
            pl.semaphore_wait(barrier, len(peers))
            r0d = rcopy(R0.at[0], R0.at[2], r0_sem.at[0], sib)
            r0d.start()
    r0d.wait()
    R0[1] = R0[1] + R0[2]
    r0y = rcopy(R0.at[1], R0.at[3], r0_sem.at[1], ypeer)
    r0y.start()
    a_load.wait()
    r0y.wait()
    s0 = R0[1, 0:1] + R0[3, 0:1]

    def u_copy(b, j):
        o, w = subs[j]
        ref = UB.at[b, :, pl.ds(pl.multiple_of(own0 + o, 128), w)]
        return rcopy(ref, ref, u_sem.at[b, j], sib)

    def uf_copy(b):
        ref = UF.at[b, :, pl.ds(own0, half)]
        return rcopy(ref, ref, uf_sem.at[b], sib)

    for b in range(NB):
        for j, (o, w) in enumerate(subs):
            sl = pl.ds(pl.multiple_of(own0 + o, 128), w)
            UB[b, :, sl] = (A[pl.ds(b * m, m), sl] / s0[:, o:o + w]).astype(BF16)
            u_copy(b, j).start()
    b_load.wait()

    def when(cond, fn):
        pl.when(cond)(fn)

    def s_steps(b, sweep):
        par = lax.rem(sweep, 2)
        last = sweep == SWEEPS - 1

        def d_copy():
            return rcopy(DS.at[b], DR.at[b], d_sem.at[b], sib)

        def y_copy(j):
            o, w = subs[j]
            return rcopy(SP.at[b, :, pl.ds(o, w)], YR.at[par, b, :, pl.ds(o, w)], y_sem.at[par, b, j], ypeer)

        def s1():
            for o, w in tiles(half):
                DS[b, :, o:o + w] = dot_nt(VB[b], K[pl.ds(pl.multiple_of(sib0 + o, 128), w), :])
            d_copy().start()

        def s2():
            for o, w in tiles(half):
                SP[b, :, o:o + w] = dot_nt(VB[b], K[pl.ds(pl.multiple_of(own0 + o, 128), w), :])

        def s3():
            d_copy().wait_recv()
            for j, (o, w) in enumerate(subs):
                SP[b, :, o:o + w] = SP[b, :, o:o + w] + DR[b, :, o:o + w]
                y_copy(j).start()

        def s4(j):
            def run():
                o, w = subs[j]
                y_copy(j).wait_recv()
                sl = pl.ds(pl.multiple_of(own0 + o, 128), w)
                u = A[pl.ds(b * m, m), sl] / (SP[b, :, o:o + w] + YR[par, b, :, o:o + w])
                UB[b, :, sl] = u.astype(BF16)
                u_copy(b, j).start()
                UF[b, :, sl] = u
                if j == len(subs) - 1:
                    when(last, lambda: uf_copy(b).start())
                    d_copy().wait_send()
                y_copy(j).wait_send()
            return run

        return {"s1": s1, "s2": s2, "s3": s3, "s40": s4(0), "s41": s4(1)}

    def t_steps(b, sweep, last):
        par = lax.rem(sweep, 2)

        def piece(c):
            return pl.ds(c * width, width)

        def e_copy(c):
            return rcopy(TP.at[b, :, piece(c)], EI.at[b, :, piece(c)], e_sem.at[b, c], zpair)

        def x_copy(c):
            return rcopy(TP.at[b, :, piece(c)], XR.at[par, b, :, piece(c)], x_sem.at[par, b, c], zmid)

        def v_copy(c):
            ref = VB.at[b, :, piece(c)]
            return rcopy(ref, ref, v_sem.at[b, c], zpair)

        def vf_copy(c):
            ref = VF.at[b, :, piece(c)]
            return rcopy(ref, ref, vf_sem.at[b, c], zpair)

        def t0():
            for j in range(len(subs)):
                u_copy(b, j).wait()

        def t1(c):
            def run():
                for o, w in tiles(width):
                    o += c * width
                    TP[b, :, o:o + w] = dot_nn(UB[b], K[:, o:o + w])
                when(edge, lambda: e_copy(c).start())
            return run

        def t2(c):
            def at_inner():
                e_copy(c).wait_recv()
                TP[b, :, piece(c)] = TP[b, :, piece(c)] + EI[b, :, piece(c)]
                x_copy(c).start()
            return lambda: when(inner, at_inner)

        def t3(c):
            def at_inner():
                x_copy(c).wait_recv()
                v = B[pl.ds(b * m, m), piece(c)] / (TP[b, :, piece(c)] + XR[par, b, :, piece(c)])
                VB[b, :, piece(c)] = v.astype(BF16)
                v_copy(c).start()
                VF[b, :, piece(c)] = v
                when(last, lambda: vf_copy(c).start())
                x_copy(c).wait_send()
                v_copy(c).wait_send()

            def at_edge():
                v_copy(c).wait_recv()
                e_copy(c).wait_send()

            def run():
                when(inner, at_inner)
                when(edge, at_edge)
            return run

        def fin():
            for c in range(NT):
                when(inner, lambda: vf_copy(c).wait_send())
                when(edge, lambda: vf_copy(c).wait_recv())

        steps = {"t0": t0, "fin": fin}
        for c in range(NT):
            steps["t1%d" % c] = t1(c)
            steps["t2%d" % c] = t2(c)
            steps["t3%d" % c] = t3(c)
        return steps

    def kc_rows(i, rows):
        sl = pl.ds(pl.multiple_of(i * rows, rows), rows)
        C[sl, :] = K[sl, :] * C[sl, :]

    def cost_step(b):
        acc = jnp.zeros((m, 128), F32)
        for o, w in tiles(n):
            p = UF[b, :, o:o + w] * dot_nt(VB[b], C[o:o + w, :])
            for q in range(0, w, 128):
                acc = acc + p[:, q:q + 128]
        ACC[b * m:(b + 1) * m, :] = acc

    def run(steps, *names):
        for group in names:
            for name in group.split():
                steps[name]()

    def named(prefix, *dicts):
        return {prefix + k: f for d in dicts for k, f in d.items()}

    no = jnp.bool_(False)
    yes = jnp.bool_(True)
    st = {**named("A", t_steps(0, 0, no)), **named("B", t_steps(1, 0, no))}
    run(st, "At0 At10 At11 At12")
    c_load.wait()
    run(st, "At20 At21 At22", "At30", "Bt0 Bt10 Bt11 Bt12", "At31 At32")

    def body(s, carry):
        last = s + 1 == SWEEPS - 1
        st = {**named("A", s_steps(0, s + 1), t_steps(0, s + 1, last)), **named("B", s_steps(1, s + 1))}
        old = named("b", t_steps(1, s, no))
        new = named("B", t_steps(1, s + 1, no))
        st = {**new, **st, **old, "kc": lambda: kc_rows(s, 384)}
        run(st, "As1 As2 bt20 As3", "kc bt21 bt22", "As40 bt30 As41 bt31", "At0 At10 At11 At12", "bt32",
            "Bs1 Bs2 At20 Bs3", "At21 At22", "Bs40 At30 Bs41 At31", "Bt0 Bt10 Bt11 Bt12", "At32")
        return carry

    lax.fori_loop(0, SWEEPS - 1, body, 0)

    kc_rows(SWEEPS - 1, 384)
    stb = named("B", t_steps(1, SWEEPS - 1, yes))
    sta = named("A", t_steps(0, SWEEPS - 1, yes))
    uf_copy(0).wait()
    run(stb, "Bt20 Bt21 Bt22")
    cost_step(0)
    run(stb, "Bt30 Bt31 Bt32")
    uf_copy(1).wait()
    u_out = [pltpu.make_async_copy(UF.at[b], u_hbm.at[pl.ds(b * m, m), :], out_sem.at[b]) for b in range(NB)]
    for cp in u_out:
        cp.start()
    cost_step(1)
    tot = jnp.sum(jnp.transpose(ACC[...]), axis=0, keepdims=True)
    CPS[...] = jnp.broadcast_to(tot, CPS.shape)
    me = row * n_col + col
    cps = [rcopy(CPS, CPR.at[me], cp_sem.at[i], dev) for i, dev in enumerate(peers)]
    for cp in cps:
        cp.start()
    CPR[me] = CPS[...]
    run(sta, "Afin")
    run(stb, "Bfin")
    v_out = [pltpu.make_async_copy(VF.at[b], v_hbm.at[pl.ds(b * m, m), :], out_sem.at[NB + b]) for b in range(NB)]
    for cp in v_out:
        cp.start()
    for cp in cps:
        cp.wait()
    total = CPR[0]
    for i in range(1, n_row * n_col):
        total = total + CPR[i]
    cost_ref[...] = total[0:1, 0:cost_ref.shape[1]] / norm
    for cp in u_out + v_out:
        cp.wait()


def solution(mesh):
    n_row = mesh.shape["row"]
    n_col = mesh.shape["col"]

    def local_fn(kern, cost_mat, src_mass, tgt_mass):
        n = kern.shape[0]
        q = src_mass.shape[1]
        m = q // NB
        half = n // 2
        norm = float(n * n_row) * float(kern.shape[1] * n_col)
        dma = pltpu.SemaphoreType.DMA
        any_spec = pl.BlockSpec(memory_space=pl.ANY)
        u, v, cost = pl.pallas_call(
            functools.partial(kernel, n_row, n_col, norm),
            out_shape=(jax.ShapeDtypeStruct((q, n), F32), jax.ShapeDtypeStruct((q, n), F32),
                       jax.ShapeDtypeStruct((1, q), F32)),
            in_specs=[any_spec] * 4,
            out_specs=(any_spec, any_spec, pl.BlockSpec(memory_space=pltpu.VMEM)),
            scratch_shapes=[
                pltpu.VMEM((n, n), BF16), pltpu.VMEM((n, n), BF16),
                pltpu.VMEM((q, n), F32), pltpu.VMEM((q, n), F32),
                pltpu.VMEM((NB, m, n), BF16), pltpu.VMEM((NB, m, n), BF16),
                pltpu.VMEM((NB, m, n), F32), pltpu.VMEM((NB, m, n), F32),
                pltpu.VMEM((NB, m, half), F32), pltpu.VMEM((NB, m, half), F32),
                pltpu.VMEM((NB, m, half), F32), pltpu.VMEM((2, NB, m, half), F32),
                pltpu.VMEM((NB, m, n), F32), pltpu.VMEM((NB, m, n), F32),
                pltpu.VMEM((2, NB, m, n), F32),
                pltpu.VMEM((4, 8, half), F32),
                pltpu.VMEM((128, 128), F32), pltpu.VMEM((8, 128), F32), pltpu.VMEM((n_row * n_col, 8, 128), F32),
                dma((6,)), dma((3,)), dma((2 * NB,)), dma((2, 2)),
                dma((NB, 2)), dma((2, NB, 2, 2)), dma((NB, 2, 2)), dma((NB, 2)),
                dma((NB, NT, 2)), dma((2, NB, NT, 2)), dma((NB, NT, 2)), dma((NB, NT, 2)),
                dma((n_row * n_col - 1, 2)),
            ],
            compiler_params=pltpu.CompilerParams(collective_id=0, has_side_effects=True, vmem_limit_bytes=60 * 1024 * 1024),
        )(kern, cost_mat, src_mass.T, tgt_mass.T)
        return u.T, v.T, cost.reshape(q)

    return jax.shard_map(local_fn, mesh=mesh, in_specs=(P("row", "col"), P("row", "col"), P("row", "prob"), P("col", "prob")),
                         out_specs=(P("row", "prob"), P("col", "prob"), P("prob")), check_vma=False)
```

```python
import functools

import jax
import jax.numpy as jnp
from jax import lax
from jax.experimental import pallas as pl
from jax.experimental.pallas import tpu as pltpu
from jax.sharding import PartitionSpec as P

SWEEPS = 6
MESH = pl.DeviceIdType.MESH
F32 = jnp.float32
BF16 = jnp.bfloat16
NB = 4
T_PIECES = (768, 768, 768)
S_PIECES = (512, 640)


def dot_nn(x, y):
    return jnp.dot(x, y, preferred_element_type=F32)


def spans(sizes):
    out, o = [], 0
    for w in sizes:
        out.append((o, w))
        o += w
    return out


def tiles(size, tile=256):
    return [(o, min(tile, size - o)) for o in range(0, size, tile)]


def kernel(n_row, n_col, norm,
           k_hbm, c_hbm, a_hbm, b_hbm, u_hbm, v_hbm, cost_ref,
           K, KT, C, KCT, A, B, UB, VB, UF, VF, DS, DR, SP, YR, TP, EI, XR, R0, ACC, CPS, CPR,
           k_sem, in_sem, out_sem, r0_sem,
           d_sem, y_sem, u_sem, uf_sem, e_sem, x_sem, v_sem, vf_sem, cp_sem):
    row = lax.axis_index("row")
    col = lax.axis_index("col")
    core = lax.rem(col, 2)
    n = K.shape[0]
    half = n // 2
    m = UB.shape[1]
    total_inst = SWEEPS * NB
    sib = {"col": col + 1 - 2 * core}
    ypeer = {"col": lax.rem(col + 2, n_col)}
    inner = jnp.logical_or(row == 1, row == 2)
    edge = jnp.logical_not(inner)
    zpair = {"row": row + 1 - 2 * lax.rem(row, 2)}
    zmid = {"row": n_row - 1 - row}
    own0 = pl.multiple_of(core * half, 128)
    sib0 = pl.multiple_of((1 - core) * half, 128)
    t_pieces = spans(T_PIECES)
    s_pieces = spans(S_PIECES)

    def at(o, w):
        return pl.ds(pl.multiple_of(o, 128), w)

    def rcopy(src, dst, sem, dev):
        return pltpu.make_async_remote_copy(src_ref=src, dst_ref=dst, send_sem=sem.at[0], recv_sem=sem.at[1],
                                            device_id=dev, device_id_type=MESH)

    rows_per = 384
    per_half = half // rows_per
    k_loads = []
    for h0 in (sib0, own0):
        for j in range(per_half):
            sl = at(h0 + j * rows_per, rows_per)
            cp = pltpu.make_async_copy(k_hbm.at[sl, :], K.at[sl, :], k_sem.at[len(k_loads)])
            cp.start()
            k_loads.append((sl, cp))
    a_load = pltpu.make_async_copy(a_hbm, A, in_sem.at[0])
    b_load = pltpu.make_async_copy(b_hbm, B, in_sem.at[1])
    c_load = pltpu.make_async_copy(c_hbm, C, in_sem.at[2])
    a_load.start()
    b_load.start()
    c_load.start()

    barrier = pltpu.get_barrier_semaphore()
    rel = [(dr, dc) for dr in range(n_row) for dc in range(n_col) if (dr, dc) != (0, 0)]
    peers = [{"row": lax.rem(row + dr, n_row), "col": lax.rem(col + dc, n_col)} for dr, dc in rel]
    for dev in peers:
        pl.semaphore_signal(barrier, inc=1, device_id=dev, device_id_type=MESH)

    ACC[...] = jnp.zeros_like(ACC)

    ones = jnp.ones((16, n), BF16)
    for h in range(2):
        for j in range(per_half):
            sl, cp = k_loads[h * per_half + j]
            cp.wait()

            def turn(t, carry, sl=sl):
                cols = at(t * 256, 256)
                KT[cols, sl] = jnp.transpose(K[sl, cols])
                return carry

            lax.fori_loop(0, n // 256, turn, 0)
            R0[h, :, j * rows_per:(j + 1) * rows_per] = dot_nn(ones, KT[:, sl])[:8]
        if h == 0:
            pl.semaphore_wait(barrier, len(peers))
            r0d = rcopy(R0.at[0], R0.at[2], r0_sem.at[0], sib)
            r0d.start()
    r0d.wait()
    R0[1] = R0[1] + R0[2]
    r0y = rcopy(R0.at[1], R0.at[3], r0_sem.at[1], ypeer)
    r0y.start()
    a_load.wait()
    r0y.wait()
    s0 = R0[1, 0:1] + R0[3, 0:1]

    def u_copy(b, j):
        o, w = s_pieces[j]
        ref = UB.at[b, :, at(own0 + o, w)]
        return rcopy(ref, ref, u_sem.at[b, j], sib)

    def uf_copy(b):
        ref = UF.at[b, :, at(own0, half)]
        return rcopy(ref, ref, uf_sem.at[b], sib)

    for b in range(NB):
        for j, (o, w) in enumerate(s_pieces):
            sl = at(own0 + o, w)
            UB[b, :, sl] = (A[b, :, sl] / s0[:, o:o + w]).astype(BF16)
            u_copy(b, j).start()
    b_load.wait()
    c_load.wait()

    def d_copy(b):
        return rcopy(DS.at[b], DR.at[b], d_sem.at[b], sib)

    def y_copy(par, b, j):
        o, w = s_pieces[j]
        return rcopy(SP.at[b, :, pl.ds(o, w)], YR.at[par, b, :, pl.ds(o, w)], y_sem.at[par, b, j], ypeer)

    def e_copy(b, c):
        o, w = t_pieces[c]
        return rcopy(TP.at[b, :, pl.ds(o, w)], EI.at[b, :, pl.ds(o, w)], e_sem.at[b, c], zpair)

    def x_copy(par, b, c):
        o, w = t_pieces[c]
        return rcopy(TP.at[b, :, pl.ds(o, w)], XR.at[par, b, :, pl.ds(o, w)], x_sem.at[par, b, c], zmid)

    def v_copy(b, c):
        o, w = t_pieces[c]
        ref = VB.at[b, :, pl.ds(o, w)]
        return rcopy(ref, ref, v_sem.at[b, c], zpair)

    def vf_copy(b, c):
        o, w = t_pieces[c]
        ref = VF.at[b, :, pl.ds(o, w)]
        return rcopy(ref, ref, vf_sem.at[b, c], zpair)

    def s1(b, par, last):
        for o, w in tiles(half):
            DS[b, :, o:o + w] = dot_nn(VB[b], KT[:, at(sib0 + o, w)])
        d_copy(b).start()

    def s2(b, par, last):
        for o, w in tiles(half):
            SP[b, :, o:o + w] = dot_nn(VB[b], KT[:, at(own0 + o, w)])

    def v_drain(b):
        @pl.when(inner)
        def _():
            for c in range(len(t_pieces)):
                v_copy(b, c).wait_send()

    def s3(b, par, last):
        d_copy(b).wait_recv()
        for j, (o, w) in enumerate(s_pieces):
            SP[b, :, o:o + w] = SP[b, :, o:o + w] + DR[b, :, o:o + w]
            y_copy(par, b, j).start()
        v_drain(b)

    def s4(j, b, par, last):
        o, w = s_pieces[j]
        y_copy(par, b, j).wait_recv()
        sl = at(own0 + o, w)
        u = A[b, :, sl] / (SP[b, :, o:o + w] + YR[par, b, :, o:o + w])
        UB[b, :, sl] = u.astype(BF16)
        u_copy(b, j).start()
        UF[b, :, sl] = u
        if j == len(s_pieces) - 1:
            pl.when(last)(lambda: uf_copy(b).start())
            d_copy(b).wait_send()
        y_copy(par, b, j).wait_send()

    def t0(b, par, last):
        for j in range(len(s_pieces)):
            u_copy(b, j).wait()

    def t1(c, b, par, last):
        o0, width = t_pieces[c]
        for o, w in tiles(width):
            TP[b, :, o0 + o:o0 + o + w] = dot_nn(UB[b], K[:, o0 + o:o0 + o + w])
        pl.when(edge)(lambda: e_copy(b, c).start())

    def t2(c, b, par, last):
        o, w = t_pieces[c]

        @pl.when(inner)
        def _():
            e_copy(b, c).wait_recv()
            TP[b, :, o:o + w] = TP[b, :, o:o + w] + EI[b, :, o:o + w]
            x_copy(par, b, c).start()

    def t3i(c, b, par, last):
        o, w = t_pieces[c]

        @pl.when(inner)
        def _():
            x_copy(par, b, c).wait_recv()
            v = B[b, :, o:o + w] / (TP[b, :, o:o + w] + XR[par, b, :, o:o + w])
            VB[b, :, o:o + w] = v.astype(BF16)
            v_copy(b, c).start()
            VF[b, :, o:o + w] = v
            pl.when(last)(lambda: vf_copy(b, c).start())
            x_copy(par, b, c).wait_send()

    def t3e(c, b, par, last):
        @pl.when(edge)
        def _():
            v_copy(b, c).wait_recv()
            e_copy(b, c).wait_send()

    def out_copies(b):
        return (pltpu.make_async_copy(UF.at[b], u_hbm.at[b], out_sem.at[b, 0]),
                pltpu.make_async_copy(VF.at[b], v_hbm.at[b], out_sem.at[b, 1]))

    def cost_part(b):
        v_drain(b)
        uf_copy(b).wait()
        acc = jnp.zeros((m, 128), F32)
        for o, w in tiles(n):
            p = UF[b, :, o:o + w] * dot_nn(VB[b], KCT[:, o:o + w])
            for q in range(0, w, 128):
                acc = acc + p[:, q:q + 128]
        ACC[pl.ds(pl.multiple_of(b * m, m), m), :] = acc
        for c in range(len(t_pieces)):
            pl.when(inner)(lambda c=c: vf_copy(b, c).wait_send())
            pl.when(edge)(lambda c=c: vf_copy(b, c).wait_recv())
        for cp in out_copies(b):
            cp.start()

    def kc(t):
        rows = at(t * 128, 128)

        def turn(q, carry):
            cols = at(q * 256, 256)
            KCT[cols, rows] = KT[cols, rows] * jnp.transpose(C[rows, cols])
            return carry

        lax.fori_loop(0, n // 256, turn, 0)

    kc_first = 2

    def tick(i, carry):
        def do(fn, lag, first=0):
            g = i - lag

            @pl.when(jnp.logical_and(g >= first, g < total_inst))
            def _():
                sweep = lax.div(g, NB)
                fn(lax.rem(g, NB), lax.rem(sweep, 2), sweep == SWEEPS - 1)

        part = functools.partial
        do(s1, 0, NB)
        do(s2, 0, NB)
        pl.when(i >= total_inst)(lambda: cost_part(i - total_inst))
        do(part(s4, 0), 1, NB)
        do(part(s4, 1), 1, NB)
        do(part(t3i, 1), 3)
        do(part(t2, 0), 2)
        do(part(t3i, 2), 3)
        do(s3, 0, NB)
        do(part(t2, 1), 2)
        do(t0, 1)
        do(part(t1, 0), 1)
        do(part(t1, 1), 1)
        do(part(t1, 2), 1)
        do(part(t2, 2), 2)
        do(part(t3e, 0), 3)
        do(part(t3e, 1), 3)
        pl.when(jnp.logical_and(i >= kc_first, i < kc_first + n // 128))(lambda: kc(i - kc_first))
        do(part(t3i, 0), 2)
        do(part(t3e, 2), 3)
        return carry

    lax.fori_loop(1, total_inst + NB, tick, 0)

    tot = jnp.sum(jnp.transpose(ACC[...]), axis=0, keepdims=True)
    CPS[...] = jnp.broadcast_to(tot, CPS.shape)
    me = row * n_col + col
    cps = [rcopy(CPS, CPR.at[me], cp_sem.at[i], dev) for i, dev in enumerate(peers)]
    for cp in cps:
        cp.start()
    CPR[me] = CPS[...]
    for cp in cps:
        cp.wait()
    total = CPR[0]
    for i in range(1, n_row * n_col):
        total = total + CPR[i]
    cost_ref[...] = total[0:1, 0:cost_ref.shape[1]] / norm
    for b in range(NB):
        for cp in out_copies(b):
            cp.wait()


def solution(mesh):
    n_row = mesh.shape["row"]
    n_col = mesh.shape["col"]

    def local_fn(kern, cost_mat, src_mass, tgt_mass):
        n = kern.shape[0]
        q = src_mass.shape[1]
        m = q // NB
        half = n // 2
        norm = float(n * n_row) * float(kern.shape[1] * n_col)
        dma = pltpu.SemaphoreType.DMA
        vmem = pltpu.VMEM
        any_spec = pl.BlockSpec(memory_space=pl.ANY)
        np_, ns = len(T_PIECES), len(S_PIECES)
        u, v, cost = pl.pallas_call(
            functools.partial(kernel, n_row, n_col, norm),
            out_shape=(jax.ShapeDtypeStruct((NB, m, n), F32), jax.ShapeDtypeStruct((NB, m, n), F32),
                       jax.ShapeDtypeStruct((1, q), F32)),
            in_specs=[any_spec] * 4,
            out_specs=(any_spec, any_spec, pl.BlockSpec(memory_space=pltpu.VMEM)),
            scratch_shapes=[
                vmem((n, n), BF16), vmem((n, n), BF16), vmem((n, n), BF16), vmem((n, n), BF16),
                vmem((NB, m, n), F32), vmem((NB, m, n), F32),
                vmem((NB, m, n), BF16), vmem((NB, m, n), BF16),
                vmem((NB, m, n), F32), vmem((NB, m, n), F32),
                vmem((NB, m, half), F32), vmem((NB, m, half), F32),
                vmem((NB, m, half), F32), vmem((2, NB, m, half), F32),
                vmem((NB, m, n), F32), vmem((NB, m, n), F32),
                vmem((2, NB, m, n), F32),
                vmem((4, 8, half), F32),
                vmem((128, 128), F32), vmem((8, 128), F32), vmem((n_row * n_col, 8, 128), F32),
                dma((6,)), dma((3,)), dma((NB, 2)), dma((2, 2)),
                dma((NB, 2)), dma((2, NB, ns, 2)), dma((NB, ns, 2)), dma((NB, 2)),
                dma((NB, np_, 2)), dma((2, NB, np_, 2)), dma((NB, np_, 2)), dma((NB, np_, 2)),
                dma((n_row * n_col - 1, 2)),
            ],
            compiler_params=pltpu.CompilerParams(collective_id=0, has_side_effects=True, vmem_limit_bytes=60 * 1024 * 1024),
        )(kern, cost_mat, src_mass.T.reshape(NB, m, n), tgt_mass.T.reshape(NB, m, n))
        return u.reshape(q, n).T, v.reshape(q, n).T, cost.reshape(q)

    return jax.shard_map(local_fn, mesh=mesh, in_specs=(P("row", "col"), P("row", "col"), P("row", "prob"), P("col", "prob")),
                         out_specs=(P("row", "prob"), P("col", "prob"), P("prob")), check_vma=False)
```

```python
import functools

import jax
import jax.numpy as jnp
from jax import lax
from jax.experimental import pallas as pl
from jax.experimental.pallas import tpu as pltpu
from jax.sharding import PartitionSpec as P

SWEEPS = 6
MESH = pl.DeviceIdType.MESH
F32 = jnp.float32
BF16 = jnp.bfloat16
NB = 4
T_PIECES = (512, 512, 512, 512, 256)
EARLY = 3
S_PIECES = (512, 640)
KC_FIRST = 5
ORDER = (
    ("e", 4, 4), ("t2", 4, 3), ("s4", 0, 1), ("t2", 3, 3), ("e", 3, 4), ("s1", None, 0), ("t3", 0, 3),
    ("s2", None, 0), ("s4", 1, 1), ("ta", None, 1), ("s3", 0, 0), ("t3", 1, 3), ("t0", None, 1), ("t1", 0, 1),
    ("t2", 0, 2), ("s3", 1, 0), ("t1", 1, 1), ("t3", 2, 3), ("t1", 2, 1), ("kc", None, 0), ("e", 0, 3),
    ("t2", 1, 2), ("t1", 3, 1), ("t2", 2, 2), ("kt", None, 0), ("t3", 4, 3), ("t3", 3, 3), ("cost", None, 0),
    ("e", 1, 3), ("t1", 4, 1), ("e", 2, 3), ("sa", None, -1),
)


def dot_nn(x, y):
    return jnp.dot(x, y, preferred_element_type=F32)


def dot_nt(x, y):
    return lax.dot_general(x, y, (((1,), (1,)), ((), ())), preferred_element_type=F32)


def spans(sizes):
    out, o = [], 0
    for w in sizes:
        out.append((o, w))
        o += w
    return out


def tiles(size, tile=256):
    return [(o, min(tile, size - o)) for o in range(0, size, tile)]


def kernel(n_row, n_col, norm,
           k_hbm, c_hbm, a_hbm, b_hbm, u_hbm, v_hbm, cost_ref,
           K, KT, C, KCT, A, B, UB, VB, UF, VF, DS, DR, SP, YR, TP, EI, XR, R0, ACC, CPS, CPR,
           k_sem, in_sem, out_sem, r0_sem,
           d_sem, y_sem, u_sem, uf_sem, e_sem, x_sem, v_sem, vf_sem, cp_sem):
    row = lax.axis_index("row")
    col = lax.axis_index("col")
    core = lax.rem(col, 2)
    n = K.shape[0]
    half = n // 2
    m = UB.shape[1]
    total_inst = SWEEPS * NB
    sib = {"col": col + 1 - 2 * core}
    ypeer = {"col": lax.rem(col + 2, n_col)}
    inner = jnp.logical_or(row == 1, row == 2)
    edge = jnp.logical_not(inner)
    zpair = {"row": row + 1 - 2 * lax.rem(row, 2)}
    zmid = {"row": n_row - 1 - row}
    own0 = pl.multiple_of(core * half, 128)
    sib0 = pl.multiple_of((1 - core) * half, 128)
    t_pieces = spans(T_PIECES)
    s_pieces = spans(S_PIECES)

    def at(o, w):
        return pl.ds(pl.multiple_of(o, 128), w)

    def rcopy(src, dst, sem, dev):
        return pltpu.make_async_remote_copy(src_ref=src, dst_ref=dst, send_sem=sem.at[0], recv_sem=sem.at[1],
                                            device_id=dev, device_id_type=MESH)

    rows_per = 384
    per_half = half // rows_per
    a_load = pltpu.make_async_copy(a_hbm, A, in_sem.at[0])
    b_load = pltpu.make_async_copy(b_hbm, B, in_sem.at[1])
    c_load = pltpu.make_async_copy(c_hbm, C, in_sem.at[2])
    k_loads = []
    for h0 in (sib0, own0):
        for j in range(per_half):
            sl = at(h0 + j * rows_per, rows_per)
            cp = pltpu.make_async_copy(k_hbm.at[sl, :], K.at[sl, :], k_sem.at[len(k_loads)])
            cp.start()
            k_loads.append((sl, cp))
    a_load.start()

    barrier = pltpu.get_barrier_semaphore()
    rel = [(dr, dc) for dr in range(n_row) for dc in range(n_col) if (dr, dc) != (0, 0)]
    peers = [{"row": lax.rem(row + dr, n_row), "col": lax.rem(col + dc, n_col)} for dr, dc in rel]
    for dev in peers:
        pl.semaphore_signal(barrier, inc=1, device_id=dev, device_id_type=MESH)

    ACC[...] = jnp.zeros_like(ACC)

    ones = jnp.ones((16, n), BF16)
    for h in range(2):
        for j in range(per_half):
            sl, cp = k_loads[h * per_half + j]
            cp.wait()
            R0[h, :, j * rows_per:(j + 1) * rows_per] = dot_nt(ones, K[sl, :])[:8]
        if h == 0:
            pl.semaphore_wait(barrier, len(peers))
            r0d = rcopy(R0.at[0], R0.at[2], r0_sem.at[0], sib)
            r0d.start()
    b_load.start()
    c_load.start()
    r0d.wait()
    R0[1] = R0[1] + R0[2]
    r0y = rcopy(R0.at[1], R0.at[3], r0_sem.at[1], ypeer)
    r0y.start()
    a_load.wait()
    r0y.wait()
    s0 = R0[1, 0:1] + R0[3, 0:1]

    def u_copy(b, j):
        o, w = s_pieces[j]
        ref = UB.at[b, :, at(own0 + o, w)]
        return rcopy(ref, ref, u_sem.at[b, j], sib)

    def uf_copy(b):
        ref = UF.at[b, :, at(own0, half)]
        return rcopy(ref, ref, uf_sem.at[b], sib)

    for b in range(NB):
        for j, (o, w) in enumerate(s_pieces):
            sl = at(own0 + o, w)
            UB[b, :, sl] = (A[b, :, sl] / s0[:, o:o + w]).astype(BF16)
            u_copy(b, j).start()
    b_load.wait()

    def d_copy(b, j):
        o, w = s_pieces[j]
        return rcopy(DS.at[b, :, pl.ds(o, w)], DR.at[b, :, pl.ds(o, w)], d_sem.at[b, j], sib)

    def y_copy(par, b, j):
        o, w = s_pieces[j]
        return rcopy(SP.at[b, :, pl.ds(o, w)], YR.at[par, b, :, pl.ds(o, w)], y_sem.at[par, b, j], ypeer)

    def e_copy(b, c):
        o, w = t_pieces[c]
        return rcopy(TP.at[b, :, pl.ds(o, w)], EI.at[b, :, pl.ds(o, w)], e_sem.at[b, c], zpair)

    def x_copy(par, b, c):
        o, w = t_pieces[c]
        return rcopy(TP.at[b, :, pl.ds(o, w)], XR.at[par, b, :, pl.ds(o, w)], x_sem.at[par, b, c], zmid)

    def v_copy(b, c):
        o, w = t_pieces[c]
        ref = VB.at[b, :, pl.ds(o, w)]
        return rcopy(ref, ref, v_sem.at[b, c], zpair)

    def vf_copy(b, c):
        o, w = t_pieces[c]
        ref = VF.at[b, :, pl.ds(o, w)]
        return rcopy(ref, ref, vf_sem.at[b, c], zpair)

    early = sum(T_PIECES[:EARLY])

    def sa(b, par, last):
        for dst, h0 in ((DS, sib0), (SP, own0)):
            for o, w in tiles(half):
                dst[b, :, o:o + w] = dot_nn(VB[b, :, :early], KT[:early, at(h0 + o, w)])

    def s1(b, par, last):
        for j, (o0, width) in enumerate(s_pieces):
            for o, w in tiles(width):
                o += o0
                DS[b, :, o:o + w] += dot_nn(VB[b, :, early:], KT[early:, at(sib0 + o, w)])
            d_copy(b, j).start()

    def s2(b, par, last):
        for o, w in tiles(half):
            SP[b, :, o:o + w] += dot_nn(VB[b, :, early:], KT[early:, at(own0 + o, w)])

    def v_drain(b):
        @pl.when(inner)
        def _():
            for c in range(len(t_pieces)):
                v_copy(b, c).wait_send()

    def s3(j, b, par, last):
        o, w = s_pieces[j]
        d_copy(b, j).wait_recv()
        SP[b, :, o:o + w] = SP[b, :, o:o + w] + DR[b, :, o:o + w]
        y_copy(par, b, j).start()
        if j == len(s_pieces) - 1:
            v_drain(b)

    def s4(j, b, par, last):
        o, w = s_pieces[j]
        y_copy(par, b, j).wait_recv()
        sl = at(own0 + o, w)
        u = A[b, :, sl] / (SP[b, :, o:o + w] + YR[par, b, :, o:o + w])
        UB[b, :, sl] = u.astype(BF16)
        u_copy(b, j).start()
        UF[b, :, sl] = u
        if j == len(s_pieces) - 1:
            pl.when(last)(lambda: uf_copy(b).start())
        d_copy(b, j).wait_send()
        y_copy(par, b, j).wait_send()

    def t0(b, par, last):
        for j in range(len(s_pieces)):
            u_copy(b, j).wait()

    def ta(b, par, last):
        for o, w in tiles(n):
            TP[b, :, o:o + w] = dot_nn(UB[b, :, at(own0, half)], K[at(own0, half), o:o + w])

    def t1(c, b, par, last):
        o0, width = t_pieces[c]
        for o, w in tiles(width):
            o += o0
            TP[b, :, o:o + w] += dot_nn(UB[b, :, at(sib0, half)], K[at(sib0, half), o:o + w])
        pl.when(edge)(lambda: e_copy(b, c).start())

    def t2(c, b, par, last):
        o, w = t_pieces[c]

        @pl.when(inner)
        def _():
            e_copy(b, c).wait_recv()
            TP[b, :, o:o + w] = TP[b, :, o:o + w] + EI[b, :, o:o + w]
            x_copy(par, b, c).start()

    def t3i(c, b, par, last):
        o, w = t_pieces[c]

        @pl.when(inner)
        def _():
            x_copy(par, b, c).wait_recv()
            v = B[b, :, o:o + w] / (TP[b, :, o:o + w] + XR[par, b, :, o:o + w])
            VB[b, :, o:o + w] = v.astype(BF16)
            v_copy(b, c).start()
            VF[b, :, o:o + w] = v
            pl.when(last)(lambda: vf_copy(b, c).start())
            x_copy(par, b, c).wait_send()

    def t3e(c, b, par, last):
        @pl.when(edge)
        def _():
            v_copy(b, c).wait_recv()
            e_copy(b, c).wait_send()

    def out_copies(b):
        return (pltpu.make_async_copy(UF.at[b], u_hbm.at[b], out_sem.at[b, 0]),
                pltpu.make_async_copy(VF.at[b], v_hbm.at[b], out_sem.at[b, 1]))

    def cost_part(b):
        v_drain(b)
        uf_copy(b).wait()
        acc = jnp.zeros((m, 128), F32)
        for o, w in tiles(n):
            p = UF[b, :, o:o + w] * dot_nn(VB[b], KCT[:, o:o + w])
            for q in range(0, w, 128):
                acc = acc + p[:, q:q + 128]
        ACC[pl.ds(pl.multiple_of(b * m, m), m), :] = acc
        for c in range(len(t_pieces)):
            pl.when(inner)(lambda c=c: vf_copy(b, c).wait_send())
            pl.when(edge)(lambda c=c: vf_copy(b, c).wait_recv())
        for cp in out_copies(b):
            cp.start()

    def kc(t):
        rows = at(t * 128, 128)

        def turn(q, carry):
            cols = at(q * 256, 256)
            KCT[cols, rows] = KT[cols, rows] * jnp.transpose(C[rows, cols])
            return carry

        lax.fori_loop(0, n // 256, turn, 0)

    def kt(t):
        rows = at(t * (n // 3), n // 3)

        def turn(q, carry):
            cols = at(q * 256, 256)
            KT[cols, rows] = jnp.transpose(K[rows, cols])
            return carry

        lax.fori_loop(0, n // 256, turn, 0)

    steps = {"sa": sa, "s1": s1, "s2": s2, "s3": s3, "s4": s4, "ta": ta, "t0": t0, "t1": t1, "t2": t2, "t3": t3i, "e": t3e}

    def tick(i, carry):
        for name, piece, lag in ORDER:
            if name == "cost":
                pl.when(i >= total_inst)(lambda: cost_part(i - total_inst))
            elif name == "kt":
                pl.when(i < 4)(lambda: kt(i - 1))
            elif name == "kc":
                pl.when(i == KC_FIRST)(lambda: c_load.wait())
                pl.when(jnp.logical_and(i >= KC_FIRST, i < KC_FIRST + n // 128))(lambda: kc(i - KC_FIRST))
            else:
                g = i - lag
                fn = steps[name] if piece is None else functools.partial(steps[name], piece)

                @pl.when(jnp.logical_and(g >= (NB if name[0] == "s" else 0), g < total_inst))
                def _():
                    sweep = lax.div(g, NB)
                    fn(lax.rem(g, NB), lax.rem(sweep, 2), sweep == SWEEPS - 1)
        return carry

    lax.fori_loop(1, total_inst + NB, tick, 0)

    tot = jnp.sum(jnp.transpose(ACC[...]), axis=0, keepdims=True)
    CPS[...] = jnp.broadcast_to(tot, CPS.shape)
    me = row * n_col + col
    cps = [rcopy(CPS, CPR.at[me], cp_sem.at[i], dev) for i, dev in enumerate(peers)]
    for cp in cps:
        cp.start()
    CPR[me] = CPS[...]
    for cp in cps:
        cp.wait()
    total = CPR[0]
    for i in range(1, n_row * n_col):
        total = total + CPR[i]
    cost_ref[...] = total[0:1, 0:cost_ref.shape[1]] / norm
    for b in range(NB):
        for cp in out_copies(b):
            cp.wait()


def solution(mesh):
    n_row = mesh.shape["row"]
    n_col = mesh.shape["col"]

    def local_fn(kern, cost_mat, src_mass, tgt_mass):
        n = kern.shape[0]
        q = src_mass.shape[1]
        m = q // NB
        half = n // 2
        norm = float(n * n_row) * float(kern.shape[1] * n_col)
        dma = pltpu.SemaphoreType.DMA
        vmem = pltpu.VMEM
        any_spec = pl.BlockSpec(memory_space=pl.ANY)
        np_, ns = len(T_PIECES), len(S_PIECES)
        u, v, cost = pl.pallas_call(
            functools.partial(kernel, n_row, n_col, norm),
            out_shape=(jax.ShapeDtypeStruct((NB, m, n), F32), jax.ShapeDtypeStruct((NB, m, n), F32),
                       jax.ShapeDtypeStruct((1, q), F32)),
            in_specs=[any_spec] * 4,
            out_specs=(any_spec, any_spec, pl.BlockSpec(memory_space=pltpu.VMEM)),
            scratch_shapes=[
                vmem((n, n), BF16), vmem((n, n), BF16), vmem((n, n), BF16), vmem((n, n), BF16),
                vmem((NB, m, n), F32), vmem((NB, m, n), F32),
                vmem((NB, m, n), BF16), vmem((NB, m, n), BF16),
                vmem((NB, m, n), F32), vmem((NB, m, n), F32),
                vmem((NB, m, half), F32), vmem((NB, m, half), F32),
                vmem((NB, m, half), F32), vmem((2, NB, m, half), F32),
                vmem((NB, m, n), F32), vmem((NB, m, n), F32),
                vmem((2, NB, m, n), F32),
                vmem((4, 8, half), F32),
                vmem((128, 128), F32), vmem((8, 128), F32), vmem((n_row * n_col, 8, 128), F32),
                dma((6,)), dma((3,)), dma((NB, 2)), dma((2, 2)),
                dma((NB, ns, 2)), dma((2, NB, ns, 2)), dma((NB, ns, 2)), dma((NB, 2)),
                dma((NB, np_, 2)), dma((2, NB, np_, 2)), dma((NB, np_, 2)), dma((NB, np_, 2)),
                dma((n_row * n_col - 1, 2)),
            ],
            compiler_params=pltpu.CompilerParams(collective_id=0, has_side_effects=True, vmem_limit_bytes=60 * 1024 * 1024),
        )(kern, cost_mat, src_mass.T.reshape(NB, m, n), tgt_mass.T.reshape(NB, m, n))
        return u.reshape(q, n).T, v.reshape(q, n).T, cost.reshape(q)

    return jax.shard_map(local_fn, mesh=mesh, in_specs=(P("row", "col"), P("row", "col"), P("row", "prob"), P("col", "prob")),
                         out_specs=(P("row", "prob"), P("col", "prob"), P("prob")), check_vma=False)
```

```python
import functools

import jax
import jax.numpy as jnp
from jax import lax
from jax.experimental import pallas as pl
from jax.experimental.pallas import tpu as pltpu
from jax.sharding import PartitionSpec as P

SWEEPS = 6
MESH = pl.DeviceIdType.MESH
F32 = jnp.float32
BF16 = jnp.bfloat16
NB = 4
T_PIECES = (512, 512, 512, 512, 256)
EARLY = 3
S_PIECES = (512, 640)
K_PIECES = (768, 768, 512, 256)
KC_FIRST = 5
ORDER = (
    ("e", 4, 4), ("t2", 4, 3), ("s4", 0, 1), ("t2", 3, 3), ("e", 3, 4), ("s1", None, 0), ("t3", 0, 3),
    ("s2", None, 0), ("cost", None, 0), ("s4", 1, 1), ("ta", None, 1), ("s3", 0, 0), ("t3", 1, 3),
    ("t0", None, 1), ("t1", 0, 1), ("t2", 0, 2), ("s3", 1, 0), ("t1", 1, 1), ("t3", 2, 3), ("t1", 2, 1),
    ("kc", None, 0), ("e", 0, 3), ("t2", 1, 2), ("t1", 3, 1), ("t2", 2, 2), ("kt", None, 0), ("t3", 4, 3),
    ("t3", 3, 3), ("e", 1, 3), ("t1", 4, 1), ("e", 2, 3), ("sa", None, -1), ("ca", None, -1),
)


def dot_nn(x, y):
    return jnp.dot(x, y, preferred_element_type=F32)


def dot_nt(x, y):
    return lax.dot_general(x, y, (((1,), (1,)), ((), ())), preferred_element_type=F32)


def spans(sizes):
    out, o = [], 0
    for w in sizes:
        out.append((o, w))
        o += w
    return out


def tiles(size, tile=256):
    return [(o, min(tile, size - o)) for o in range(0, size, tile)]


def kernel(n_row, n_col, norm,
           k_hbm, c_hbm, a_hbm, b_hbm, UF, VF, cost_ref,
           K, KT, C, KCT, A, B, UB, VB, WP, DS, DR, SP, YR, TP, EI, XR, RX, ACC, CPS, CPR,
           k_sem, in_sem, r_sem,
           d_sem, y_sem, u_sem, uf_sem, e_sem, x_sem, v_sem, vf_sem, cp_sem):
    row = lax.axis_index("row")
    col = lax.axis_index("col")
    core = lax.rem(col, 2)
    n = K.shape[0]
    half = n // 2
    m = UB.shape[1]
    total_inst = SWEEPS * NB
    sib = {"col": col + 1 - 2 * core}
    ypeer = {"col": lax.rem(col + 2, n_col)}
    inner = jnp.logical_or(row == 1, row == 2)
    edge = jnp.logical_not(inner)
    zpair = {"row": row + 1 - 2 * lax.rem(row, 2)}
    zmid = {"row": n_row - 1 - row}
    own0 = pl.multiple_of(core * half, 128)
    sib0 = pl.multiple_of((1 - core) * half, 128)
    t_pieces = spans(T_PIECES)
    s_pieces = spans(S_PIECES)

    def at(o, w):
        return pl.ds(pl.multiple_of(o, 128), w)

    def rcopy(src, dst, sem, dev):
        return pltpu.make_async_remote_copy(src_ref=src, dst_ref=dst, send_sem=sem.at[0], recv_sem=sem.at[1],
                                            device_id=dev, device_id_type=MESH)

    a_load = pltpu.make_async_copy(a_hbm, A, in_sem.at[0])
    b_load = pltpu.make_async_copy(b_hbm, B, in_sem.at[1])
    c_load = pltpu.make_async_copy(c_hbm, C, in_sem.at[2])
    k_loads = [pltpu.make_async_copy(k_hbm.at[o:o + w, :], K.at[o:o + w, :], k_sem.at[j])
               for j, (o, w) in enumerate(spans(K_PIECES))]
    for cp in k_loads:
        cp.start()
    a_load.start()

    barrier = pltpu.get_barrier_semaphore()
    rel = [(dr, dc) for dr in range(n_row) for dc in range(n_col) if (dr, dc) != (0, 0)]
    peers = [{"row": lax.rem(row + dr, n_row), "col": lax.rem(col + dc, n_col)} for dr, dc in rel]
    for dev in peers:
        pl.semaphore_signal(barrier, inc=1, device_id=dev, device_id_type=MESH)

    ACC[...] = jnp.zeros_like(ACC)

    ones = jnp.ones((16, n), BF16)
    for cp, (o, w) in zip(k_loads, spans(K_PIECES)):
        cp.wait()
        RX[col, :, o:o + w] = dot_nt(ones, K[o:o + w, :])[:1]
    pl.semaphore_wait(barrier, len(peers))
    r_copies = [rcopy(RX.at[col], RX.at[col], r_sem.at[d - 1], {"col": lax.rem(col + d, n_col)}) for d in range(1, n_col)]
    for cp in r_copies:
        cp.start()
    b_load.start()
    c_load.start()
    a_load.wait()
    for cp in r_copies:
        cp.wait()
    s0 = RX[0] + RX[1]
    for d in range(2, n_col):
        s0 = s0 + RX[d]
    for b in range(NB):
        UB[b] = (A[b] / s0).astype(BF16)
    b_load.wait()

    def u_copy(b, j):
        o, w = s_pieces[j]
        ref = UB.at[b, :, at(own0 + o, w)]
        return rcopy(ref, ref, u_sem.at[b, j], sib)

    def uf_copy(b):
        ref = UF.at[b, :, at(own0, half)]
        return rcopy(ref, ref, uf_sem.at[b], sib)

    def d_copy(b, j):
        o, w = s_pieces[j]
        return rcopy(DS.at[b, :, pl.ds(o, w)], DR.at[b, :, pl.ds(o, w)], d_sem.at[b, j], sib)

    def y_copy(par, b, j):
        o, w = s_pieces[j]
        return rcopy(SP.at[b, :, pl.ds(o, w)], YR.at[par, b, :, pl.ds(o, w)], y_sem.at[par, b, j], ypeer)

    def e_copy(b, c):
        o, w = t_pieces[c]
        return rcopy(TP.at[b, :, pl.ds(o, w)], EI.at[b, :, pl.ds(o, w)], e_sem.at[b, c], zpair)

    def x_copy(par, b, c):
        o, w = t_pieces[c]
        return rcopy(TP.at[b, :, pl.ds(o, w)], XR.at[par, b, :, pl.ds(o, w)], x_sem.at[par, b, c], zmid)

    def v_copy(b, c):
        o, w = t_pieces[c]
        ref = VB.at[b, :, pl.ds(o, w)]
        return rcopy(ref, ref, v_sem.at[b, c], zpair)

    def vf_copy(b, c):
        o, w = t_pieces[c]
        ref = VF.at[b, :, pl.ds(o, w)]
        return rcopy(ref, ref, vf_sem.at[b, c], zpair)

    early = sum(T_PIECES[:EARLY])

    def sa(b, par, last):
        for dst, h0 in ((DS, sib0), (SP, own0)):
            for o, w in tiles(half):
                dst[b, :, o:o + w] = dot_nn(VB[b, :, :early], KT[:early, at(h0 + o, w)])

    def s1(b, par, last):
        for j, (o0, width) in enumerate(s_pieces):
            for o, w in tiles(width):
                o += o0
                DS[b, :, o:o + w] += dot_nn(VB[b, :, early:], KT[early:, at(sib0 + o, w)])
            d_copy(b, j).start()

    def s2(b, par, last):
        for o, w in tiles(half):
            SP[b, :, o:o + w] += dot_nn(VB[b, :, early:], KT[early:, at(own0 + o, w)])

    def v_drain(b):
        @pl.when(inner)
        def _():
            for c in range(len(t_pieces)):
                v_copy(b, c).wait_send()

    def s3(j, b, par, last):
        o, w = s_pieces[j]
        d_copy(b, j).wait_recv()
        SP[b, :, o:o + w] = SP[b, :, o:o + w] + DR[b, :, o:o + w]
        y_copy(par, b, j).start()
        if j == len(s_pieces) - 1:
            v_drain(b)

    def s4(j, b, par, last):
        o, w = s_pieces[j]
        y_copy(par, b, j).wait_recv()
        sl = at(own0 + o, w)
        u = A[b, :, sl] / (SP[b, :, o:o + w] + YR[par, b, :, o:o + w])
        UB[b, :, sl] = u.astype(BF16)
        u_copy(b, j).start()
        UF[b, :, sl] = u
        if j == len(s_pieces) - 1:
            pl.when(last)(lambda: uf_copy(b).start())
        d_copy(b, j).wait_send()
        y_copy(par, b, j).wait_send()

    def t0(b, par, last):
        for j in range(len(s_pieces)):
            u_copy(b, j).wait()

    def ta(b, par, last):
        for o, w in tiles(n):
            TP[b, :, o:o + w] = dot_nn(UB[b, :, at(own0, half)], K[at(own0, half), o:o + w])

    def t1(c, b, par, last):
        o0, width = t_pieces[c]
        for o, w in tiles(width):
            o += o0
            TP[b, :, o:o + w] += dot_nn(UB[b, :, at(sib0, half)], K[at(sib0, half), o:o + w])
        pl.when(edge)(lambda: e_copy(b, c).start())

    def t2(c, b, par, last):
        o, w = t_pieces[c]

        @pl.when(inner)
        def _():
            e_copy(b, c).wait_recv()
            TP[b, :, o:o + w] = TP[b, :, o:o + w] + EI[b, :, o:o + w]
            x_copy(par, b, c).start()

    def t3i(c, b, par, last):
        o, w = t_pieces[c]

        @pl.when(inner)
        def _():
            x_copy(par, b, c).wait_recv()
            v = B[b, :, o:o + w] / (TP[b, :, o:o + w] + XR[par, b, :, o:o + w])
            VB[b, :, o:o + w] = v.astype(BF16)
            v_copy(b, c).start()
            VF[b, :, o:o + w] = v
            pl.when(last)(lambda: vf_copy(b, c).start())
            x_copy(par, b, c).wait_send()

    def t3e(c, b, par, last):
        @pl.when(edge)
        def _():
            v_copy(b, c).wait_recv()
            e_copy(b, c).wait_send()

    def cost_early(b):
        for o, w in tiles(n):
            WP[:, o:o + w] = dot_nn(VB[b, :, :early], KCT[:early, o:o + w])

    def cost_part(b):
        v_drain(b)
        uf_copy(b).wait()
        acc = jnp.zeros((m, 128), F32)
        for o, w in tiles(n):
            p = UF[b, :, o:o + w] * (WP[:, o:o + w] + dot_nn(VB[b, :, early:], KCT[early:, o:o + w]))
            for q in range(0, w, 128):
                acc = acc + p[:, q:q + 128]
        ACC[pl.ds(pl.multiple_of(b * m, m), m), :] = acc
        for c in range(len(t_pieces)):
            pl.when(inner)(lambda c=c: vf_copy(b, c).wait_send())
            pl.when(edge)(lambda c=c: vf_copy(b, c).wait_recv())

    def kc(t):
        rows = at(t * 128, 128)

        def turn(q, carry):
            cols = at(q * 256, 256)
            KCT[cols, rows] = KT[cols, rows] * jnp.transpose(C[rows, cols])
            return carry

        lax.fori_loop(0, n // 256, turn, 0)

    def kt(t):
        rows = at(t * (n // 3), n // 3)

        def turn(q, carry):
            cols = at(q * 256, 256)
            KT[cols, rows] = jnp.transpose(K[rows, cols])
            return carry

        lax.fori_loop(0, n // 256, turn, 0)

    steps = {"sa": sa, "s1": s1, "s2": s2, "s3": s3, "s4": s4, "ta": ta, "t0": t0, "t1": t1, "t2": t2, "t3": t3i, "e": t3e}

    def tick(i, carry):
        for name, piece, lag in ORDER:
            if name == "cost":
                pl.when(i >= total_inst)(lambda: cost_part(i - total_inst))
            elif name == "ca":
                g = i - lag
                pl.when(jnp.logical_and(g >= total_inst, g < total_inst + NB))(lambda: cost_early(g - total_inst))
            elif name == "kt":
                pl.when(i < 4)(lambda: kt(i - 1))
            elif name == "kc":
                pl.when(i == KC_FIRST)(lambda: c_load.wait())
                pl.when(jnp.logical_and(i >= KC_FIRST, i < KC_FIRST + n // 128))(lambda: kc(i - KC_FIRST))
            else:
                g = i - lag
                fn = steps[name] if piece is None else functools.partial(steps[name], piece)

                @pl.when(jnp.logical_and(g >= (NB if name[0] == "s" or name == "t0" else 0), g < total_inst))
                def _():
                    sweep = lax.div(g, NB)
                    fn(lax.rem(g, NB), lax.rem(sweep, 2), sweep == SWEEPS - 1)
        return carry

    lax.fori_loop(1, total_inst + NB, tick, 0)

    tot = jnp.sum(jnp.transpose(ACC[...]), axis=0, keepdims=True)
    CPS[...] = jnp.broadcast_to(tot, CPS.shape)
    me = row * n_col + col
    cps = [rcopy(CPS, CPR.at[me], cp_sem.at[i], dev) for i, dev in enumerate(peers)]
    for cp in cps:
        cp.start()
    CPR[me] = CPS[...]
    for cp in cps:
        cp.wait()
    total = CPR[0]
    for i in range(1, n_row * n_col):
        total = total + CPR[i]
    cost_ref[...] = total[0:1, 0:cost_ref.shape[1]] / norm


def solution(mesh):
    n_row = mesh.shape["row"]
    n_col = mesh.shape["col"]

    def local_fn(kern, cost_mat, src_mass, tgt_mass):
        n = kern.shape[0]
        q = src_mass.shape[1]
        m = q // NB
        half = n // 2
        norm = float(n * n_row) * float(kern.shape[1] * n_col)
        dma = pltpu.SemaphoreType.DMA
        vmem = pltpu.VMEM
        any_spec = pl.BlockSpec(memory_space=pl.ANY)
        np_, ns = len(T_PIECES), len(S_PIECES)
        u, v, cost = pl.pallas_call(
            functools.partial(kernel, n_row, n_col, norm),
            out_shape=(vmem((NB, m, n), F32), vmem((NB, m, n), F32), vmem((1, q), F32)),
            in_specs=[any_spec] * 4,
            out_specs=(pl.BlockSpec(memory_space=vmem),) * 3,
            scratch_shapes=[
                vmem((n, n), BF16), vmem((n, n), BF16), vmem((n, n), BF16), vmem((n, n), BF16),
                vmem((NB, m, n), F32), vmem((NB, m, n), F32),
                vmem((NB, m, n), BF16), vmem((NB, m, n), BF16),
                vmem((m, n), F32),
                vmem((NB, m, half), F32), vmem((NB, m, half), F32),
                vmem((NB, m, half), F32), vmem((2, NB, m, half), F32),
                vmem((NB, m, n), F32), vmem((NB, m, n), F32),
                vmem((2, NB, m, n), F32),
                vmem((n_col, 1, n), F32),
                vmem((128, 128), F32), vmem((8, 128), F32), vmem((n_row * n_col, 8, 128), F32),
                dma((len(K_PIECES),)), dma((3,)), dma((n_col - 1, 2)),
                dma((NB, ns, 2)), dma((2, NB, ns, 2)), dma((NB, ns, 2)), dma((NB, 2)),
                dma((NB, np_, 2)), dma((2, NB, np_, 2)), dma((NB, np_, 2)), dma((NB, np_, 2)),
                dma((n_row * n_col - 1, 2)),
            ],
            compiler_params=pltpu.CompilerParams(collective_id=0, has_side_effects=True, vmem_limit_bytes=60 * 1024 * 1024),
        )(kern, cost_mat, src_mass.T.reshape(NB, m, n), tgt_mass.T.reshape(NB, m, n))
        return u.reshape(q, n).T, v.reshape(q, n).T, cost.reshape(q)

    return jax.shard_map(local_fn, mesh=mesh, in_specs=(P("row", "col"), P("row", "col"), P("row", "prob"), P("col", "prob")),
                         out_specs=(P("row", "prob"), P("col", "prob"), P("prob")), check_vma=False)
```

```python
import functools

import jax
import jax.numpy as jnp
from jax import lax
from jax.experimental import pallas as pl
from jax.experimental.pallas import tpu as pltpu
from jax.sharding import PartitionSpec as P

SWEEPS = 6
MESH = pl.DeviceIdType.MESH
F32 = jnp.float32
BF16 = jnp.bfloat16
NB = 4
T_PIECES = (512, 512, 512, 512, 256)
EARLY = ((0, 1), (2,))
TA_PIECES = (1024, 1280)
S_PIECES = (512, 640)
K_PIECES = (768, 768, 512, 256)
KC_FIRST = 5
ORDER = (
    ("s4", 0, 1), ("t3", 1, 3), ("s4", 1, 1), ("ta", 0, 1), ("t2", 0, 2), ("t3", 2, 3), ("s3", 0, 0),
    ("ta", 1, 1), ("s3", 1, 0), ("t2", 1, 2), ("t3", 3, 3), ("t0", None, 1), ("t1", 0, 1), ("t3", 4, 3),
    ("t1", 1, 1), ("t2", 2, 2), ("kc", None, 0), ("t1", 2, 1), ("t2", 3, 2), ("t1", 3, 1), ("e", 0, 3),
    ("t2", 4, 2), ("kt", None, 0), ("e", 1, 3), ("sa", 0, -1), ("e", 2, 3), ("sa", 1, -1), ("ca", None, -1),
    ("t3", 0, 2), ("e", 3, 3), ("t1", 4, 1), ("e", 4, 3), ("s1", None, -1), ("s2", None, -1),
    ("cost", None, -1),
)


def dot_nn(x, y):
    return jnp.dot(x, y, preferred_element_type=F32)


def dot_nt(x, y):
    return lax.dot_general(x, y, (((1,), (1,)), ((), ())), preferred_element_type=F32)


def spans(sizes):
    out, o = [], 0
    for w in sizes:
        out.append((o, w))
        o += w
    return out


def tiles(size, tile=256):
    return [(o, min(tile, size - o)) for o in range(0, size, tile)]


def kernel(n_row, n_col, norm,
           k_hbm, c_hbm, a_hbm, b_hbm, UF, VF, cost_ref,
           K, KT, C, KCT, A, B, UB, VB, WP, DS, DR, SP, YR, TP, EI, XR, RX, ACC, CPS, CPR,
           k_sem, in_sem, r_sem,
           d_sem, y_sem, u_sem, uf_sem, e_sem, x_sem, v_sem, vf_sem, cp_sem):
    row = lax.axis_index("row")
    col = lax.axis_index("col")
    core = lax.rem(col, 2)
    n = K.shape[0]
    half = n // 2
    m = UB.shape[1]
    total_inst = SWEEPS * NB
    sib = {"col": col + 1 - 2 * core}
    ypeer = {"col": lax.rem(col + 2, n_col)}
    inner = jnp.logical_or(row == 1, row == 2)
    edge = jnp.logical_not(inner)
    zpair = {"row": row + 1 - 2 * lax.rem(row, 2)}
    zmid = {"row": n_row - 1 - row}
    own0 = pl.multiple_of(core * half, 128)
    sib0 = pl.multiple_of((1 - core) * half, 128)
    t_pieces = spans(T_PIECES)
    s_pieces = spans(S_PIECES)

    def at(o, w):
        return pl.ds(pl.multiple_of(o, 128), w)

    def rcopy(src, dst, sem, dev):
        return pltpu.make_async_remote_copy(src_ref=src, dst_ref=dst, send_sem=sem.at[0], recv_sem=sem.at[1],
                                            device_id=dev, device_id_type=MESH)

    a_load = pltpu.make_async_copy(a_hbm, A, in_sem.at[0])
    b_load = pltpu.make_async_copy(b_hbm, B, in_sem.at[1])
    c_load = pltpu.make_async_copy(c_hbm, C, in_sem.at[2])
    k_loads = [pltpu.make_async_copy(k_hbm.at[o:o + w, :], K.at[o:o + w, :], k_sem.at[j])
               for j, (o, w) in enumerate(spans(K_PIECES))]
    for cp in k_loads:
        cp.start()
    a_load.start()

    barrier = pltpu.get_barrier_semaphore()
    rel = [(dr, dc) for dr in range(n_row) for dc in range(n_col) if (dr, dc) != (0, 0)]
    peers = [{"row": lax.rem(row + dr, n_row), "col": lax.rem(col + dc, n_col)} for dr, dc in rel]
    for dev in peers:
        pl.semaphore_signal(barrier, inc=1, device_id=dev, device_id_type=MESH)

    ACC[...] = jnp.zeros_like(ACC)

    ones = jnp.ones((16, n), BF16)
    for cp, (o, w) in zip(k_loads, spans(K_PIECES)):
        cp.wait()
        RX[col, :, o:o + w] = dot_nt(ones, K[o:o + w, :])[:1]
    pl.semaphore_wait(barrier, len(peers))
    r_copies = [rcopy(RX.at[col], RX.at[col], r_sem.at[d - 1], {"col": lax.rem(col + d, n_col)}) for d in range(1, n_col)]
    for cp in r_copies:
        cp.start()
    b_load.start()
    c_load.start()
    a_load.wait()
    for cp in r_copies:
        cp.wait()
    s0 = RX[0] + RX[1]
    for d in range(2, n_col):
        s0 = s0 + RX[d]
    for b in range(NB):
        UB[b] = (A[b] / s0).astype(BF16)
    b_load.wait()

    def u_copy(b, j):
        o, w = s_pieces[j]
        ref = UB.at[b, :, at(own0 + o, w)]
        return rcopy(ref, ref, u_sem.at[b, j], sib)

    def uf_copy(b):
        ref = UF.at[b, :, at(own0, half)]
        return rcopy(ref, ref, uf_sem.at[b], sib)

    def d_copy(b, j):
        o, w = s_pieces[j]
        return rcopy(DS.at[b, :, pl.ds(o, w)], DR.at[b, :, pl.ds(o, w)], d_sem.at[b, j], sib)

    def y_copy(par, b, j):
        o, w = s_pieces[j]
        return rcopy(SP.at[b, :, pl.ds(o, w)], YR.at[par, b, :, pl.ds(o, w)], y_sem.at[par, b, j], ypeer)

    def e_copy(b, c):
        o, w = t_pieces[c]
        return rcopy(TP.at[b, :, pl.ds(o, w)], EI.at[b, :, pl.ds(o, w)], e_sem.at[b, c], zpair)

    def x_copy(par, b, c):
        o, w = t_pieces[c]
        return rcopy(TP.at[b, :, pl.ds(o, w)], XR.at[par, b, :, pl.ds(o, w)], x_sem.at[par, b, c], zmid)

    def v_copy(b, c):
        o, w = t_pieces[c]
        ref = VB.at[b, :, pl.ds(o, w)]
        return rcopy(ref, ref, v_sem.at[b, c], zpair)

    def vf_copy(b, c):
        o, w = t_pieces[c]
        ref = VF.at[b, :, pl.ds(o, w)]
        return rcopy(ref, ref, vf_sem.at[b, c], zpair)

    early_spans = spans([sum(T_PIECES[c] for c in group) for group in EARLY])
    early = sum(w for _, w in early_spans)

    def sa(q, b, par, last):
        k0, kw = early_spans[q]
        for dst, h0 in ((DS, sib0), (SP, own0)):
            for o, w in tiles(half):
                part = dot_nn(VB[b, :, k0:k0 + kw], KT[k0:k0 + kw, at(h0 + o, w)])
                dst[b, :, o:o + w] = part if q == 0 else dst[b, :, o:o + w] + part

    def s1(b, par, last):
        for j, (o0, width) in enumerate(s_pieces):
            for o, w in tiles(width):
                o += o0
                DS[b, :, o:o + w] += dot_nn(VB[b, :, early:], KT[early:, at(sib0 + o, w)])
            d_copy(b, j).start()

    def s2(b, par, last):
        for o, w in tiles(half):
            SP[b, :, o:o + w] += dot_nn(VB[b, :, early:], KT[early:, at(own0 + o, w)])

    def v_drain(b):
        @pl.when(inner)
        def _():
            for c in range(len(t_pieces)):
                v_copy(b, c).wait_send()

    def s3(j, b, par, last):
        o, w = s_pieces[j]
        d_copy(b, j).wait_recv()
        SP[b, :, o:o + w] = SP[b, :, o:o + w] + DR[b, :, o:o + w]
        y_copy(par, b, j).start()
        if j == len(s_pieces) - 1:
            v_drain(b)

    def s4(j, b, par, last):
        o, w = s_pieces[j]
        y_copy(par, b, j).wait_recv()
        sl = at(own0 + o, w)
        u = A[b, :, sl] / (SP[b, :, o:o + w] + YR[par, b, :, o:o + w])
        UB[b, :, sl] = u.astype(BF16)
        u_copy(b, j).start()
        UF[b, :, sl] = u
        if j == len(s_pieces) - 1:
            pl.when(last)(lambda: uf_copy(b).start())
        d_copy(b, j).wait_send()
        y_copy(par, b, j).wait_send()

    def t0(b, par, last):
        for j in range(len(s_pieces)):
            u_copy(b, j).wait()

    def ta(q, b, par, last):
        o0, width = spans(TA_PIECES)[q]
        for o, w in tiles(width):
            o += o0
            TP[b, :, o:o + w] = dot_nn(UB[b, :, at(own0, half)], K[at(own0, half), o:o + w])

    def t1(c, b, par, last):
        o0, width = t_pieces[c]
        for o, w in tiles(width):
            o += o0
            TP[b, :, o:o + w] += dot_nn(UB[b, :, at(sib0, half)], K[at(sib0, half), o:o + w])
        pl.when(edge)(lambda: e_copy(b, c).start())

    def t2(c, b, par, last):
        o, w = t_pieces[c]

        @pl.when(inner)
        def _():
            e_copy(b, c).wait_recv()
            TP[b, :, o:o + w] = TP[b, :, o:o + w] + EI[b, :, o:o + w]
            x_copy(par, b, c).start()

    def t3i(c, b, par, last):
        o, w = t_pieces[c]

        @pl.when(inner)
        def _():
            x_copy(par, b, c).wait_recv()
            v = B[b, :, o:o + w] / (TP[b, :, o:o + w] + XR[par, b, :, o:o + w])
            VB[b, :, o:o + w] = v.astype(BF16)
            v_copy(b, c).start()
            VF[b, :, o:o + w] = v
            pl.when(last)(lambda: vf_copy(b, c).start())
            x_copy(par, b, c).wait_send()

    def t3e(c, b, par, last):
        @pl.when(edge)
        def _():
            v_copy(b, c).wait_recv()
            e_copy(b, c).wait_send()

    def cost_early(b):
        for o, w in tiles(n):
            WP[:, o:o + w] = dot_nn(VB[b, :, :early], KCT[:early, o:o + w])

    def cost_part(b):
        v_drain(b)
        uf_copy(b).wait()
        acc = jnp.zeros((m, 128), F32)
        for o, w in tiles(n):
            p = UF[b, :, o:o + w] * (WP[:, o:o + w] + dot_nn(VB[b, :, early:], KCT[early:, o:o + w]))
            for q in range(0, w, 128):
                acc = acc + p[:, q:q + 128]
        ACC[pl.ds(pl.multiple_of(b * m, m), m), :] = acc
        for c in range(len(t_pieces)):
            pl.when(inner)(lambda c=c: vf_copy(b, c).wait_send())
            pl.when(edge)(lambda c=c: vf_copy(b, c).wait_recv())

    def kc(t):
        rows = at(t * 128, 128)

        def turn(q, carry):
            cols = at(q * 256, 256)
            KCT[cols, rows] = KT[cols, rows] * jnp.transpose(C[rows, cols])
            return carry

        lax.fori_loop(0, n // 256, turn, 0)

    def kt(t):
        rows = at(t * (n // 3), n // 3)

        def turn(q, carry):
            cols = at(q * 256, 256)
            KT[cols, rows] = jnp.transpose(K[rows, cols])
            return carry

        lax.fori_loop(0, n // 256, turn, 0)

    steps = {"sa": sa, "s1": s1, "s2": s2, "s3": s3, "s4": s4, "ta": ta, "t0": t0, "t1": t1, "t2": t2, "t3": t3i, "e": t3e}

    def tick(i, carry):
        for name, piece, lag in ORDER:
            if name == "cost":
                g = i - lag
                pl.when(jnp.logical_and(g >= total_inst, g < total_inst + NB))(lambda: cost_part(g - total_inst))
            elif name == "ca":
                g = i - lag
                pl.when(jnp.logical_and(g >= total_inst, g < total_inst + NB))(lambda: cost_early(g - total_inst))
            elif name == "kt":
                pl.when(i < 4)(lambda: kt(i - 1))
            elif name == "kc":
                pl.when(i == KC_FIRST)(lambda: c_load.wait())
                pl.when(jnp.logical_and(i >= KC_FIRST, i < KC_FIRST + n // 128))(lambda: kc(i - KC_FIRST))
            else:
                g = i - lag
                fn = steps[name] if piece is None else functools.partial(steps[name], piece)

                @pl.when(jnp.logical_and(g >= (NB if name[0] == "s" or name == "t0" else 0), g < total_inst))
                def _():
                    sweep = lax.div(g, NB)
                    fn(lax.rem(g, NB), lax.rem(sweep, 2), sweep == SWEEPS - 1)
        return carry

    lax.fori_loop(1, total_inst + NB, tick, 0)

    tot = jnp.sum(jnp.transpose(ACC[...]), axis=0, keepdims=True)
    CPS[...] = jnp.broadcast_to(tot, CPS.shape)
    me = row * n_col + col
    cps = [rcopy(CPS, CPR.at[me], cp_sem.at[i], dev) for i, dev in enumerate(peers)]
    for cp in cps:
        cp.start()
    CPR[me] = CPS[...]
    for cp in cps:
        cp.wait()
    total = CPR[0]
    for i in range(1, n_row * n_col):
        total = total + CPR[i]
    cost_ref[...] = total[0:1, 0:cost_ref.shape[1]] / norm


def solution(mesh):
    n_row = mesh.shape["row"]
    n_col = mesh.shape["col"]

    def local_fn(kern, cost_mat, src_mass, tgt_mass):
        n = kern.shape[0]
        q = src_mass.shape[1]
        m = q // NB
        half = n // 2
        norm = float(n * n_row) * float(kern.shape[1] * n_col)
        dma = pltpu.SemaphoreType.DMA
        vmem = pltpu.VMEM
        any_spec = pl.BlockSpec(memory_space=pl.ANY)
        np_, ns = len(T_PIECES), len(S_PIECES)
        u, v, cost = pl.pallas_call(
            functools.partial(kernel, n_row, n_col, norm),
            out_shape=(vmem((NB, m, n), F32), vmem((NB, m, n), F32), vmem((1, q), F32)),
            in_specs=[any_spec] * 4,
            out_specs=(pl.BlockSpec(memory_space=vmem),) * 3,
            scratch_shapes=[
                vmem((n, n), BF16), vmem((n, n), BF16), vmem((n, n), BF16), vmem((n, n), BF16),
                vmem((NB, m, n), F32), vmem((NB, m, n), F32),
                vmem((NB, m, n), BF16), vmem((NB, m, n), BF16),
                vmem((m, n), F32),
                vmem((NB, m, half), F32), vmem((NB, m, half), F32),
                vmem((NB, m, half), F32), vmem((2, NB, m, half), F32),
                vmem((NB, m, n), F32), vmem((NB, m, n), F32),
                vmem((2, NB, m, n), F32),
                vmem((n_col, 1, n), F32),
                vmem((128, 128), F32), vmem((8, 128), F32), vmem((n_row * n_col, 8, 128), F32),
                dma((len(K_PIECES),)), dma((3,)), dma((n_col - 1, 2)),
                dma((NB, ns, 2)), dma((2, NB, ns, 2)), dma((NB, ns, 2)), dma((NB, 2)),
                dma((NB, np_, 2)), dma((2, NB, np_, 2)), dma((NB, np_, 2)), dma((NB, np_, 2)),
                dma((n_row * n_col - 1, 2)),
            ],
            compiler_params=pltpu.CompilerParams(collective_id=0, has_side_effects=True, vmem_limit_bytes=60 * 1024 * 1024),
        )(kern, cost_mat, src_mass.T.reshape(NB, m, n), tgt_mass.T.reshape(NB, m, n))
        return u.reshape(q, n).T, v.reshape(q, n).T, cost.reshape(q)

    return jax.shard_map(local_fn, mesh=mesh, in_specs=(P("row", "col"), P("row", "col"), P("row", "prob"), P("col", "prob")),
                         out_specs=(P("row", "prob"), P("col", "prob"), P("prob")), check_vma=False)
```

```python
import functools

import jax
import jax.numpy as jnp
from jax import lax
from jax.experimental import pallas as pl
from jax.experimental.pallas import tpu as pltpu
from jax.sharding import PartitionSpec as P

SWEEPS = 6
MESH = pl.DeviceIdType.MESH
F32 = jnp.float32
BF16 = jnp.bfloat16
NB = 4
T_PIECES = (512, 512, 512, 512, 256)
EARLY = ((0, 1, 2),)
TA_PIECES = (2304,)
S_PIECES = (512, 640)
K_PIECES = (768, 768, 512, 256)
KC_FIRST = 5
ORDER = (
    ("e", 1, 4), ("e", 2, 4), ("sa", 0, 0), ("ca", None, 0), ("e", 3, 4), ("t3", 0, 3), ("s4", 0, 1),
    ("e", 4, 4), ("s1", None, 0), ("cost", None, 0), ("t3", 1, 3), ("s4", 1, 1), ("ta", 0, 1), ("s3", 0, 0),
    ("t2", 0, 2), ("s3", 1, 0), ("t3", 2, 3), ("t2", 1, 2), ("t0", None, 1), ("t1", None, 1), ("t3", 3, 3),
    ("t2", 2, 2), ("t3", 4, 3), ("e", 0, 3), ("kc", None, 0), ("t2", 3, 2), ("t2", 4, 2), ("kt", None, 0),
)


def dot_nn(x, y):
    return jnp.dot(x, y, preferred_element_type=F32)


def dot_nt(x, y):
    return lax.dot_general(x, y, (((1,), (1,)), ((), ())), preferred_element_type=F32)


def spans(sizes):
    out, o = [], 0
    for w in sizes:
        out.append((o, w))
        o += w
    return out


def tiles(size, tile=256):
    return [(o, min(tile, size - o)) for o in range(0, size, tile)]


def kernel(n_row, n_col, norm,
           k_hbm, c_hbm, a_hbm, b_hbm, UF, VF, cost_ref,
           K, KT, C, KCT, A, B, UB, VB, WP, DS, DR, SP, YR, TP, EI, XR, RX, ACC, CPS, CPR,
           k_sem, in_sem, r_sem,
           d_sem, y_sem, u_sem, uf_sem, e_sem, x_sem, v_sem, vf_sem, cp_sem):
    row = lax.axis_index("row")
    col = lax.axis_index("col")
    core = lax.rem(col, 2)
    n = K.shape[0]
    half = n // 2
    m = UB.shape[1]
    total_inst = SWEEPS * NB
    sib = {"col": col + 1 - 2 * core}
    ypeer = {"col": lax.rem(col + 2, n_col)}
    inner = jnp.logical_or(row == 1, row == 2)
    edge = jnp.logical_not(inner)
    zpair = {"row": row + 1 - 2 * lax.rem(row, 2)}
    zmid = {"row": n_row - 1 - row}
    own0 = pl.multiple_of(core * half, 128)
    sib0 = pl.multiple_of((1 - core) * half, 128)
    t_pieces = spans(T_PIECES)
    s_pieces = spans(S_PIECES)

    def at(o, w):
        return pl.ds(pl.multiple_of(o, 128), w)

    def rcopy(src, dst, sem, dev):
        return pltpu.make_async_remote_copy(src_ref=src, dst_ref=dst, send_sem=sem.at[0], recv_sem=sem.at[1],
                                            device_id=dev, device_id_type=MESH)

    a_load = pltpu.make_async_copy(a_hbm, A, in_sem.at[0])
    b_load = pltpu.make_async_copy(b_hbm, B, in_sem.at[1])
    c_load = pltpu.make_async_copy(c_hbm, C, in_sem.at[2])
    k_loads = [pltpu.make_async_copy(k_hbm.at[o:o + w, :], K.at[o:o + w, :], k_sem.at[j])
               for j, (o, w) in enumerate(spans(K_PIECES))]
    for cp in k_loads:
        cp.start()
    a_load.start()

    barrier = pltpu.get_barrier_semaphore()
    rel = [(dr, dc) for dr in range(n_row) for dc in range(n_col) if (dr, dc) != (0, 0)]
    peers = [{"row": lax.rem(row + dr, n_row), "col": lax.rem(col + dc, n_col)} for dr, dc in rel]
    for dev in peers:
        pl.semaphore_signal(barrier, inc=1, device_id=dev, device_id_type=MESH)

    ACC[...] = jnp.zeros_like(ACC)

    ones = jnp.ones((16, n), BF16)
    for cp, (o, w) in zip(k_loads, spans(K_PIECES)):
        cp.wait()
        RX[col, :, o:o + w] = dot_nt(ones, K[o:o + w, :])[:1]
    pl.semaphore_wait(barrier, len(peers))
    r_copies = [rcopy(RX.at[col], RX.at[col], r_sem.at[d - 1], {"col": lax.rem(col + d, n_col)}) for d in range(1, n_col)]
    for cp in r_copies:
        cp.start()
    b_load.start()
    c_load.start()
    a_load.wait()
    for cp in r_copies:
        cp.wait()
    s0 = RX[0] + RX[1]
    for d in range(2, n_col):
        s0 = s0 + RX[d]
    for b in range(NB):
        UB[b] = (A[b] / s0).astype(BF16)
    b_load.wait()

    def u_copy(b, j):
        o, w = s_pieces[j]
        ref = UB.at[b, :, at(own0 + o, w)]
        return rcopy(ref, ref, u_sem.at[b, j], sib)

    def uf_copy(b):
        ref = UF.at[b, :, at(own0, half)]
        return rcopy(ref, ref, uf_sem.at[b], sib)

    def d_copy(b, j):
        o, w = s_pieces[j]
        return rcopy(DS.at[b, :, pl.ds(o, w)], DR.at[b, :, pl.ds(o, w)], d_sem.at[b, j], sib)

    def y_copy(par, b, j):
        o, w = s_pieces[j]
        return rcopy(SP.at[b, :, pl.ds(o, w)], YR.at[par, b, :, pl.ds(o, w)], y_sem.at[par, b, j], ypeer)

    def e_copy(b, c):
        o, w = t_pieces[c]
        return rcopy(TP.at[b, :, pl.ds(o, w)], EI.at[b, :, pl.ds(o, w)], e_sem.at[b, c], zpair)

    def x_copy(par, b, c):
        o, w = t_pieces[c]
        return rcopy(TP.at[b, :, pl.ds(o, w)], XR.at[par, b, :, pl.ds(o, w)], x_sem.at[par, b, c], zmid)

    def v_copy(b, c):
        o, w = t_pieces[c]
        ref = VB.at[b, :, pl.ds(o, w)]
        return rcopy(ref, ref, v_sem.at[b, c], zpair)

    def vf_copy(b, c):
        o, w = t_pieces[c]
        ref = VF.at[b, :, pl.ds(o, w)]
        return rcopy(ref, ref, vf_sem.at[b, c], zpair)

    early_spans = spans([sum(T_PIECES[c] for c in group) for group in EARLY])
    early = sum(w for _, w in early_spans)

    def sa(q, b, par, last):
        k0, kw = early_spans[q]
        for dst, h0 in ((DS, sib0), (SP, own0)):
            for o, w in tiles(half):
                part = dot_nn(VB[b, :, k0:k0 + kw], KT[k0:k0 + kw, at(h0 + o, w)])
                dst[b, :, o:o + w] = part if q == 0 else dst[b, :, o:o + w] + part

    def s1(b, par, last):
        for j, (o0, width) in enumerate(s_pieces):
            for o, w in tiles(width):
                o += o0
                DS[b, :, o:o + w] += dot_nn(VB[b, :, early:], KT[early:, at(sib0 + o, w)])
            d_copy(b, j).start()
        for o, w in tiles(half):
            SP[b, :, o:o + w] += dot_nn(VB[b, :, early:], KT[early:, at(own0 + o, w)])

    def v_drain(b):
        @pl.when(inner)
        def _():
            for c in range(len(t_pieces)):
                v_copy(b, c).wait_send()

    def s3(j, b, par, last):
        o, w = s_pieces[j]
        d_copy(b, j).wait_recv()
        SP[b, :, o:o + w] = SP[b, :, o:o + w] + DR[b, :, o:o + w]
        y_copy(par, b, j).start()
        if j == len(s_pieces) - 1:
            v_drain(b)

    def s4(j, b, par, last):
        o, w = s_pieces[j]
        y_copy(par, b, j).wait_recv()
        sl = at(own0 + o, w)
        u = A[b, :, sl] / (SP[b, :, o:o + w] + YR[par, b, :, o:o + w])
        UB[b, :, sl] = u.astype(BF16)
        u_copy(b, j).start()
        UF[b, :, sl] = u
        if j == len(s_pieces) - 1:
            pl.when(last)(lambda: uf_copy(b).start())
        d_copy(b, j).wait_send()
        y_copy(par, b, j).wait_send()

    def t0(b, par, last):
        for j in range(len(s_pieces)):
            u_copy(b, j).wait()

    def ta(q, b, par, last):
        o0, width = spans(TA_PIECES)[q]
        for o, w in tiles(width):
            o += o0
            TP[b, :, o:o + w] = dot_nn(UB[b, :, at(own0, half)], K[at(own0, half), o:o + w])

    def t1(b, par, last):
        def products(send):
            for c, (o0, width) in enumerate(t_pieces):
                for o, w in tiles(width):
                    o += o0
                    TP[b, :, o:o + w] += dot_nn(UB[b, :, at(sib0, half)], K[at(sib0, half), o:o + w])
                if send:
                    e_copy(b, c).start()

        pl.when(edge)(lambda: products(True))
        pl.when(inner)(lambda: products(False))

    def t2(c, b, par, last):
        o, w = t_pieces[c]

        @pl.when(inner)
        def _():
            e_copy(b, c).wait_recv()
            TP[b, :, o:o + w] = TP[b, :, o:o + w] + EI[b, :, o:o + w]
            x_copy(par, b, c).start()

    def t3i(c, b, par, last):
        o, w = t_pieces[c]

        @pl.when(inner)
        def _():
            x_copy(par, b, c).wait_recv()
            v = B[b, :, o:o + w] / (TP[b, :, o:o + w] + XR[par, b, :, o:o + w])
            VB[b, :, o:o + w] = v.astype(BF16)
            v_copy(b, c).start()
            VF[b, :, o:o + w] = v
            pl.when(last)(lambda: vf_copy(b, c).start())
            x_copy(par, b, c).wait_send()

    def t3e(c, b, par, last):
        @pl.when(edge)
        def _():
            v_copy(b, c).wait_recv()
            e_copy(b, c).wait_send()

    def cost_early(b):
        for o, w in tiles(n):
            WP[:, o:o + w] = dot_nn(VB[b, :, :early], KCT[:early, o:o + w])

    def cost_part(b):
        v_drain(b)
        uf_copy(b).wait()
        acc = jnp.zeros((m, 128), F32)
        for o, w in tiles(n):
            p = UF[b, :, o:o + w] * (WP[:, o:o + w] + dot_nn(VB[b, :, early:], KCT[early:, o:o + w]))
            for q in range(0, w, 128):
                acc = acc + p[:, q:q + 128]
        ACC[pl.ds(pl.multiple_of(b * m, m), m), :] = acc
        for c in range(len(t_pieces)):
            pl.when(inner)(lambda c=c: vf_copy(b, c).wait_send())
            pl.when(edge)(lambda c=c: vf_copy(b, c).wait_recv())

    def kc(t):
        rows = at(t * 128, 128)

        def turn(q, carry):
            cols = at(q * 256, 256)
            KCT[cols, rows] = KT[cols, rows] * jnp.transpose(C[rows, cols])
            return carry

        lax.fori_loop(0, n // 256, turn, 0)

    def kt(t):
        rows = at(t * (n // 3), n // 3)

        def turn(q, carry):
            cols = at(q * 256, 256)
            KT[cols, rows] = jnp.transpose(K[rows, cols])
            return carry

        lax.fori_loop(0, n // 256, turn, 0)

    steps = {"sa": sa, "s1": s1, "s3": s3, "s4": s4, "ta": ta, "t0": t0, "t1": t1, "t2": t2, "t3": t3i, "e": t3e}

    def tick(i, carry):
        for name, piece, lag in ORDER:
            if name == "cost":
                g = i - lag
                pl.when(jnp.logical_and(g >= total_inst, g < total_inst + NB))(lambda: cost_part(g - total_inst))
            elif name == "ca":
                g = i - lag
                pl.when(jnp.logical_and(g >= total_inst, g < total_inst + NB))(lambda: cost_early(g - total_inst))
            elif name == "kt":
                pl.when(i < 4)(lambda: kt(i - 1))
            elif name == "kc":
                pl.when(i == KC_FIRST)(lambda: c_load.wait())
                pl.when(jnp.logical_and(i >= KC_FIRST, i < KC_FIRST + n // 128))(lambda: kc(i - KC_FIRST))
            else:
                g = i - lag
                fn = steps[name] if piece is None else functools.partial(steps[name], piece)

                @pl.when(jnp.logical_and(g >= (NB if name[0] == "s" or name == "t0" else 0), g < total_inst))
                def _():
                    sweep = lax.div(g, NB)
                    fn(lax.rem(g, NB), lax.rem(sweep, 2), sweep == SWEEPS - 1)
        return carry

    lax.fori_loop(1, total_inst + NB, tick, 0)

    tot = jnp.sum(jnp.transpose(ACC[...]), axis=0, keepdims=True)
    CPS[...] = jnp.broadcast_to(tot, CPS.shape)
    me = row * n_col + col
    cps = [rcopy(CPS, CPR.at[me], cp_sem.at[i], dev) for i, dev in enumerate(peers)]
    for cp in cps:
        cp.start()
    CPR[me] = CPS[...]
    for cp in cps:
        cp.wait()
    total = CPR[0]
    for i in range(1, n_row * n_col):
        total = total + CPR[i]
    cost_ref[...] = total[0:1, 0:cost_ref.shape[1]] / norm


def solution(mesh):
    n_row = mesh.shape["row"]
    n_col = mesh.shape["col"]

    def local_fn(kern, cost_mat, src_mass, tgt_mass):
        n = kern.shape[0]
        q = src_mass.shape[1]
        m = q // NB
        half = n // 2
        norm = float(n * n_row) * float(kern.shape[1] * n_col)
        dma = pltpu.SemaphoreType.DMA
        vmem = pltpu.VMEM
        any_spec = pl.BlockSpec(memory_space=pl.ANY)
        np_, ns = len(T_PIECES), len(S_PIECES)
        u, v, cost = pl.pallas_call(
            functools.partial(kernel, n_row, n_col, norm),
            out_shape=(vmem((NB, m, n), F32), vmem((NB, m, n), F32), vmem((1, q), F32)),
            in_specs=[any_spec] * 4,
            out_specs=(pl.BlockSpec(memory_space=vmem),) * 3,
            scratch_shapes=[
                vmem((n, n), BF16), vmem((n, n), BF16), vmem((n, n), BF16), vmem((n, n), BF16),
                vmem((NB, m, n), F32), vmem((NB, m, n), F32),
                vmem((NB, m, n), BF16), vmem((NB, m, n), BF16),
                vmem((m, n), F32),
                vmem((NB, m, half), F32), vmem((NB, m, half), F32),
                vmem((NB, m, half), F32), vmem((2, NB, m, half), F32),
                vmem((NB, m, n), F32), vmem((NB, m, n), F32),
                vmem((2, NB, m, n), F32),
                vmem((n_col, 1, n), F32),
                vmem((128, 128), F32), vmem((8, 128), F32), vmem((n_row * n_col, 8, 128), F32),
                dma((len(K_PIECES),)), dma((3,)), dma((n_col - 1, 2)),
                dma((NB, ns, 2)), dma((2, NB, ns, 2)), dma((NB, ns, 2)), dma((NB, 2)),
                dma((NB, np_, 2)), dma((2, NB, np_, 2)), dma((NB, np_, 2)), dma((NB, np_, 2)),
                dma((n_row * n_col - 1, 2)),
            ],
            compiler_params=pltpu.CompilerParams(collective_id=0, has_side_effects=True, vmem_limit_bytes=60 * 1024 * 1024),
        )(kern, cost_mat, src_mass.T.reshape(NB, m, n), tgt_mass.T.reshape(NB, m, n))
        return u.reshape(q, n).T, v.reshape(q, n).T, cost.reshape(q)

    return jax.shard_map(local_fn, mesh=mesh, in_specs=(P("row", "col"), P("row", "col"), P("row", "prob"), P("col", "prob")),
                         out_specs=(P("row", "prob"), P("col", "prob"), P("prob")), check_vma=False)
```

```python
import functools

import jax
import jax.numpy as jnp
from jax import lax
from jax.experimental import pallas as pl
from jax.experimental.pallas import tpu as pltpu
from jax.sharding import PartitionSpec as P

SWEEPS = 6
MESH = pl.DeviceIdType.MESH
F32 = jnp.float32
BF16 = jnp.bfloat16
NB = 4
T_PIECES = (512, 512, 512, 512, 256)
EARLY = ((0, 1, 2),)
TA_PIECES = (2304,)
S_PIECES = (512, 640)
K_PIECES = (768, 768, 512, 256)
KC_FIRST = 5
ORDER = (
    ("t3", 0, 3), ("s4", 0, 1), ("s4", 1, 1), ("s3", 0, 0), ("t3", 1, 3), ("ta", 0, 1), ("t2", 0, 2),
    ("t0", None, 1), ("t3", 2, 3), ("s3", 1, 0), ("t1", None, 1), ("t2", 1, 2), ("t3", 3, 3), ("kc", None, 0),
    ("e", 0, 3), ("e", 1, 3), ("e", 2, 3), ("t3", 4, 3), ("t2", 2, 2), ("kt", None, 0), ("sa", 0, -1),
    ("ca", None, -1), ("e", 3, 3), ("t2", 3, 2), ("e", 4, 3), ("s1", None, -1), ("cost", None, -1),
    ("t2", 4, 2),
)


def dot_nn(x, y):
    return jnp.dot(x, y, preferred_element_type=F32)


def dot_nt(x, y):
    return lax.dot_general(x, y, (((1,), (1,)), ((), ())), preferred_element_type=F32)


def spans(sizes):
    out, o = [], 0
    for w in sizes:
        out.append((o, w))
        o += w
    return out


def tiles(size, tile=256):
    return [(o, min(tile, size - o)) for o in range(0, size, tile)]


def kernel(n_row, n_col, norm,
           k_hbm, c_hbm, a_hbm, b_hbm, UF, VF, cost_ref,
           K, KT, C, KCT, A, B, UB, VB, WP, DS, DR, SP, YR, TP, EI, XR, RX, ACC, CPS, CPR,
           k_sem, in_sem, r_sem,
           d_sem, y_sem, u_sem, uf_sem, e_sem, x_sem, v_sem, vf_sem, cp_sem):
    row = lax.axis_index("row")
    col = lax.axis_index("col")
    core = lax.rem(col, 2)
    n = K.shape[0]
    half = n // 2
    m = UB.shape[1]
    total_inst = SWEEPS * NB
    sib = {"col": col + 1 - 2 * core}
    ypeer = {"col": lax.rem(col + 2, n_col)}
    inner = jnp.logical_or(row == 1, row == 2)
    edge = jnp.logical_not(inner)
    zpair = {"row": row + 1 - 2 * lax.rem(row, 2)}
    zmid = {"row": n_row - 1 - row}
    own0 = pl.multiple_of(core * half, 128)
    sib0 = pl.multiple_of((1 - core) * half, 128)
    t_pieces = spans(T_PIECES)
    s_pieces = spans(S_PIECES)

    def at(o, w):
        return pl.ds(pl.multiple_of(o, 128), w)

    def rcopy(src, dst, sem, dev):
        return pltpu.make_async_remote_copy(src_ref=src, dst_ref=dst, send_sem=sem.at[0], recv_sem=sem.at[1],
                                            device_id=dev, device_id_type=MESH)

    a_load = pltpu.make_async_copy(a_hbm, A, in_sem.at[0])
    b_load = pltpu.make_async_copy(b_hbm, B, in_sem.at[1])
    c_load = pltpu.make_async_copy(c_hbm, C, in_sem.at[2])
    k_loads = [pltpu.make_async_copy(k_hbm.at[o:o + w, :], K.at[o:o + w, :], k_sem.at[j])
               for j, (o, w) in enumerate(spans(K_PIECES))]
    for cp in k_loads:
        cp.start()
    a_load.start()

    barrier = pltpu.get_barrier_semaphore()
    rel = [(dr, dc) for dr in range(n_row) for dc in range(n_col) if (dr, dc) != (0, 0)]
    peers = [{"row": lax.rem(row + dr, n_row), "col": lax.rem(col + dc, n_col)} for dr, dc in rel]
    for dev in peers:
        pl.semaphore_signal(barrier, inc=1, device_id=dev, device_id_type=MESH)

    ACC[...] = jnp.zeros_like(ACC)

    ones = jnp.ones((16, n), BF16)
    for cp, (o, w) in zip(k_loads, spans(K_PIECES)):
        cp.wait()
        RX[col, :, o:o + w] = dot_nt(ones, K[o:o + w, :])[:1]
    pl.semaphore_wait(barrier, len(peers))
    r_copies = [rcopy(RX.at[col], RX.at[col], r_sem.at[d - 1], {"col": lax.rem(col + d, n_col)}) for d in range(1, n_col)]
    for cp in r_copies:
        cp.start()
    b_load.start()
    c_load.start()
    a_load.wait()
    for cp in r_copies:
        cp.wait()
    s0 = RX[0] + RX[1]
    for d in range(2, n_col):
        s0 = s0 + RX[d]
    for b in range(NB):
        UB[b] = (A[b] / s0).astype(BF16)
    b_load.wait()

    def u_copy(b, j):
        o, w = s_pieces[j]
        ref = UB.at[b, :, at(own0 + o, w)]
        return rcopy(ref, ref, u_sem.at[b, j], sib)

    def uf_copy(b):
        ref = UF.at[b, :, at(own0, half)]
        return rcopy(ref, ref, uf_sem.at[b], sib)

    def d_copy(b, j):
        o, w = s_pieces[j]
        return rcopy(DS.at[b, :, pl.ds(o, w)], DR.at[b, :, pl.ds(o, w)], d_sem.at[b, j], sib)

    def y_copy(par, b, j):
        o, w = s_pieces[j]
        return rcopy(SP.at[b, :, pl.ds(o, w)], YR.at[par, b, :, pl.ds(o, w)], y_sem.at[par, b, j], ypeer)

    def e_copy(b, c):
        o, w = t_pieces[c]
        return rcopy(TP.at[b, :, pl.ds(o, w)], EI.at[b, :, pl.ds(o, w)], e_sem.at[b, c], zpair)

    def x_copy(par, b, c):
        o, w = t_pieces[c]
        return rcopy(TP.at[b, :, pl.ds(o, w)], XR.at[par, b, :, pl.ds(o, w)], x_sem.at[par, b, c], zmid)

    def v_copy(b, c):
        o, w = t_pieces[c]
        ref = VB.at[b, :, pl.ds(o, w)]
        return rcopy(ref, ref, v_sem.at[b, c], zpair)

    def vf_copy(b, c):
        o, w = t_pieces[c]
        ref = VF.at[b, :, pl.ds(o, w)]
        return rcopy(ref, ref, vf_sem.at[b, c], zpair)

    early_spans = spans([sum(T_PIECES[c] for c in group) for group in EARLY])
    early = sum(w for _, w in early_spans)

    def s_drain(b, par):
        for j in range(len(s_pieces)):
            d_copy(b, j).wait_send()
            y_copy(par, b, j).wait_send()

    def t_drain(b, par):
        @pl.when(inner)
        def _():
            for c in range(len(t_pieces)):
                x_copy(par, b, c).wait_send()

        @pl.when(edge)
        def _():
            for c in range(len(t_pieces)):
                e_copy(b, c).wait_send()

    def sa(q, b, par, sweep):
        if q == 0:
            pl.when(sweep > 1)(lambda: s_drain(b, 1 - par))
        k0, kw = early_spans[q]
        for dst, h0 in ((DS, sib0), (SP, own0)):
            for o, w in tiles(half):
                part = dot_nn(VB[b, :, k0:k0 + kw], KT[k0:k0 + kw, at(h0 + o, w)])
                dst[b, :, o:o + w] = part if q == 0 else dst[b, :, o:o + w] + part

    def s1(b, par, sweep):
        for j, (o0, width) in enumerate(s_pieces):
            for o, w in tiles(width):
                o += o0
                DS[b, :, o:o + w] += dot_nn(VB[b, :, early:], KT[early:, at(sib0 + o, w)])
            d_copy(b, j).start()
        for o, w in tiles(half):
            SP[b, :, o:o + w] += dot_nn(VB[b, :, early:], KT[early:, at(own0 + o, w)])

    def v_drain(b):
        @pl.when(inner)
        def _():
            for c in range(len(t_pieces)):
                v_copy(b, c).wait_send()

    def s3(j, b, par, sweep):
        o, w = s_pieces[j]
        d_copy(b, j).wait_recv()
        SP[b, :, o:o + w] = SP[b, :, o:o + w] + DR[b, :, o:o + w]
        y_copy(par, b, j).start()
        if j == len(s_pieces) - 1:
            v_drain(b)

    def s4(j, b, par, sweep):
        o, w = s_pieces[j]
        y_copy(par, b, j).wait_recv()
        sl = at(own0 + o, w)
        u = A[b, :, sl] / (SP[b, :, o:o + w] + YR[par, b, :, o:o + w])
        UB[b, :, sl] = u.astype(BF16)
        u_copy(b, j).start()
        UF[b, :, sl] = u
        if j == len(s_pieces) - 1:
            pl.when(sweep == SWEEPS - 1)(lambda: uf_copy(b).start())

    def t0(b, par, sweep):
        for j in range(len(s_pieces)):
            u_copy(b, j).wait()

    def ta(q, b, par, sweep):
        if q == 0:
            pl.when(sweep > 0)(lambda: t_drain(b, 1 - par))
        o0, width = spans(TA_PIECES)[q]
        for o, w in tiles(width):
            o += o0
            TP[b, :, o:o + w] = dot_nn(UB[b, :, at(own0, half)], K[at(own0, half), o:o + w])

    def t1(b, par, sweep):
        def products(send):
            for c, (o0, width) in enumerate(t_pieces):
                for o, w in tiles(width):
                    o += o0
                    TP[b, :, o:o + w] += dot_nn(UB[b, :, at(sib0, half)], K[at(sib0, half), o:o + w])
                if send:
                    e_copy(b, c).start()

        pl.when(edge)(lambda: products(True))
        pl.when(inner)(lambda: products(False))

    def t2(c, b, par, sweep):
        o, w = t_pieces[c]

        @pl.when(inner)
        def _():
            e_copy(b, c).wait_recv()
            TP[b, :, o:o + w] = TP[b, :, o:o + w] + EI[b, :, o:o + w]
            x_copy(par, b, c).start()

    def t3i(c, b, par, sweep):
        o, w = t_pieces[c]

        @pl.when(inner)
        def _():
            x_copy(par, b, c).wait_recv()
            v = B[b, :, o:o + w] / (TP[b, :, o:o + w] + XR[par, b, :, o:o + w])
            VB[b, :, o:o + w] = v.astype(BF16)
            v_copy(b, c).start()
            VF[b, :, o:o + w] = v
            pl.when(sweep == SWEEPS - 1)(lambda: vf_copy(b, c).start())

    def t3e(c, b, par, sweep):
        @pl.when(edge)
        def _():
            v_copy(b, c).wait_recv()

    def cost_early(b):
        for o, w in tiles(n):
            WP[:, o:o + w] = dot_nn(VB[b, :, :early], KCT[:early, o:o + w])

    def cost_part(b):
        v_drain(b)
        s_drain(b, (SWEEPS - 1) % 2)
        t_drain(b, (SWEEPS - 1) % 2)
        uf_copy(b).wait()
        acc = jnp.zeros((m, 128), F32)
        for o, w in tiles(n):
            p = UF[b, :, o:o + w] * (WP[:, o:o + w] + dot_nn(VB[b, :, early:], KCT[early:, o:o + w]))
            for q in range(0, w, 128):
                acc = acc + p[:, q:q + 128]
        ACC[pl.ds(pl.multiple_of(b * m, m), m), :] = acc
        for c in range(len(t_pieces)):
            pl.when(inner)(lambda c=c: vf_copy(b, c).wait_send())
            pl.when(edge)(lambda c=c: vf_copy(b, c).wait_recv())

    def kc(t):
        rows = at(t * 128, 128)

        def turn(q, carry):
            cols = at(q * 256, 256)
            KCT[cols, rows] = KT[cols, rows] * jnp.transpose(C[rows, cols])
            return carry

        lax.fori_loop(0, n // 256, turn, 0)

    def kt(t):
        rows = at(t * (n // 3), n // 3)

        def turn(q, carry):
            cols = at(q * 256, 256)
            KT[cols, rows] = jnp.transpose(K[rows, cols])
            return carry

        lax.fori_loop(0, n // 256, turn, 0)

    steps = {"sa": sa, "s1": s1, "s3": s3, "s4": s4, "ta": ta, "t0": t0, "t1": t1, "t2": t2, "t3": t3i, "e": t3e}

    def tick(i, carry):
        for name, piece, lag in ORDER:
            if name == "cost":
                g = i - lag
                pl.when(jnp.logical_and(g >= total_inst, g < total_inst + NB))(lambda: cost_part(g - total_inst))
            elif name == "ca":
                g = i - lag
                pl.when(jnp.logical_and(g >= total_inst, g < total_inst + NB))(lambda: cost_early(g - total_inst))
            elif name == "kt":
                pl.when(i < 4)(lambda: kt(i - 1))
            elif name == "kc":
                pl.when(i == KC_FIRST)(lambda: c_load.wait())
                pl.when(jnp.logical_and(i >= KC_FIRST, i < KC_FIRST + n // 128))(lambda: kc(i - KC_FIRST))
            else:
                g = i - lag
                fn = steps[name] if piece is None else functools.partial(steps[name], piece)

                @pl.when(jnp.logical_and(g >= (NB if name[0] == "s" or name == "t0" else 0), g < total_inst))
                def _():
                    sweep = lax.div(g, NB)
                    fn(lax.rem(g, NB), lax.rem(sweep, 2), sweep)
        return carry

    lax.fori_loop(1, total_inst + NB, tick, 0)

    tot = jnp.sum(jnp.transpose(ACC[...]), axis=0, keepdims=True)
    CPS[...] = jnp.broadcast_to(tot, CPS.shape)
    me = row * n_col + col
    cps = [rcopy(CPS, CPR.at[me], cp_sem.at[i], dev) for i, dev in enumerate(peers)]
    for cp in cps:
        cp.start()
    CPR[me] = CPS[...]
    for cp in cps:
        cp.wait()
    total = CPR[0]
    for i in range(1, n_row * n_col):
        total = total + CPR[i]
    cost_ref[...] = total[0:1, 0:cost_ref.shape[1]] / norm


def solution(mesh):
    n_row = mesh.shape["row"]
    n_col = mesh.shape["col"]

    def local_fn(kern, cost_mat, src_mass, tgt_mass):
        n = kern.shape[0]
        q = src_mass.shape[1]
        m = q // NB
        half = n // 2
        norm = float(n * n_row) * float(kern.shape[1] * n_col)
        dma = pltpu.SemaphoreType.DMA
        vmem = pltpu.VMEM
        any_spec = pl.BlockSpec(memory_space=pl.ANY)
        np_, ns = len(T_PIECES), len(S_PIECES)
        u, v, cost = pl.pallas_call(
            functools.partial(kernel, n_row, n_col, norm),
            out_shape=(vmem((NB, m, n), F32), vmem((NB, m, n), F32), vmem((1, q), F32)),
            in_specs=[any_spec] * 4,
            out_specs=(pl.BlockSpec(memory_space=vmem),) * 3,
            scratch_shapes=[
                vmem((n, n), BF16), vmem((n, n), BF16), vmem((n, n), BF16), vmem((n, n), BF16),
                vmem((NB, m, n), F32), vmem((NB, m, n), F32),
                vmem((NB, m, n), BF16), vmem((NB, m, n), BF16),
                vmem((m, n), F32),
                vmem((NB, m, half), F32), vmem((NB, m, half), F32),
                vmem((NB, m, half), F32), vmem((2, NB, m, half), F32),
                vmem((NB, m, n), F32), vmem((NB, m, n), F32),
                vmem((2, NB, m, n), F32),
                vmem((n_col, 1, n), F32),
                vmem((128, 128), F32), vmem((8, 128), F32), vmem((n_row * n_col, 8, 128), F32),
                dma((len(K_PIECES),)), dma((3,)), dma((n_col - 1, 2)),
                dma((NB, ns, 2)), dma((2, NB, ns, 2)), dma((NB, ns, 2)), dma((NB, 2)),
                dma((NB, np_, 2)), dma((2, NB, np_, 2)), dma((NB, np_, 2)), dma((NB, np_, 2)),
                dma((n_row * n_col - 1, 2)),
            ],
            compiler_params=pltpu.CompilerParams(collective_id=0, has_side_effects=True, vmem_limit_bytes=60 * 1024 * 1024),
        )(kern, cost_mat, src_mass.T.reshape(NB, m, n), tgt_mass.T.reshape(NB, m, n))
        return u.reshape(q, n).T, v.reshape(q, n).T, cost.reshape(q)

    return jax.shard_map(local_fn, mesh=mesh, in_specs=(P("row", "col"), P("row", "col"), P("row", "prob"), P("col", "prob")),
                         out_specs=(P("row", "prob"), P("col", "prob"), P("prob")), check_vma=False)
```

```python
import functools

import jax
import jax.numpy as jnp
from jax import lax
from jax.experimental import pallas as pl
from jax.experimental.pallas import tpu as pltpu
from jax.sharding import PartitionSpec as P

SWEEPS = 6
MESH = pl.DeviceIdType.MESH
F32 = jnp.float32
BF16 = jnp.bfloat16
NB = 4
T_PIECES = (512, 512, 512, 512, 256)
EARLY = ((0, 1, 2),)
TA_PIECES = (2304,)
S_PIECES = (512, 640)
K_PIECES = (768, 768, 512, 256)
KC_FIRST = 5
ORDER = (
    ("e", 0, 4), ("t2", 3, 3), ("e", 1, 4), ("e", 2, 4), ("kt", None, 0), ("sa", 0, 0), ("ca", None, 0),
    ("s4", 0, 1), ("e", 3, 4), ("t2", 4, 3), ("e", 4, 4), ("s1", None, 0), ("cost", None, 0), ("t3", 0, 3),
    ("s4", 1, 1), ("ta", 0, 1), ("s3", 0, 0), ("t3", 1, 3), ("t2", 0, 2), ("s3", 1, 0), ("t0", None, 1),
    ("t3", 2, 3), ("t1", None, 1), ("t2", 1, 2), ("t3", 3, 3), ("t2", 2, 2), ("t3", 4, 3), ("kc", None, 0),
)


def dot_nn(x, y):
    return jnp.dot(x, y, preferred_element_type=F32)


def dot_nt(x, y):
    return lax.dot_general(x, y, (((1,), (1,)), ((), ())), preferred_element_type=F32)


def spans(sizes):
    out, o = [], 0
    for w in sizes:
        out.append((o, w))
        o += w
    return out


def tiles(size, tile=256):
    return [(o, min(tile, size - o)) for o in range(0, size, tile)]


def kernel(n_row, n_col, norm,
           k_hbm, c_hbm, a_hbm, b_hbm, UF, VF, cost_ref,
           K, KT, C, KCT, A, B, UB, VB, WP, DS, DR, SP, YR, TP, EI, XR, RX, ACC, CPS, CPR,
           k_sem, in_sem, r_sem,
           d_sem, y_sem, u_sem, uf_sem, e_sem, x_sem, v_sem, vf_sem, cp_sem):
    row = lax.axis_index("row")
    col = lax.axis_index("col")
    core = lax.rem(col, 2)
    n = K.shape[0]
    half = n // 2
    m = UB.shape[1]
    total_inst = SWEEPS * NB
    sib = {"col": col + 1 - 2 * core}
    ypeer = {"col": lax.rem(col + 2, n_col)}
    inner = jnp.logical_or(row == 1, row == 2)
    edge = jnp.logical_not(inner)
    zpair = {"row": row + 1 - 2 * lax.rem(row, 2)}
    zmid = {"row": n_row - 1 - row}
    own0 = pl.multiple_of(core * half, 128)
    sib0 = pl.multiple_of((1 - core) * half, 128)
    t_pieces = spans(T_PIECES)
    s_pieces = spans(S_PIECES)

    def at(o, w):
        return pl.ds(pl.multiple_of(o, 128), w)

    def rcopy(src, dst, sem, dev):
        return pltpu.make_async_remote_copy(src_ref=src, dst_ref=dst, send_sem=sem.at[0], recv_sem=sem.at[1],
                                            device_id=dev, device_id_type=MESH)

    a_load = pltpu.make_async_copy(a_hbm, A, in_sem.at[0])
    b_load = pltpu.make_async_copy(b_hbm, B, in_sem.at[1])
    c_load = pltpu.make_async_copy(c_hbm, C, in_sem.at[2])
    k_loads = [pltpu.make_async_copy(k_hbm.at[o:o + w, :], K.at[o:o + w, :], k_sem.at[j])
               for j, (o, w) in enumerate(spans(K_PIECES))]
    for cp in k_loads:
        cp.start()
    a_load.start()

    barrier = pltpu.get_barrier_semaphore()
    rel = [(dr, dc) for dr in range(n_row) for dc in range(n_col) if (dr, dc) != (0, 0)]
    peers = [{"row": lax.rem(row + dr, n_row), "col": lax.rem(col + dc, n_col)} for dr, dc in rel]
    for dev in peers:
        pl.semaphore_signal(barrier, inc=1, device_id=dev, device_id_type=MESH)

    ACC[...] = jnp.zeros_like(ACC)

    ones = jnp.ones((16, n), BF16)
    for cp, (o, w) in zip(k_loads, spans(K_PIECES)):
        cp.wait()
        RX[col, :, o:o + w] = dot_nt(ones, K[o:o + w, :])[:1]
    pl.semaphore_wait(barrier, len(peers))
    r_copies = [rcopy(RX.at[col], RX.at[col], r_sem.at[d - 1], {"col": lax.rem(col + d, n_col)}) for d in range(1, n_col)]
    for cp in r_copies:
        cp.start()
    b_load.start()
    c_load.start()
    a_load.wait()
    for cp in r_copies:
        cp.wait()
    s0 = RX[0] + RX[1]
    for d in range(2, n_col):
        s0 = s0 + RX[d]
    for b in range(NB):
        UB[b] = (A[b] / s0).astype(BF16)
    b_load.wait()

    def u_copy(b, j):
        o, w = s_pieces[j]
        ref = UB.at[b, :, at(own0 + o, w)]
        return rcopy(ref, ref, u_sem.at[b, j], sib)

    def uf_copy(b):
        ref = UF.at[b, :, at(own0, half)]
        return rcopy(ref, ref, uf_sem.at[b], sib)

    def d_copy(b, j):
        o, w = s_pieces[j]
        return rcopy(DS.at[b, :, pl.ds(o, w)], DR.at[b, :, pl.ds(o, w)], d_sem.at[b, j], sib)

    def y_copy(par, b, j):
        o, w = s_pieces[j]
        return rcopy(SP.at[b, :, pl.ds(o, w)], YR.at[par, b, :, pl.ds(o, w)], y_sem.at[par, b, j], ypeer)

    def e_copy(b, c):
        o, w = t_pieces[c]
        return rcopy(TP.at[b, :, pl.ds(o, w)], EI.at[b, :, pl.ds(o, w)], e_sem.at[b, c], zpair)

    def x_copy(par, b, c):
        o, w = t_pieces[c]
        return rcopy(TP.at[b, :, pl.ds(o, w)], XR.at[par, b, :, pl.ds(o, w)], x_sem.at[par, b, c], zmid)

    def v_copy(b, c):
        o, w = t_pieces[c]
        ref = VB.at[b, :, pl.ds(o, w)]
        return rcopy(ref, ref, v_sem.at[b, c], zpair)

    def vf_copy(b, c):
        o, w = t_pieces[c]
        ref = VF.at[b, :, pl.ds(o, w)]
        return rcopy(ref, ref, vf_sem.at[b, c], zpair)

    early_spans = spans([sum(T_PIECES[c] for c in group) for group in EARLY])
    early = sum(w for _, w in early_spans)

    def s_drain(b, par):
        for j in range(len(s_pieces)):
            d_copy(b, j).wait_send()
            y_copy(par, b, j).wait_send()

    def t_drain(b, par):
        @pl.when(inner)
        def _():
            for c in range(len(t_pieces)):
                x_copy(par, b, c).wait_send()

        @pl.when(edge)
        def _():
            for c in range(len(t_pieces)):
                e_copy(b, c).wait_send()

    def sa(q, b, par, sweep):
        if q == 0:
            pl.when(sweep > 1)(lambda: s_drain(b, 1 - par))
        k0, kw = early_spans[q]
        for dst, h0 in ((DS, sib0), (SP, own0)):
            for o, w in tiles(half):
                part = dot_nn(VB[b, :, k0:k0 + kw], KT[k0:k0 + kw, at(h0 + o, w)])
                dst[b, :, o:o + w] = part if q == 0 else dst[b, :, o:o + w] + part

    def s1(b, par, sweep):
        for j, (o0, width) in enumerate(s_pieces):
            for o, w in tiles(width):
                o += o0
                DS[b, :, o:o + w] += dot_nn(VB[b, :, early:], KT[early:, at(sib0 + o, w)])
            d_copy(b, j).start()
        for o, w in tiles(half):
            SP[b, :, o:o + w] += dot_nn(VB[b, :, early:], KT[early:, at(own0 + o, w)])

    def v_drain(b):
        @pl.when(inner)
        def _():
            for c in range(len(t_pieces)):
                v_copy(b, c).wait_send()

    def s3(j, b, par, sweep):
        o, w = s_pieces[j]
        d_copy(b, j).wait_recv()
        SP[b, :, o:o + w] = SP[b, :, o:o + w] + DR[b, :, o:o + w]
        y_copy(par, b, j).start()
        if j == len(s_pieces) - 1:
            v_drain(b)

    def s4(j, b, par, sweep):
        o, w = s_pieces[j]
        y_copy(par, b, j).wait_recv()
        sl = at(own0 + o, w)
        u = A[b, :, sl] / (SP[b, :, o:o + w] + YR[par, b, :, o:o + w])
        UB[b, :, sl] = u.astype(BF16)
        u_copy(b, j).start()
        UF[b, :, sl] = u
        if j == len(s_pieces) - 1:
            pl.when(sweep == SWEEPS - 1)(lambda: uf_copy(b).start())

    def t0(b, par, sweep):
        for j in range(len(s_pieces)):
            u_copy(b, j).wait()

    def ta(q, b, par, sweep):
        if q == 0:
            pl.when(sweep > 0)(lambda: t_drain(b, 1 - par))
        o0, width = spans(TA_PIECES)[q]
        for o, w in tiles(width):
            o += o0
            TP[b, :, o:o + w] = dot_nn(UB[b, :, at(own0, half)], K[at(own0, half), o:o + w])

    def t1(b, par, sweep):
        def products(send):
            for c, (o0, width) in enumerate(t_pieces):
                for o, w in tiles(width):
                    o += o0
                    TP[b, :, o:o + w] += dot_nn(UB[b, :, at(sib0, half)], K[at(sib0, half), o:o + w])
                if send:
                    e_copy(b, c).start()

        pl.when(edge)(lambda: products(True))
        pl.when(inner)(lambda: products(False))

    def t2(c, b, par, sweep):
        o, w = t_pieces[c]

        @pl.when(inner)
        def _():
            e_copy(b, c).wait_recv()
            TP[b, :, o:o + w] = TP[b, :, o:o + w] + EI[b, :, o:o + w]
            x_copy(par, b, c).start()

    def t3i(c, b, par, sweep):
        o, w = t_pieces[c]

        @pl.when(inner)
        def _():
            x_copy(par, b, c).wait_recv()
            v = B[b, :, o:o + w] / (TP[b, :, o:o + w] + XR[par, b, :, o:o + w])
            VB[b, :, o:o + w] = v.astype(BF16)
            v_copy(b, c).start()
            VF[b, :, o:o + w] = v
            pl.when(sweep == SWEEPS - 1)(lambda: vf_copy(b, c).start())

    def t3e(c, b, par, sweep):
        @pl.when(edge)
        def _():
            v_copy(b, c).wait_recv()

    def cost_early(b):
        for o, w in tiles(n):
            WP[:, o:o + w] = dot_nn(VB[b, :, :early], KCT[:early, o:o + w])

    def cost_part(b):
        v_drain(b)
        s_drain(b, (SWEEPS - 1) % 2)
        t_drain(b, (SWEEPS - 1) % 2)
        uf_copy(b).wait()
        acc = jnp.zeros((m, 128), F32)
        for o, w in tiles(n):
            p = UF[b, :, o:o + w] * (WP[:, o:o + w] + dot_nn(VB[b, :, early:], KCT[early:, o:o + w]))
            for q in range(0, w, 128):
                acc = acc + p[:, q:q + 128]
        ACC[pl.ds(pl.multiple_of(b * m, m), m), :] = acc
        for c in range(len(t_pieces)):
            pl.when(inner)(lambda c=c: vf_copy(b, c).wait_send())
            pl.when(edge)(lambda c=c: vf_copy(b, c).wait_recv())

    def kc(t):
        rows = at(t * 128, 128)

        def turn(q, carry):
            cols = at(q * 256, 256)
            KCT[cols, rows] = KT[cols, rows] * jnp.transpose(C[rows, cols])
            return carry

        lax.fori_loop(0, n // 256, turn, 0)

    def kt(t):
        rows = at(t * (n // 3), n // 3)

        def turn(q, carry):
            cols = at(q * 256, 256)
            KT[cols, rows] = jnp.transpose(K[rows, cols])
            return carry

        lax.fori_loop(0, n // 256, turn, 0)

    steps = {"sa": sa, "s1": s1, "s3": s3, "s4": s4, "ta": ta, "t0": t0, "t1": t1, "t2": t2, "t3": t3i, "e": t3e}

    def tick(i, carry):
        for name, piece, lag in ORDER:
            if name == "cost":
                g = i - lag
                pl.when(jnp.logical_and(g >= total_inst, g < total_inst + NB))(lambda: cost_part(g - total_inst))
            elif name == "ca":
                g = i - lag
                pl.when(jnp.logical_and(g >= total_inst, g < total_inst + NB))(lambda: cost_early(g - total_inst))
            elif name == "kt":
                pl.when(i < 4)(lambda: kt(i - 1))
            elif name == "kc":
                pl.when(i == KC_FIRST)(lambda: c_load.wait())
                pl.when(jnp.logical_and(i >= KC_FIRST, i < KC_FIRST + n // 128))(lambda: kc(i - KC_FIRST))
            else:
                g = i - lag
                fn = steps[name] if piece is None else functools.partial(steps[name], piece)

                @pl.when(jnp.logical_and(g >= (NB if name[0] == "s" or name == "t0" else 0), g < total_inst))
                def _():
                    sweep = lax.div(g, NB)
                    fn(lax.rem(g, NB), lax.rem(sweep, 2), sweep)
        return carry

    lax.fori_loop(1, total_inst + NB, tick, 0)

    tot = jnp.sum(jnp.transpose(ACC[...]), axis=0, keepdims=True)
    CPS[...] = jnp.broadcast_to(tot, CPS.shape)
    me = row * n_col + col
    cps = [rcopy(CPS, CPR.at[me], cp_sem.at[i], dev) for i, dev in enumerate(peers)]
    for cp in cps:
        cp.start()
    CPR[me] = CPS[...]
    for cp in cps:
        cp.wait()
    total = CPR[0]
    for i in range(1, n_row * n_col):
        total = total + CPR[i]
    cost_ref[...] = total[0:1, 0:cost_ref.shape[1]] / norm


def solution(mesh):
    n_row = mesh.shape["row"]
    n_col = mesh.shape["col"]

    def local_fn(kern, cost_mat, src_mass, tgt_mass):
        n = kern.shape[0]
        q = src_mass.shape[1]
        m = q // NB
        half = n // 2
        norm = float(n * n_row) * float(kern.shape[1] * n_col)
        dma = pltpu.SemaphoreType.DMA
        vmem = pltpu.VMEM
        any_spec = pl.BlockSpec(memory_space=pl.ANY)
        np_, ns = len(T_PIECES), len(S_PIECES)
        u, v, cost = pl.pallas_call(
            functools.partial(kernel, n_row, n_col, norm),
            out_shape=(vmem((NB, m, n), F32), vmem((NB, m, n), F32), vmem((1, q), F32)),
            in_specs=[any_spec] * 4,
            out_specs=(pl.BlockSpec(memory_space=vmem),) * 3,
            scratch_shapes=[
                vmem((n, n), BF16), vmem((n, n), BF16), vmem((n, n), BF16), vmem((n, n), BF16),
                vmem((NB, m, n), F32), vmem((NB, m, n), F32),
                vmem((NB, m, n), BF16), vmem((NB, m, n), BF16),
                vmem((m, n), F32),
                vmem((NB, m, half), F32), vmem((NB, m, half), F32),
                vmem((NB, m, half), F32), vmem((2, NB, m, half), F32),
                vmem((NB, m, n), F32), vmem((NB, m, n), F32),
                vmem((2, NB, m, n), F32),
                vmem((n_col, 1, n), F32),
                vmem((128, 128), F32), vmem((8, 128), F32), vmem((n_row * n_col, 8, 128), F32),
                dma((len(K_PIECES),)), dma((3,)), dma((n_col - 1, 2)),
                dma((NB, ns, 2)), dma((2, NB, ns, 2)), dma((NB, ns, 2)), dma((NB, 2)),
                dma((NB, np_, 2)), dma((2, NB, np_, 2)), dma((NB, np_, 2)), dma((NB, np_, 2)),
                dma((n_row * n_col - 1, 2)),
            ],
            compiler_params=pltpu.CompilerParams(collective_id=0, has_side_effects=True, vmem_limit_bytes=60 * 1024 * 1024),
        )(kern, cost_mat, src_mass.T.reshape(NB, m, n), tgt_mass.T.reshape(NB, m, n))
        return u.reshape(q, n).T, v.reshape(q, n).T, cost.reshape(q)

    return jax.shard_map(local_fn, mesh=mesh, in_specs=(P("row", "col"), P("row", "col"), P("row", "prob"), P("col", "prob")),
                         out_specs=(P("row", "prob"), P("col", "prob"), P("prob")), check_vma=False)
```

```python
import functools

import jax
import jax.numpy as jnp
from jax import lax
from jax.experimental import pallas as pl
from jax.experimental.pallas import tpu as pltpu
from jax.sharding import PartitionSpec as P

SWEEPS = 6
MESH = pl.DeviceIdType.MESH
F32 = jnp.float32
BF16 = jnp.bfloat16
NB = 4
T_PIECES = (512, 512, 512, 512, 256)
EARLY = ((0, 1, 2),)
TA_PIECES = (2304,)
S_PIECES = (512, 640)
K_PIECES = (768, 768, 512, 256)
KC_FIRST = 5
ORDER = (
    ("e", 1, 4), ("e", 2, 4), ("sa", 0, 0), ("ca", None, 0), ("e", 3, 4), ("t3", 0, 3), ("s4", 0, 1),
    ("e", 4, 4), ("s1", None, 0), ("cost", None, 0), ("t3", 1, 3), ("s4", 1, 1), ("ta", 0, 1), ("s3", 0, 0),
    ("t2", 0, 2), ("s3", 1, 0), ("t3", 2, 3), ("t2", 1, 2), ("t0", None, 1), ("t1", None, 1), ("t3", 3, 3),
    ("t2", 2, 2), ("t3", 4, 3), ("e", 0, 3), ("kc", None, 0), ("t2", 3, 2), ("t2", 4, 2), ("kt", None, 0),
)


def dot_nn(x, y):
    return jnp.dot(x, y, preferred_element_type=F32)


def dot_nt(x, y):
    return lax.dot_general(x, y, (((1,), (1,)), ((), ())), preferred_element_type=F32)


def spans(sizes):
    out, o = [], 0
    for w in sizes:
        out.append((o, w))
        o += w
    return out


def tiles(size, tile=256):
    return [(o, min(tile, size - o)) for o in range(0, size, tile)]


def kernel(n_row, n_col, norm,
           k_hbm, c_hbm, a_hbm, b_hbm, UF, VF, cost_ref,
           K, KT, C, KCT, A, B, UB, VB, WP, DS, DR, SP, YR, TP, EI, XR, RX, ACC, CPS, CPR,
           k_sem, in_sem, r_sem,
           d_sem, y_sem, u_sem, uf_sem, e_sem, x_sem, v_sem, vf_sem, cp_sem):
    row = lax.axis_index("row")
    col = lax.axis_index("col")
    core = lax.rem(col, 2)
    n = K.shape[0]
    half = n // 2
    m = UB.shape[1]
    total_inst = SWEEPS * NB
    sib = {"col": col + 1 - 2 * core}
    ypeer = {"col": lax.rem(col + 2, n_col)}
    inner = jnp.logical_or(row == 1, row == 2)
    edge = jnp.logical_not(inner)
    zpair = {"row": row + 1 - 2 * lax.rem(row, 2)}
    zmid = {"row": n_row - 1 - row}
    own0 = pl.multiple_of(core * half, 128)
    sib0 = pl.multiple_of((1 - core) * half, 128)
    t_pieces = spans(T_PIECES)
    s_pieces = spans(S_PIECES)

    def at(o, w):
        return pl.ds(pl.multiple_of(o, 128), w)

    def rcopy(src, dst, sem, dev):
        return pltpu.make_async_remote_copy(src_ref=src, dst_ref=dst, send_sem=sem.at[0], recv_sem=sem.at[1],
                                            device_id=dev, device_id_type=MESH)

    a_load = pltpu.make_async_copy(a_hbm, A, in_sem.at[0])
    b_load = pltpu.make_async_copy(b_hbm, B, in_sem.at[1])
    c_load = pltpu.make_async_copy(c_hbm, C, in_sem.at[2])
    k_loads = [pltpu.make_async_copy(k_hbm.at[o:o + w, :], K.at[o:o + w, :], k_sem.at[j])
               for j, (o, w) in enumerate(spans(K_PIECES))]
    for cp in k_loads:
        cp.start()
    a_load.start()

    barrier = pltpu.get_barrier_semaphore()
    rel = [(dr, dc) for dr in range(n_row) for dc in range(n_col) if (dr, dc) != (0, 0)]
    peers = [{"row": lax.rem(row + dr, n_row), "col": lax.rem(col + dc, n_col)} for dr, dc in rel]
    for dev in peers:
        pl.semaphore_signal(barrier, inc=1, device_id=dev, device_id_type=MESH)

    ACC[...] = jnp.zeros_like(ACC)

    def kt(t):
        rows = at(t * (n // 3), n // 3)

        def turn(q, carry):
            cols = at(q * 256, 256)
            KT[cols, rows] = jnp.transpose(K[rows, cols])
            return carry

        lax.fori_loop(0, n // 256, turn, 0)

    ones = jnp.ones((16, n), BF16)
    for cp, (o, w) in zip(k_loads, spans(K_PIECES)):
        cp.wait()
        RX[col, :, o:o + w] = dot_nt(ones, K[o:o + w, :])[:1]
    pl.semaphore_wait(barrier, len(peers))
    r_copies = [rcopy(RX.at[col], RX.at[col], r_sem.at[d - 1], {"col": lax.rem(col + d, n_col)}) for d in range(1, n_col)]
    for cp in r_copies:
        cp.start()
    b_load.start()
    c_load.start()
    a_load.wait()
    kt(0)
    for cp in r_copies:
        cp.wait()
    s0 = RX[0] + RX[1]
    for d in range(2, n_col):
        s0 = s0 + RX[d]
    for b in range(NB):
        UB[b] = (A[b] / s0).astype(BF16)
    b_load.wait()

    def u_copy(b, j):
        o, w = s_pieces[j]
        ref = UB.at[b, :, at(own0 + o, w)]
        return rcopy(ref, ref, u_sem.at[b, j], sib)

    def uf_copy(b):
        ref = UF.at[b, :, at(own0, half)]
        return rcopy(ref, ref, uf_sem.at[b], sib)

    def d_copy(b, j):
        o, w = s_pieces[j]
        return rcopy(DS.at[b, :, pl.ds(o, w)], DR.at[b, :, pl.ds(o, w)], d_sem.at[b, j], sib)

    def y_copy(par, b, j):
        o, w = s_pieces[j]
        return rcopy(SP.at[b, :, pl.ds(o, w)], YR.at[par, b, :, pl.ds(o, w)], y_sem.at[par, b, j], ypeer)

    def e_copy(b, c):
        o, w = t_pieces[c]
        return rcopy(TP.at[b, :, pl.ds(o, w)], EI.at[b, :, pl.ds(o, w)], e_sem.at[b, c], zpair)

    def x_copy(par, b, c):
        o, w = t_pieces[c]
        return rcopy(TP.at[b, :, pl.ds(o, w)], XR.at[par, b, :, pl.ds(o, w)], x_sem.at[par, b, c], zmid)

    def v_copy(b, c):
        o, w = t_pieces[c]
        ref = VB.at[b, :, pl.ds(o, w)]
        return rcopy(ref, ref, v_sem.at[b, c], zpair)

    def vf_copy(b, c):
        o, w = t_pieces[c]
        ref = VF.at[b, :, pl.ds(o, w)]
        return rcopy(ref, ref, vf_sem.at[b, c], zpair)

    early_spans = spans([sum(T_PIECES[c] for c in group) for group in EARLY])
    early = sum(w for _, w in early_spans)

    def s_drain(b, par):
        for j in range(len(s_pieces)):
            d_copy(b, j).wait_send()
            y_copy(par, b, j).wait_send()

    def t_drain(b, par):
        @pl.when(inner)
        def _():
            for c in range(len(t_pieces)):
                x_copy(par, b, c).wait_send()

        @pl.when(edge)
        def _():
            for c in range(len(t_pieces)):
                e_copy(b, c).wait_send()

    def sa(q, b, par, sweep):
        if q == 0:
            pl.when(sweep > 1)(lambda: s_drain(b, 1 - par))
        k0, kw = early_spans[q]
        for dst, h0 in ((DS, sib0), (SP, own0)):
            for o, w in tiles(half):
                part = dot_nn(VB[b, :, k0:k0 + kw], KT[k0:k0 + kw, at(h0 + o, w)])
                dst[b, :, o:o + w] = part if q == 0 else dst[b, :, o:o + w] + part

    def s1(b, par, sweep):
        for j, (o0, width) in enumerate(s_pieces):
            for o, w in tiles(width):
                o += o0
                DS[b, :, o:o + w] += dot_nn(VB[b, :, early:], KT[early:, at(sib0 + o, w)])
            d_copy(b, j).start()
        for o, w in tiles(half):
            SP[b, :, o:o + w] += dot_nn(VB[b, :, early:], KT[early:, at(own0 + o, w)])

    def v_drain(b):
        @pl.when(inner)
        def _():
            for c in range(len(t_pieces)):
                v_copy(b, c).wait_send()

    def s3(j, b, par, sweep):
        o, w = s_pieces[j]
        d_copy(b, j).wait_recv()
        SP[b, :, o:o + w] = SP[b, :, o:o + w] + DR[b, :, o:o + w]
        y_copy(par, b, j).start()
        if j == len(s_pieces) - 1:
            v_drain(b)

    def s4(j, b, par, sweep):
        o, w = s_pieces[j]
        y_copy(par, b, j).wait_recv()
        sl = at(own0 + o, w)
        u = A[b, :, sl] / (SP[b, :, o:o + w] + YR[par, b, :, o:o + w])
        UB[b, :, sl] = u.astype(BF16)
        u_copy(b, j).start()
        UF[b, :, sl] = u
        if j == len(s_pieces) - 1:
            pl.when(sweep == SWEEPS - 1)(lambda: uf_copy(b).start())

    def t0(b, par, sweep):
        for j in range(len(s_pieces)):
            u_copy(b, j).wait()

    def ta(q, b, par, sweep):
        if q == 0:
            pl.when(sweep > 0)(lambda: t_drain(b, 1 - par))
        o0, width = spans(TA_PIECES)[q]
        for o, w in tiles(width):
            o += o0
            TP[b, :, o:o + w] = dot_nn(UB[b, :, at(own0, half)], K[at(own0, half), o:o + w])

    def t1(b, par, sweep):
        def products(send):
            for c, (o0, width) in enumerate(t_pieces):
                for o, w in tiles(width):
                    o += o0
                    TP[b, :, o:o + w] += dot_nn(UB[b, :, at(sib0, half)], K[at(sib0, half), o:o + w])
                if send:
                    e_copy(b, c).start()

        pl.when(edge)(lambda: products(True))
        pl.when(inner)(lambda: products(False))

    def t2(c, b, par, sweep):
        o, w = t_pieces[c]

        @pl.when(inner)
        def _():
            e_copy(b, c).wait_recv()
            TP[b, :, o:o + w] = TP[b, :, o:o + w] + EI[b, :, o:o + w]
            x_copy(par, b, c).start()

    def t3i(c, b, par, sweep):
        o, w = t_pieces[c]

        @pl.when(inner)
        def _():
            x_copy(par, b, c).wait_recv()
            v = B[b, :, o:o + w] / (TP[b, :, o:o + w] + XR[par, b, :, o:o + w])
            VB[b, :, o:o + w] = v.astype(BF16)
            VF[b, :, o:o + w] = v
            pl.when(sweep == SWEEPS - 1)(lambda: vf_copy(b, c).start())
            pl.when(sweep < SWEEPS - 1)(lambda: v_copy(b, c).start())

    def t3e(c, b, par, sweep):
        o, w = t_pieces[c]

        @pl.when(jnp.logical_and(edge, sweep < SWEEPS - 1))
        def _():
            v_copy(b, c).wait_recv()

        @pl.when(jnp.logical_and(edge, sweep == SWEEPS - 1))
        def _():
            vf_copy(b, c).wait_recv()
            VB[b, :, o:o + w] = VF[b, :, o:o + w].astype(BF16)

    def cost_early(b):
        for o, w in tiles(n):
            WP[:, o:o + w] = dot_nn(VB[b, :, :early], KCT[:early, o:o + w])

    def cost_part(b):
        s_drain(b, (SWEEPS - 1) % 2)
        t_drain(b, (SWEEPS - 1) % 2)
        uf_copy(b).wait()
        acc = jnp.zeros((m, 128), F32)
        for o, w in tiles(n):
            p = UF[b, :, o:o + w] * (WP[:, o:o + w] + dot_nn(VB[b, :, early:], KCT[early:, o:o + w]))
            for q in range(0, w, 128):
                acc = acc + p[:, q:q + 128]
        ACC[pl.ds(pl.multiple_of(b * m, m), m), :] = acc
        for c in range(len(t_pieces)):
            pl.when(inner)(lambda c=c: vf_copy(b, c).wait_send())

    def kc(t):
        rows = at(t * 128, 128)

        def turn(q, carry):
            cols = at(q * 256, 256)
            KCT[cols, rows] = KT[cols, rows] * jnp.transpose(C[rows, cols])
            return carry

        lax.fori_loop(0, n // 256, turn, 0)

    steps = {"sa": sa, "s1": s1, "s3": s3, "s4": s4, "ta": ta, "t0": t0, "t1": t1, "t2": t2, "t3": t3i, "e": t3e}

    def tick(i, carry):
        for name, piece, lag in ORDER:
            if name == "cost":
                g = i - lag
                pl.when(jnp.logical_and(g >= total_inst, g < total_inst + NB))(lambda: cost_part(g - total_inst))
            elif name == "ca":
                g = i - lag
                pl.when(jnp.logical_and(g >= total_inst, g < total_inst + NB))(lambda: cost_early(g - total_inst))
            elif name == "kt":
                pl.when(i < 3)(lambda: kt(i))
            elif name == "kc":
                pl.when(i == KC_FIRST)(lambda: c_load.wait())
                pl.when(jnp.logical_and(i >= KC_FIRST, i < KC_FIRST + n // 128))(lambda: kc(i - KC_FIRST))
            else:
                g = i - lag
                fn = steps[name] if piece is None else functools.partial(steps[name], piece)

                @pl.when(jnp.logical_and(g >= (NB if name[0] == "s" or name == "t0" else 0), g < total_inst))
                def _():
                    sweep = lax.div(g, NB)
                    fn(lax.rem(g, NB), lax.rem(sweep, 2), sweep)
        return carry

    lax.fori_loop(1, total_inst + NB, tick, 0)

    tot = jnp.sum(jnp.transpose(ACC[...]), axis=0, keepdims=True)
    CPS[...] = jnp.broadcast_to(tot, CPS.shape)
    me = row * n_col + col
    cps = [rcopy(CPS, CPR.at[me], cp_sem.at[i], dev) for i, dev in enumerate(peers)]
    for cp in cps:
        cp.start()
    CPR[me] = CPS[...]
    for cp in cps:
        cp.wait()
    total = CPR[0]
    for i in range(1, n_row * n_col):
        total = total + CPR[i]
    cost_ref[...] = total[0:1, 0:cost_ref.shape[1]] / norm


def solution(mesh):
    n_row = mesh.shape["row"]
    n_col = mesh.shape["col"]

    def local_fn(kern, cost_mat, src_mass, tgt_mass):
        n = kern.shape[0]
        q = src_mass.shape[1]
        m = q // NB
        half = n // 2
        norm = float(n * n_row) * float(kern.shape[1] * n_col)
        dma = pltpu.SemaphoreType.DMA
        vmem = pltpu.VMEM
        any_spec = pl.BlockSpec(memory_space=pl.ANY)
        np_, ns = len(T_PIECES), len(S_PIECES)
        u, v, cost = pl.pallas_call(
            functools.partial(kernel, n_row, n_col, norm),
            out_shape=(vmem((NB, m, n), F32), vmem((NB, m, n), F32), vmem((1, q), F32)),
            in_specs=[any_spec] * 4,
            out_specs=(pl.BlockSpec(memory_space=vmem),) * 3,
            scratch_shapes=[
                vmem((n, n), BF16), vmem((n, n), BF16), vmem((n, n), BF16), vmem((n, n), BF16),
                vmem((NB, m, n), F32), vmem((NB, m, n), F32),
                vmem((NB, m, n), BF16), vmem((NB, m, n), BF16),
                vmem((m, n), F32),
                vmem((NB, m, half), F32), vmem((NB, m, half), F32),
                vmem((NB, m, half), F32), vmem((2, NB, m, half), F32),
                vmem((NB, m, n), F32), vmem((NB, m, n), F32),
                vmem((2, NB, m, n), F32),
                vmem((n_col, 1, n), F32),
                vmem((128, 128), F32), vmem((8, 128), F32), vmem((n_row * n_col, 8, 128), F32),
                dma((len(K_PIECES),)), dma((3,)), dma((n_col - 1, 2)),
                dma((NB, ns, 2)), dma((2, NB, ns, 2)), dma((NB, ns, 2)), dma((NB, 2)),
                dma((NB, np_, 2)), dma((2, NB, np_, 2)), dma((NB, np_, 2)), dma((NB, np_, 2)),
                dma((n_row * n_col - 1, 2)),
            ],
            compiler_params=pltpu.CompilerParams(collective_id=0, has_side_effects=True, vmem_limit_bytes=60 * 1024 * 1024),
        )(kern, cost_mat, src_mass.T.reshape(NB, m, n), tgt_mass.T.reshape(NB, m, n))
        return u.reshape(q, n).T, v.reshape(q, n).T, cost.reshape(q)

    return jax.shard_map(local_fn, mesh=mesh, in_specs=(P("row", "col"), P("row", "col"), P("row", "prob"), P("col", "prob")),
                         out_specs=(P("row", "prob"), P("col", "prob"), P("prob")), check_vma=False)
```

```python
import functools

import jax
import jax.numpy as jnp
from jax import lax
from jax.experimental import pallas as pl
from jax.experimental.pallas import tpu as pltpu
from jax.sharding import PartitionSpec as P

SWEEPS = 6
MESH = pl.DeviceIdType.MESH
F32 = jnp.float32
BF16 = jnp.bfloat16
NB = 4
T_PIECES = (512, 512, 512, 512, 256)
EARLY = ((0, 1, 2),)
TA_PIECES = (2304,)
S_PIECES = (512, 640)
K_PIECES = (768, 768, 512, 256)
KC_FIRST = 5
ORDER = (
    ("s4", 0, 1), ("t2", 1, 2), ("t3", 3, 3), ("s4", 1, 1), ("t3", 4, 3), ("s3", 0, 0), ("t2", 2, 2),
    ("ta", 0, 1), ("t2", 3, 2), ("s3", 1, 0), ("t0", None, 1), ("t1", None, 1), ("t2", 4, 2), ("e", 0, 3),
    ("kc", None, 0), ("e", 1, 3), ("t3", 0, 2), ("e", 2, 3), ("kt", None, 0), ("sa", 0, -1), ("ca", None, -1),
    ("t3", 1, 2), ("t3", 2, 2), ("e", 3, 3), ("t2", 0, 1), ("e", 4, 3), ("s1", None, -1), ("cost", None, -1),
)


def dot_nn(x, y):
    return jnp.dot(x, y, preferred_element_type=F32)


def dot_nt(x, y):
    return lax.dot_general(x, y, (((1,), (1,)), ((), ())), preferred_element_type=F32)


def spans(sizes):
    out, o = [], 0
    for w in sizes:
        out.append((o, w))
        o += w
    return out


def tiles(size, tile=256):
    return [(o, min(tile, size - o)) for o in range(0, size, tile)]


def kernel(n_row, n_col, norm,
           k_hbm, c_hbm, a_hbm, b_hbm, UF, VF, cost_ref,
           K, KT, C, KCT, A, B, UB, VB, WP, DS, DR, SP, YR, TP, EI, XR, RX, ACC, CPS, CPR,
           k_sem, in_sem, r_sem,
           d_sem, y_sem, u_sem, uf_sem, e_sem, x_sem, v_sem, vf_sem, cp_sem):
    row = lax.axis_index("row")
    col = lax.axis_index("col")
    core = lax.rem(col, 2)
    n = K.shape[0]
    half = n // 2
    m = UB.shape[1]
    total_inst = SWEEPS * NB
    sib = {"col": col + 1 - 2 * core}
    ypeer = {"col": lax.rem(col + 2, n_col)}
    inner = jnp.logical_or(row == 1, row == 2)
    edge = jnp.logical_not(inner)
    zpair = {"row": row + 1 - 2 * lax.rem(row, 2)}
    zmid = {"row": n_row - 1 - row}
    own0 = pl.multiple_of(core * half, 128)
    sib0 = pl.multiple_of((1 - core) * half, 128)
    t_pieces = spans(T_PIECES)
    s_pieces = spans(S_PIECES)

    def at(o, w):
        return pl.ds(pl.multiple_of(o, 128), w)

    def rcopy(src, dst, sem, dev):
        return pltpu.make_async_remote_copy(src_ref=src, dst_ref=dst, send_sem=sem.at[0], recv_sem=sem.at[1],
                                            device_id=dev, device_id_type=MESH)

    a_load = pltpu.make_async_copy(a_hbm, A, in_sem.at[0])
    b_load = pltpu.make_async_copy(b_hbm, B, in_sem.at[1])
    c_load = pltpu.make_async_copy(c_hbm, C, in_sem.at[2])
    k_loads = [pltpu.make_async_copy(k_hbm.at[o:o + w, :], K.at[o:o + w, :], k_sem.at[j])
               for j, (o, w) in enumerate(spans(K_PIECES))]
    for cp in k_loads:
        cp.start()
    a_load.start()

    barrier = pltpu.get_barrier_semaphore()
    rel = [(dr, dc) for dr in range(n_row) for dc in range(n_col) if (dr, dc) != (0, 0)]
    peers = [{"row": lax.rem(row + dr, n_row), "col": lax.rem(col + dc, n_col)} for dr, dc in rel]
    for dev in peers:
        pl.semaphore_signal(barrier, inc=1, device_id=dev, device_id_type=MESH)

    ACC[...] = jnp.zeros_like(ACC)

    def kt(t):
        rows = at(t * (n // 3), n // 3)

        def turn(q, carry):
            cols = at(q * 256, 256)
            KT[cols, rows] = jnp.transpose(K[rows, cols])
            return carry

        lax.fori_loop(0, n // 256, turn, 0)

    ones = jnp.ones((16, n), BF16)
    for cp, (o, w) in zip(k_loads, spans(K_PIECES)):
        cp.wait()
        RX[col, :, o:o + w] = dot_nt(ones, K[o:o + w, :])[:1]
    pl.semaphore_wait(barrier, len(peers))
    r_copies = [rcopy(RX.at[col], RX.at[col], r_sem.at[d - 1], {"col": lax.rem(col + d, n_col)}) for d in range(1, n_col)]
    for cp in r_copies:
        cp.start()
    b_load.start()
    c_load.start()
    a_load.wait()
    kt(0)
    for cp in r_copies:
        cp.wait()
    s0 = RX[0] + RX[1]
    for d in range(2, n_col):
        s0 = s0 + RX[d]
    for b in range(NB):
        UB[b] = (A[b] / s0).astype(BF16)
    b_load.wait()

    def u_copy(b, j):
        o, w = s_pieces[j]
        ref = UB.at[b, :, at(own0 + o, w)]
        return rcopy(ref, ref, u_sem.at[b, j], sib)

    def uf_copy(b):
        ref = UF.at[b, :, at(own0, half)]
        return rcopy(ref, ref, uf_sem.at[b], sib)

    def d_copy(b, j):
        o, w = s_pieces[j]
        return rcopy(DS.at[b, :, pl.ds(o, w)], DR.at[b, :, pl.ds(o, w)], d_sem.at[b, j], sib)

    def y_copy(par, b, j):
        o, w = s_pieces[j]
        return rcopy(SP.at[b, :, pl.ds(o, w)], YR.at[par, b, :, pl.ds(o, w)], y_sem.at[par, b, j], ypeer)

    def e_copy(b, c):
        o, w = t_pieces[c]
        return rcopy(TP.at[b, :, pl.ds(o, w)], EI.at[b, :, pl.ds(o, w)], e_sem.at[b, c], zpair)

    def x_copy(par, b, c):
        o, w = t_pieces[c]
        return rcopy(TP.at[b, :, pl.ds(o, w)], XR.at[par, b, :, pl.ds(o, w)], x_sem.at[par, b, c], zmid)

    def v_copy(b, c):
        o, w = t_pieces[c]
        ref = VB.at[b, :, pl.ds(o, w)]
        return rcopy(ref, ref, v_sem.at[b, c], zpair)

    def vf_copy(b, c):
        o, w = t_pieces[c]
        ref = VF.at[b, :, pl.ds(o, w)]
        return rcopy(ref, ref, vf_sem.at[b, c], zpair)

    early_spans = spans([sum(T_PIECES[c] for c in group) for group in EARLY])
    early = sum(w for _, w in early_spans)

    def s_drain(b, par):
        for j in range(len(s_pieces)):
            d_copy(b, j).wait_send()
            y_copy(par, b, j).wait_send()

    def t_drain(b, par):
        @pl.when(inner)
        def _():
            for c in range(len(t_pieces)):
                x_copy(par, b, c).wait_send()

        @pl.when(edge)
        def _():
            for c in range(len(t_pieces)):
                e_copy(b, c).wait_send()

    def sa(q, b, par, sweep):
        if q == 0:
            pl.when(sweep > 1)(lambda: s_drain(b, 1 - par))
        k0, kw = early_spans[q]
        for dst, h0 in ((DS, sib0), (SP, own0)):
            for o, w in tiles(half):
                part = dot_nn(VB[b, :, k0:k0 + kw], KT[k0:k0 + kw, at(h0 + o, w)])
                dst[b, :, o:o + w] = part if q == 0 else dst[b, :, o:o + w] + part

    def s1(b, par, sweep):
        for j, (o0, width) in enumerate(s_pieces):
            for o, w in tiles(width):
                o += o0
                DS[b, :, o:o + w] += dot_nn(VB[b, :, early:], KT[early:, at(sib0 + o, w)])
            d_copy(b, j).start()
        for o, w in tiles(half):
            SP[b, :, o:o + w] += dot_nn(VB[b, :, early:], KT[early:, at(own0 + o, w)])

    def v_drain(b):
        @pl.when(inner)
        def _():
            for c in range(len(t_pieces)):
                v_copy(b, c).wait_send()

    def s3(j, b, par, sweep):
        o, w = s_pieces[j]
        d_copy(b, j).wait_recv()
        SP[b, :, o:o + w] = SP[b, :, o:o + w] + DR[b, :, o:o + w]
        y_copy(par, b, j).start()
        if j == len(s_pieces) - 1:
            v_drain(b)

    def s4(j, b, par, sweep):
        o, w = s_pieces[j]
        y_copy(par, b, j).wait_recv()
        sl = at(own0 + o, w)
        u = A[b, :, sl] / (SP[b, :, o:o + w] + YR[par, b, :, o:o + w])
        UB[b, :, sl] = u.astype(BF16)
        u_copy(b, j).start()
        UF[b, :, sl] = u
        if j == len(s_pieces) - 1:
            pl.when(sweep == SWEEPS - 1)(lambda: uf_copy(b).start())

    def t0(b, par, sweep):
        for j in range(len(s_pieces)):
            u_copy(b, j).wait()

    def ta(q, b, par, sweep):
        if q == 0:
            pl.when(sweep > 0)(lambda: t_drain(b, 1 - par))
        o0, width = spans(TA_PIECES)[q]
        for o, w in tiles(width):
            o += o0
            TP[b, :, o:o + w] = dot_nn(UB[b, :, at(own0, half)], K[at(own0, half), o:o + w])

    def t1(b, par, sweep):
        def products(send):
            for c, (o0, width) in enumerate(t_pieces):
                for o, w in tiles(width):
                    o += o0
                    TP[b, :, o:o + w] += dot_nn(UB[b, :, at(sib0, half)], K[at(sib0, half), o:o + w])
                if send:
                    e_copy(b, c).start()

        pl.when(edge)(lambda: products(True))
        pl.when(inner)(lambda: products(False))

    def t2(c, b, par, sweep):
        o, w = t_pieces[c]

        @pl.when(inner)
        def _():
            e_copy(b, c).wait_recv()
            TP[b, :, o:o + w] = TP[b, :, o:o + w] + EI[b, :, o:o + w]
            x_copy(par, b, c).start()

    def t3i(c, b, par, sweep):
        o, w = t_pieces[c]

        @pl.when(inner)
        def _():
            x_copy(par, b, c).wait_recv()
            v = B[b, :, o:o + w] / (TP[b, :, o:o + w] + XR[par, b, :, o:o + w])
            VB[b, :, o:o + w] = v.astype(BF16)
            VF[b, :, o:o + w] = v
            pl.when(sweep == SWEEPS - 1)(lambda: vf_copy(b, c).start())
            pl.when(sweep < SWEEPS - 1)(lambda: v_copy(b, c).start())

    def t3e(c, b, par, sweep):
        o, w = t_pieces[c]

        @pl.when(jnp.logical_and(edge, sweep < SWEEPS - 1))
        def _():
            v_copy(b, c).wait_recv()

        @pl.when(jnp.logical_and(edge, sweep == SWEEPS - 1))
        def _():
            vf_copy(b, c).wait_recv()
            VB[b, :, o:o + w] = VF[b, :, o:o + w].astype(BF16)

    def cost_early(b):
        for o, w in tiles(n):
            WP[:, o:o + w] = dot_nn(VB[b, :, :early], KCT[:early, o:o + w])

    def cost_part(b):
        s_drain(b, (SWEEPS - 1) % 2)
        t_drain(b, (SWEEPS - 1) % 2)
        uf_copy(b).wait()
        acc = jnp.zeros((m, 128), F32)
        for o, w in tiles(n):
            p = UF[b, :, o:o + w] * (WP[:, o:o + w] + dot_nn(VB[b, :, early:], KCT[early:, o:o + w]))
            for q in range(0, w, 128):
                acc = acc + p[:, q:q + 128]
        ACC[pl.ds(pl.multiple_of(b * m, m), m), :] = acc
        for c in range(len(t_pieces)):
            pl.when(inner)(lambda c=c: vf_copy(b, c).wait_send())

    def kc(t):
        rows = at(t * 128, 128)

        def turn(q, carry):
            cols = at(q * 256, 256)
            KCT[cols, rows] = KT[cols, rows] * jnp.transpose(C[rows, cols])
            return carry

        lax.fori_loop(0, n // 256, turn, 0)

    steps = {"sa": sa, "s1": s1, "s3": s3, "s4": s4, "ta": ta, "t0": t0, "t1": t1, "t2": t2, "t3": t3i, "e": t3e}

    def tick(i, carry):
        for name, piece, lag in ORDER:
            if name == "cost":
                g = i - lag
                pl.when(jnp.logical_and(g >= total_inst, g < total_inst + NB))(lambda: cost_part(g - total_inst))
            elif name == "ca":
                g = i - lag
                pl.when(jnp.logical_and(g >= total_inst, g < total_inst + NB))(lambda: cost_early(g - total_inst))
            elif name == "kt":
                pl.when(i < 3)(lambda: kt(i))
            elif name == "kc":
                pl.when(i == KC_FIRST)(lambda: c_load.wait())
                pl.when(jnp.logical_and(i >= KC_FIRST, i < KC_FIRST + n // 128))(lambda: kc(i - KC_FIRST))
            else:
                g = i - lag
                fn = steps[name] if piece is None else functools.partial(steps[name], piece)

                @pl.when(jnp.logical_and(g >= (NB if name[0] == "s" or name == "t0" else 0), g < total_inst))
                def _():
                    sweep = lax.div(g, NB)
                    fn(lax.rem(g, NB), lax.rem(sweep, 2), sweep)
        return carry

    lax.fori_loop(1, total_inst + NB, tick, 0)

    tot = jnp.sum(jnp.transpose(ACC[...]), axis=0, keepdims=True)
    CPS[...] = jnp.broadcast_to(tot, CPS.shape)
    me = row * n_col + col
    cps = [rcopy(CPS, CPR.at[me], cp_sem.at[i], dev) for i, dev in enumerate(peers)]
    for cp in cps:
        cp.start()
    CPR[me] = CPS[...]
    for cp in cps:
        cp.wait()
    total = CPR[0]
    for i in range(1, n_row * n_col):
        total = total + CPR[i]
    cost_ref[...] = total[0:1, 0:cost_ref.shape[1]] / norm


def solution(mesh):
    n_row = mesh.shape["row"]
    n_col = mesh.shape["col"]

    def local_fn(kern, cost_mat, src_mass, tgt_mass):
        n = kern.shape[0]
        q = src_mass.shape[1]
        m = q // NB
        half = n // 2
        norm = float(n * n_row) * float(kern.shape[1] * n_col)
        dma = pltpu.SemaphoreType.DMA
        vmem = pltpu.VMEM
        any_spec = pl.BlockSpec(memory_space=pl.ANY)
        np_, ns = len(T_PIECES), len(S_PIECES)
        u, v, cost = pl.pallas_call(
            functools.partial(kernel, n_row, n_col, norm),
            out_shape=(vmem((NB, m, n), F32), vmem((NB, m, n), F32), vmem((1, q), F32)),
            in_specs=[any_spec] * 4,
            out_specs=(pl.BlockSpec(memory_space=vmem),) * 3,
            scratch_shapes=[
                vmem((n, n), BF16), vmem((n, n), BF16), vmem((n, n), BF16), vmem((n, n), BF16),
                vmem((NB, m, n), F32), vmem((NB, m, n), F32),
                vmem((NB, m, n), BF16), vmem((NB, m, n), BF16),
                vmem((m, n), F32),
                vmem((NB, m, half), F32), vmem((NB, m, half), F32),
                vmem((NB, m, half), F32), vmem((2, NB, m, half), F32),
                vmem((NB, m, n), F32), vmem((NB, m, n), F32),
                vmem((2, NB, m, n), F32),
                vmem((n_col, 1, n), F32),
                vmem((128, 128), F32), vmem((8, 128), F32), vmem((n_row * n_col, 8, 128), F32),
                dma((len(K_PIECES),)), dma((3,)), dma((n_col - 1, 2)),
                dma((NB, ns, 2)), dma((2, NB, ns, 2)), dma((NB, ns, 2)), dma((NB, 2)),
                dma((NB, np_, 2)), dma((2, NB, np_, 2)), dma((NB, np_, 2)), dma((NB, np_, 2)),
                dma((n_row * n_col - 1, 2)),
            ],
            compiler_params=pltpu.CompilerParams(collective_id=0, has_side_effects=True, vmem_limit_bytes=60 * 1024 * 1024),
        )(kern, cost_mat, src_mass.T.reshape(NB, m, n), tgt_mass.T.reshape(NB, m, n))
        return u.reshape(q, n).T, v.reshape(q, n).T, cost.reshape(q)

    return jax.shard_map(local_fn, mesh=mesh, in_specs=(P("row", "col"), P("row", "col"), P("row", "prob"), P("col", "prob")),
                         out_specs=(P("row", "prob"), P("col", "prob"), P("prob")), check_vma=False)
```

```python
import functools

import jax
import jax.numpy as jnp
from jax import lax
from jax.experimental import pallas as pl
from jax.experimental.pallas import tpu as pltpu
from jax.sharding import PartitionSpec as P

SWEEPS = 6
MESH = pl.DeviceIdType.MESH
F32 = jnp.float32
BF16 = jnp.bfloat16
NB = 4
T_PIECES = (512, 512, 512, 512, 256)
EARLY = ((0, 1, 2),)
TA_PIECES = (2304,)
S_PIECES = (512, 640)
K_PIECES = (256, 512, 768, 512, 256)
KC_FIRST = 5
ORDER = (
    ("e", 2, 4), ("sa", 0, 0), ("ca", None, 0), ("t3", 0, 3), ("s4", 0, 1), ("e", 3, 4), ("e", 4, 4),
    ("s1", None, 0), ("cost", None, 0), ("t3", 1, 3), ("s4", 1, 1), ("t2", 0, 2), ("t3", 2, 3), ("s3", 0, 0),
    ("ta", 0, 1), ("t2", 1, 2), ("t3", 3, 3), ("s3", 1, 0), ("t3", 4, 3), ("t0", None, 1), ("t2", 2, 2),
    ("t1", None, 1), ("t2", 3, 2), ("e", 0, 3), ("kc", None, 0), ("t2", 4, 2), ("e", 1, 3), ("kt", None, 0),
)


def dot_nn(x, y):
    return jnp.dot(x, y, preferred_element_type=F32)


def dot_nt(x, y):
    return lax.dot_general(x, y, (((1,), (1,)), ((), ())), preferred_element_type=F32)


def spans(sizes):
    out, o = [], 0
    for w in sizes:
        out.append((o, w))
        o += w
    return out


def tiles(size, tile=256):
    return [(o, min(tile, size - o)) for o in range(0, size, tile)]


def kernel(n_row, n_col, norm,
           k_hbm, c_hbm, a_hbm, b_hbm, UF, VF, cost_ref,
           K, KT, C, KCT, A, B, UB, VB, WP, DS, DR, SP, YR, TP, EI, XR, RX, ACC, CPS, CPR,
           k_sem, in_sem, r_sem,
           d_sem, y_sem, u_sem, uf_sem, e_sem, x_sem, v_sem, vf_sem, cp_sem):
    row = lax.axis_index("row")
    col = lax.axis_index("col")
    core = lax.rem(col, 2)
    n = K.shape[0]
    half = n // 2
    m = UB.shape[1]
    total_inst = SWEEPS * NB
    sib = {"col": col + 1 - 2 * core}
    ypeer = {"col": lax.rem(col + 2, n_col)}
    inner = jnp.logical_or(row == 1, row == 2)
    edge = jnp.logical_not(inner)
    zpair = {"row": row + 1 - 2 * lax.rem(row, 2)}
    zmid = {"row": n_row - 1 - row}
    own0 = pl.multiple_of(core * half, 128)
    sib0 = pl.multiple_of((1 - core) * half, 128)
    t_pieces = spans(T_PIECES)
    s_pieces = spans(S_PIECES)

    def at(o, w):
        return pl.ds(pl.multiple_of(o, 128), w)

    def rcopy(src, dst, sem, dev):
        return pltpu.make_async_remote_copy(src_ref=src, dst_ref=dst, send_sem=sem.at[0], recv_sem=sem.at[1],
                                            device_id=dev, device_id_type=MESH)

    a_load = pltpu.make_async_copy(a_hbm, A, in_sem.at[0])
    b_load = pltpu.make_async_copy(b_hbm, B, in_sem.at[1])
    c_load = pltpu.make_async_copy(c_hbm, C, in_sem.at[2])
    k_loads = [pltpu.make_async_copy(k_hbm.at[o:o + w, :], K.at[o:o + w, :], k_sem.at[j])
               for j, (o, w) in enumerate(spans(K_PIECES))]
    for cp in k_loads:
        cp.start()
    a_load.start()

    barrier = pltpu.get_barrier_semaphore()
    rel = [(dr, dc) for dr in range(n_row) for dc in range(n_col) if (dr, dc) != (0, 0)]
    peers = [{"row": lax.rem(row + dr, n_row), "col": lax.rem(col + dc, n_col)} for dr, dc in rel]
    for dev in peers:
        pl.semaphore_signal(barrier, inc=1, device_id=dev, device_id_type=MESH)

    ACC[...] = jnp.zeros_like(ACC)

    def kt(t):
        rows = at(t * (n // 3), n // 3)

        def turn(q, carry):
            cols = at(q * 256, 256)
            KT[cols, rows] = jnp.transpose(K[rows, cols])
            return carry

        lax.fori_loop(0, n // 256, turn, 0)

    ones = jnp.ones((16, n), BF16)
    for cp, (o, w) in zip(k_loads, spans(K_PIECES)):
        cp.wait()
        RX[col, :, o:o + w] = dot_nt(ones, K[o:o + w, :])[:1]
    pl.semaphore_wait(barrier, len(peers))
    r_copies = [rcopy(RX.at[col], RX.at[col], r_sem.at[d - 1], {"col": lax.rem(col + d, n_col)}) for d in range(1, n_col)]
    for cp in r_copies:
        cp.start()
    b_load.start()
    c_load.start()
    a_load.wait()
    kt(0)
    for cp in r_copies:
        cp.wait()
    s0 = RX[0] + RX[1]
    for d in range(2, n_col):
        s0 = s0 + RX[d]
    for b in range(NB):
        UB[b] = (A[b] / s0).astype(BF16)
    b_load.wait()

    def u_copy(b, j):
        o, w = s_pieces[j]
        ref = UB.at[b, :, at(own0 + o, w)]
        return rcopy(ref, ref, u_sem.at[b, j], sib)

    def uf_copy(b):
        ref = UF.at[b, :, at(own0, half)]
        return rcopy(ref, ref, uf_sem.at[b], sib)

    def d_copy(b, j):
        o, w = s_pieces[j]
        return rcopy(DS.at[b, :, pl.ds(o, w)], DR.at[b, :, pl.ds(o, w)], d_sem.at[b, j], sib)

    def y_copy(par, b, j):
        o, w = s_pieces[j]
        return rcopy(SP.at[b, :, pl.ds(o, w)], YR.at[par, b, :, pl.ds(o, w)], y_sem.at[par, b, j], ypeer)

    def e_copy(b, c):
        o, w = t_pieces[c]
        return rcopy(TP.at[b, :, pl.ds(o, w)], EI.at[b, :, pl.ds(o, w)], e_sem.at[b, c], zpair)

    def x_copy(par, b, c):
        o, w = t_pieces[c]
        return rcopy(TP.at[b, :, pl.ds(o, w)], XR.at[par, b, :, pl.ds(o, w)], x_sem.at[par, b, c], zmid)

    def v_copy(b, c):
        o, w = t_pieces[c]
        ref = VB.at[b, :, pl.ds(o, w)]
        return rcopy(ref, ref, v_sem.at[b, c], zpair)

    def vf_copy(b, c):
        o, w = t_pieces[c]
        ref = VF.at[b, :, pl.ds(o, w)]
        return rcopy(ref, ref, vf_sem.at[b, c], zpair)

    early_spans = spans([sum(T_PIECES[c] for c in group) for group in EARLY])
    early = sum(w for _, w in early_spans)

    def s_drain(b, par):
        for j in range(len(s_pieces)):
            d_copy(b, j).wait_send()
            y_copy(par, b, j).wait_send()

    def t_drain(b, par):
        @pl.when(inner)
        def _():
            for c in range(len(t_pieces)):
                x_copy(par, b, c).wait_send()

        @pl.when(edge)
        def _():
            for c in range(len(t_pieces)):
                e_copy(b, c).wait_send()

    def sa(q, b, par, sweep):
        if q == 0:
            pl.when(sweep > 1)(lambda: s_drain(b, 1 - par))
        k0, kw = early_spans[q]
        for dst, h0 in ((DS, sib0), (SP, own0)):
            for o, w in tiles(half):
                part = dot_nn(VB[b, :, k0:k0 + kw], KT[k0:k0 + kw, at(h0 + o, w)])
                dst[b, :, o:o + w] = part if q == 0 else dst[b, :, o:o + w] + part

    def s1(b, par, sweep):
        for j, (o0, width) in enumerate(s_pieces):
            for o, w in tiles(width):
                o += o0
                DS[b, :, o:o + w] += dot_nn(VB[b, :, early:], KT[early:, at(sib0 + o, w)])
            d_copy(b, j).start()
        for o, w in tiles(half):
            SP[b, :, o:o + w] += dot_nn(VB[b, :, early:], KT[early:, at(own0 + o, w)])

    def v_drain(b):
        @pl.when(inner)
        def _():
            for c in range(len(t_pieces)):
                v_copy(b, c).wait_send()

    def s3(j, b, par, sweep):
        o, w = s_pieces[j]
        d_copy(b, j).wait_recv()
        SP[b, :, o:o + w] = SP[b, :, o:o + w] + DR[b, :, o:o + w]
        y_copy(par, b, j).start()
        if j == len(s_pieces) - 1:
            v_drain(b)

    def s4(j, b, par, sweep):
        o, w = s_pieces[j]
        y_copy(par, b, j).wait_recv()
        sl = at(own0 + o, w)
        u = A[b, :, sl] / (SP[b, :, o:o + w] + YR[par, b, :, o:o + w])
        UB[b, :, sl] = u.astype(BF16)
        u_copy(b, j).start()
        UF[b, :, sl] = u
        if j == len(s_pieces) - 1:
            pl.when(sweep == SWEEPS - 1)(lambda: uf_copy(b).start())

    def t0(b, par, sweep):
        for j in range(len(s_pieces)):
            u_copy(b, j).wait()

    def ta(q, b, par, sweep):
        if q == 0:
            pl.when(sweep > 0)(lambda: t_drain(b, 1 - par))
        o0, width = spans(TA_PIECES)[q]
        for o, w in tiles(width):
            o += o0
            TP[b, :, o:o + w] = dot_nn(UB[b, :, at(own0, half)], K[at(own0, half), o:o + w])

    def t1(b, par, sweep):
        def products(send):
            for c, (o0, width) in enumerate(t_pieces):
                for o, w in tiles(width):
                    o += o0
                    TP[b, :, o:o + w] += dot_nn(UB[b, :, at(sib0, half)], K[at(sib0, half), o:o + w])
                if send:
                    e_copy(b, c).start()

        pl.when(edge)(lambda: products(True))
        pl.when(inner)(lambda: products(False))

    def t2(c, b, par, sweep):
        o, w = t_pieces[c]

        @pl.when(inner)
        def _():
            e_copy(b, c).wait_recv()
            TP[b, :, o:o + w] = TP[b, :, o:o + w] + EI[b, :, o:o + w]
            x_copy(par, b, c).start()

    def t3i(c, b, par, sweep):
        o, w = t_pieces[c]

        @pl.when(inner)
        def _():
            x_copy(par, b, c).wait_recv()
            v = B[b, :, o:o + w] / (TP[b, :, o:o + w] + XR[par, b, :, o:o + w])
            VB[b, :, o:o + w] = v.astype(BF16)
            VF[b, :, o:o + w] = v
            pl.when(sweep == SWEEPS - 1)(lambda: vf_copy(b, c).start())
            pl.when(sweep < SWEEPS - 1)(lambda: v_copy(b, c).start())

    def t3e(c, b, par, sweep):
        o, w = t_pieces[c]

        @pl.when(jnp.logical_and(edge, sweep < SWEEPS - 1))
        def _():
            v_copy(b, c).wait_recv()

        @pl.when(jnp.logical_and(edge, sweep == SWEEPS - 1))
        def _():
            vf_copy(b, c).wait_recv()
            VB[b, :, o:o + w] = VF[b, :, o:o + w].astype(BF16)

    def cost_early(b):
        for o, w in tiles(n):
            WP[:, o:o + w] = dot_nn(VB[b, :, :early], KCT[:early, o:o + w])

    def cost_part(b):
        s_drain(b, (SWEEPS - 1) % 2)
        t_drain(b, (SWEEPS - 1) % 2)
        uf_copy(b).wait()
        acc = jnp.zeros((m, 128), F32)
        for o, w in tiles(n):
            p = UF[b, :, o:o + w] * (WP[:, o:o + w] + dot_nn(VB[b, :, early:], KCT[early:, o:o + w]))
            for q in range(0, w, 128):
                acc = acc + p[:, q:q + 128]
        ACC[pl.ds(pl.multiple_of(b * m, m), m), :] = acc
        for c in range(len(t_pieces)):
            pl.when(inner)(lambda c=c: vf_copy(b, c).wait_send())

    def kc(t):
        rows = at(t * 128, 128)

        def turn(q, carry):
            cols = at(q * 256, 256)
            KCT[cols, rows] = KT[cols, rows] * jnp.transpose(C[rows, cols])
            return carry

        lax.fori_loop(0, n // 256, turn, 0)

    steps = {"sa": sa, "s1": s1, "s3": s3, "s4": s4, "ta": ta, "t0": t0, "t1": t1, "t2": t2, "t3": t3i, "e": t3e}

    def tick(i, carry):
        for name, piece, lag in ORDER:
            if name == "cost":
                g = i - lag
                pl.when(jnp.logical_and(g >= total_inst, g < total_inst + NB))(lambda: cost_part(g - total_inst))
            elif name == "ca":
                g = i - lag
                pl.when(jnp.logical_and(g >= total_inst, g < total_inst + NB))(lambda: cost_early(g - total_inst))
            elif name == "kt":
                pl.when(i < 3)(lambda: kt(i))
            elif name == "kc":
                pl.when(i == KC_FIRST)(lambda: c_load.wait())
                pl.when(jnp.logical_and(i >= KC_FIRST, i < KC_FIRST + n // 128))(lambda: kc(i - KC_FIRST))
            else:
                g = i - lag
                fn = steps[name] if piece is None else functools.partial(steps[name], piece)

                @pl.when(jnp.logical_and(g >= (NB if name[0] == "s" or name == "t0" else 0), g < total_inst))
                def _():
                    sweep = lax.div(g, NB)
                    fn(lax.rem(g, NB), lax.rem(sweep, 2), sweep)
        return carry

    lax.fori_loop(1, total_inst + NB, tick, 0)

    tot = jnp.sum(jnp.transpose(ACC[...]), axis=0, keepdims=True)
    CPS[...] = jnp.broadcast_to(tot, CPS.shape)
    me = row * n_col + col
    cps = [rcopy(CPS, CPR.at[me], cp_sem.at[i], dev) for i, dev in enumerate(peers)]
    for cp in cps:
        cp.start()
    CPR[me] = CPS[...]
    for cp in cps:
        cp.wait()
    total = CPR[0]
    for i in range(1, n_row * n_col):
        total = total + CPR[i]
    cost_ref[...] = total[0:1, 0:cost_ref.shape[1]] / norm


def solution(mesh):
    n_row = mesh.shape["row"]
    n_col = mesh.shape["col"]

    def local_fn(kern, cost_mat, src_mass, tgt_mass):
        n = kern.shape[0]
        q = src_mass.shape[1]
        m = q // NB
        half = n // 2
        norm = float(n * n_row) * float(kern.shape[1] * n_col)
        dma = pltpu.SemaphoreType.DMA
        vmem = pltpu.VMEM
        any_spec = pl.BlockSpec(memory_space=pl.ANY)
        np_, ns = len(T_PIECES), len(S_PIECES)
        u, v, cost = pl.pallas_call(
            functools.partial(kernel, n_row, n_col, norm),
            out_shape=(vmem((NB, m, n), F32), vmem((NB, m, n), F32), vmem((1, q), F32)),
            in_specs=[any_spec] * 4,
            out_specs=(pl.BlockSpec(memory_space=vmem),) * 3,
            scratch_shapes=[
                vmem((n, n), BF16), vmem((n, n), BF16), vmem((n, n), BF16), vmem((n, n), BF16),
                vmem((NB, m, n), F32), vmem((NB, m, n), F32),
                vmem((NB, m, n), BF16), vmem((NB, m, n), BF16),
                vmem((m, n), F32),
                vmem((NB, m, half), F32), vmem((NB, m, half), F32),
                vmem((NB, m, half), F32), vmem((2, NB, m, half), F32),
                vmem((NB, m, n), F32), vmem((NB, m, n), F32),
                vmem((2, NB, m, n), F32),
                vmem((n_col, 1, n), F32),
                vmem((128, 128), F32), vmem((8, 128), F32), vmem((n_row * n_col, 8, 128), F32),
                dma((len(K_PIECES),)), dma((3,)), dma((n_col - 1, 2)),
                dma((NB, ns, 2)), dma((2, NB, ns, 2)), dma((NB, ns, 2)), dma((NB, 2)),
                dma((NB, np_, 2)), dma((2, NB, np_, 2)), dma((NB, np_, 2)), dma((NB, np_, 2)),
                dma((n_row * n_col - 1, 2)),
            ],
            compiler_params=pltpu.CompilerParams(collective_id=0, has_side_effects=True, vmem_limit_bytes=60 * 1024 * 1024),
        )(kern, cost_mat, src_mass.T.reshape(NB, m, n), tgt_mass.T.reshape(NB, m, n))
        return u.reshape(q, n).T, v.reshape(q, n).T, cost.reshape(q)

    return jax.shard_map(local_fn, mesh=mesh, in_specs=(P("row", "col"), P("row", "col"), P("row", "prob"), P("col", "prob")),
                         out_specs=(P("row", "prob"), P("col", "prob"), P("prob")), check_vma=False)
```

```python
import functools

import jax
import jax.numpy as jnp
from jax import lax
from jax.experimental import pallas as pl
from jax.experimental.pallas import tpu as pltpu
from jax.sharding import PartitionSpec as P

SWEEPS = 6
MESH = pl.DeviceIdType.MESH
F32 = jnp.float32
BF16 = jnp.bfloat16
NB = 4
T_PIECES = (512, 512, 512, 512, 256)
EARLY = ((0, 1, 2),)
TA_PIECES = (2304,)
S_PIECES = (512, 640)
K_PIECES = (768, 768, 512, 256)
KC_FIRST = 5
ORDER = (
    ("e", 1, 4), ("e", 2, 4), ("sa", 0, 0), ("ca", None, 0), ("e", 3, 4), ("t3", 0, 3), ("s4", 0, 1),
    ("e", 4, 4), ("s1", None, 0), ("cost", None, 0), ("t3", 1, 3), ("s4", 1, 1), ("ta", 0, 1), ("s3", 0, 0),
    ("t2", 0, 2), ("s3", 1, 0), ("t3", 2, 3), ("t2", 1, 2), ("t0", None, 1), ("t1", None, 1), ("t3", 3, 3),
    ("t2", 2, 2), ("t3", 4, 3), ("e", 0, 3), ("kc", None, 0), ("t2", 3, 2), ("t2", 4, 2), ("kt", None, 0),
)


def dot_nn(x, y):
    return jnp.dot(x, y, preferred_element_type=F32)


def dot_nt(x, y):
    return lax.dot_general(x, y, (((1,), (1,)), ((), ())), preferred_element_type=F32)


def spans(sizes):
    out, o = [], 0
    for w in sizes:
        out.append((o, w))
        o += w
    return out


def tiles(size, tile=256):
    return [(o, min(tile, size - o)) for o in range(0, size, tile)]


def kernel(n_row, n_col, norm,
           k_hbm, c_hbm, a_hbm, b_hbm, UF, VF, cost_ref,
           K, KT, C, KCT, A, B, UB, VB, WP, DS, DR, SP, YR, TP, EI, XR, RX, ACC, CPS, CPR,
           k_sem, in_sem, r_sem,
           d_sem, y_sem, u_sem, uf_sem, e_sem, x_sem, v_sem, vf_sem, cp_sem):
    row = lax.axis_index("row")
    col = lax.axis_index("col")
    core = lax.rem(col, 2)
    n = K.shape[0]
    half = n // 2
    m = UB.shape[1]
    total_inst = SWEEPS * NB
    sib = {"col": col + 1 - 2 * core}
    ypeer = {"col": lax.rem(col + 2, n_col)}
    inner = jnp.logical_or(row == 1, row == 2)
    edge = jnp.logical_not(inner)
    zpair = {"row": row + 1 - 2 * lax.rem(row, 2)}
    zmid = {"row": n_row - 1 - row}
    own0 = pl.multiple_of(core * half, 128)
    sib0 = pl.multiple_of((1 - core) * half, 128)
    t_pieces = spans(T_PIECES)
    s_pieces = spans(S_PIECES)

    mode = {"chip": None, "full": False}

    def on_inner(fn):
        if mode["chip"] is None:
            pl.when(inner)(fn)
        elif mode["chip"] == "inner":
            fn()

    def on_edge(fn):
        if mode["chip"] is None:
            pl.when(edge)(fn)
        elif mode["chip"] == "edge":
            fn()

    def at(o, w):
        return pl.ds(pl.multiple_of(o, 128), w)

    def rcopy(src, dst, sem, dev):
        return pltpu.make_async_remote_copy(src_ref=src, dst_ref=dst, send_sem=sem.at[0], recv_sem=sem.at[1],
                                            device_id=dev, device_id_type=MESH)

    a_load = pltpu.make_async_copy(a_hbm, A, in_sem.at[0])
    b_load = pltpu.make_async_copy(b_hbm, B, in_sem.at[1])
    c_load = pltpu.make_async_copy(c_hbm, C, in_sem.at[2])
    k_loads = [pltpu.make_async_copy(k_hbm.at[o:o + w, :], K.at[o:o + w, :], k_sem.at[j])
               for j, (o, w) in enumerate(spans(K_PIECES))]
    for cp in k_loads:
        cp.start()
    a_load.start()

    barrier = pltpu.get_barrier_semaphore()
    rel = [(dr, dc) for dr in range(n_row) for dc in range(n_col) if (dr, dc) != (0, 0)]
    peers = [{"row": lax.rem(row + dr, n_row), "col": lax.rem(col + dc, n_col)} for dr, dc in rel]
    for dev in peers:
        pl.semaphore_signal(barrier, inc=1, device_id=dev, device_id_type=MESH)

    ACC[...] = jnp.zeros_like(ACC)

    def kt(t):
        rows = at(t * (n // 3), n // 3)

        def turn(q, carry):
            cols = at(q * 256, 256)
            KT[cols, rows] = jnp.transpose(K[rows, cols])
            return carry

        lax.fori_loop(0, n // 256, turn, 0)

    ones = jnp.ones((16, n), BF16)
    for cp, (o, w) in zip(k_loads, spans(K_PIECES)):
        cp.wait()
        RX[col, :, o:o + w] = dot_nt(ones, K[o:o + w, :])[:1]
    pl.semaphore_wait(barrier, len(peers))
    r_copies = [rcopy(RX.at[col], RX.at[col], r_sem.at[d - 1], {"col": lax.rem(col + d, n_col)}) for d in range(1, n_col)]
    for cp in r_copies:
        cp.start()
    b_load.start()
    c_load.start()
    a_load.wait()
    kt(0)
    for cp in r_copies:
        cp.wait()
    s0 = RX[0] + RX[1]
    for d in range(2, n_col):
        s0 = s0 + RX[d]
    for b in range(NB):
        UB[b] = (A[b] / s0).astype(BF16)
    b_load.wait()

    def u_copy(b, j):
        o, w = s_pieces[j]
        ref = UB.at[b, :, at(own0 + o, w)]
        return rcopy(ref, ref, u_sem.at[b, j], sib)

    def uf_copy(b):
        ref = UF.at[b, :, at(own0, half)]
        return rcopy(ref, ref, uf_sem.at[b], sib)

    def d_copy(b, j):
        o, w = s_pieces[j]
        return rcopy(DS.at[b, :, pl.ds(o, w)], DR.at[b, :, pl.ds(o, w)], d_sem.at[b, j], sib)

    def y_copy(par, b, j):
        o, w = s_pieces[j]
        return rcopy(SP.at[b, :, pl.ds(o, w)], YR.at[par, b, :, pl.ds(o, w)], y_sem.at[par, b, j], ypeer)

    def e_copy(b, c):
        o, w = t_pieces[c]
        return rcopy(TP.at[b, :, pl.ds(o, w)], EI.at[b, :, pl.ds(o, w)], e_sem.at[b, c], zpair)

    def x_copy(par, b, c):
        o, w = t_pieces[c]
        return rcopy(TP.at[b, :, pl.ds(o, w)], XR.at[par, b, :, pl.ds(o, w)], x_sem.at[par, b, c], zmid)

    def v_copy(b, c):
        o, w = t_pieces[c]
        ref = VB.at[b, :, pl.ds(o, w)]
        return rcopy(ref, ref, v_sem.at[b, c], zpair)

    def vf_copy(b, c):
        o, w = t_pieces[c]
        ref = VF.at[b, :, pl.ds(o, w)]
        return rcopy(ref, ref, vf_sem.at[b, c], zpair)

    early_spans = spans([sum(T_PIECES[c] for c in group) for group in EARLY])
    early = sum(w for _, w in early_spans)

    def s_drain(b, par):
        for j in range(len(s_pieces)):
            d_copy(b, j).wait_send()
            y_copy(par, b, j).wait_send()

    def t_drain(b, par):
        @on_inner
        def _():
            for c in range(len(t_pieces)):
                x_copy(par, b, c).wait_send()

        @on_edge
        def _():
            for c in range(len(t_pieces)):
                e_copy(b, c).wait_send()

    def sa(q, b, par, sweep):
        if q == 0:
            pl.when(sweep > 1)(lambda: s_drain(b, 1 - par))
        k0, kw = early_spans[q]
        for dst, h0 in ((DS, sib0), (SP, own0)):
            for o, w in tiles(half):
                part = dot_nn(VB[b, :, k0:k0 + kw], KT[k0:k0 + kw, at(h0 + o, w)])
                dst[b, :, o:o + w] = part if q == 0 else dst[b, :, o:o + w] + part

    def s1(b, par, sweep):
        for j, (o0, width) in enumerate(s_pieces):
            for o, w in tiles(width):
                o += o0
                DS[b, :, o:o + w] += dot_nn(VB[b, :, early:], KT[early:, at(sib0 + o, w)])
            d_copy(b, j).start()
        for o, w in tiles(half):
            SP[b, :, o:o + w] += dot_nn(VB[b, :, early:], KT[early:, at(own0 + o, w)])

    def v_drain(b):
        @on_inner
        def _():
            for c in range(len(t_pieces)):
                v_copy(b, c).wait_send()

    def s3(j, b, par, sweep):
        o, w = s_pieces[j]
        d_copy(b, j).wait_recv()
        SP[b, :, o:o + w] = SP[b, :, o:o + w] + DR[b, :, o:o + w]
        y_copy(par, b, j).start()
        if j == len(s_pieces) - 1:
            v_drain(b)

    def s4(j, b, par, sweep):
        o, w = s_pieces[j]
        y_copy(par, b, j).wait_recv()
        sl = at(own0 + o, w)
        u = A[b, :, sl] / (SP[b, :, o:o + w] + YR[par, b, :, o:o + w])
        UB[b, :, sl] = u.astype(BF16)
        u_copy(b, j).start()
        UF[b, :, sl] = u
        if j == len(s_pieces) - 1:
            pl.when(sweep == SWEEPS - 1)(lambda: uf_copy(b).start())

    def t0(b, par, sweep):
        for j in range(len(s_pieces)):
            u_copy(b, j).wait()

    def ta(q, b, par, sweep):
        if q == 0:
            pl.when(sweep > 0)(lambda: t_drain(b, 1 - par))
        o0, width = spans(TA_PIECES)[q]
        for o, w in tiles(width):
            o += o0
            TP[b, :, o:o + w] = dot_nn(UB[b, :, at(own0, half)], K[at(own0, half), o:o + w])

    def t1(b, par, sweep):
        def products(send):
            for c, (o0, width) in enumerate(t_pieces):
                for o, w in tiles(width):
                    o += o0
                    TP[b, :, o:o + w] += dot_nn(UB[b, :, at(sib0, half)], K[at(sib0, half), o:o + w])
                if send:
                    e_copy(b, c).start()

        on_edge(lambda: products(True))
        on_inner(lambda: products(False))

    def t2(c, b, par, sweep):
        o, w = t_pieces[c]

        @on_inner
        def _():
            e_copy(b, c).wait_recv()
            TP[b, :, o:o + w] = TP[b, :, o:o + w] + EI[b, :, o:o + w]
            x_copy(par, b, c).start()

    def t3i(c, b, par, sweep):
        o, w = t_pieces[c]

        @on_inner
        def _():
            x_copy(par, b, c).wait_recv()
            v = B[b, :, o:o + w] / (TP[b, :, o:o + w] + XR[par, b, :, o:o + w])
            VB[b, :, o:o + w] = v.astype(BF16)
            if mode["full"]:
                v_copy(b, c).start()
            else:
                VF[b, :, o:o + w] = v
                pl.when(sweep == SWEEPS - 1)(lambda: vf_copy(b, c).start())
                pl.when(sweep < SWEEPS - 1)(lambda: v_copy(b, c).start())

    def t3e(c, b, par, sweep):
        o, w = t_pieces[c]

        def last():
            vf_copy(b, c).wait_recv()
            VB[b, :, o:o + w] = VF[b, :, o:o + w].astype(BF16)

        @on_edge
        def _():
            if mode["full"]:
                v_copy(b, c).wait_recv()
            else:
                pl.when(sweep < SWEEPS - 1)(lambda: v_copy(b, c).wait_recv())
                pl.when(sweep == SWEEPS - 1)(last)

    def cost_early(b):
        for o, w in tiles(n):
            WP[:, o:o + w] = dot_nn(VB[b, :, :early], KCT[:early, o:o + w])

    def cost_part(b):
        s_drain(b, (SWEEPS - 1) % 2)
        t_drain(b, (SWEEPS - 1) % 2)
        uf_copy(b).wait()
        acc = jnp.zeros((m, 128), F32)
        for o, w in tiles(n):
            p = UF[b, :, o:o + w] * (WP[:, o:o + w] + dot_nn(VB[b, :, early:], KCT[early:, o:o + w]))
            for q in range(0, w, 128):
                acc = acc + p[:, q:q + 128]
        ACC[pl.ds(pl.multiple_of(b * m, m), m), :] = acc
        for c in range(len(t_pieces)):
            on_inner(lambda c=c: vf_copy(b, c).wait_send())

    def kc(t):
        rows = at(t * 128, 128)

        def turn(q, carry):
            cols = at(q * 256, 256)
            KCT[cols, rows] = KT[cols, rows] * jnp.transpose(C[rows, cols])
            return carry

        lax.fori_loop(0, n // 256, turn, 0)

    steps = {"sa": sa, "s1": s1, "s3": s3, "s4": s4, "ta": ta, "t0": t0, "t1": t1, "t2": t2, "t3": t3i, "e": t3e}

    def call(name, piece, g):
        fn = steps[name] if piece is None else functools.partial(steps[name], piece)
        sweep = lax.div(g, NB)
        fn(lax.rem(g, NB), lax.rem(sweep, 2), sweep)

    def tick(i, carry):
        for name, piece, lag in ORDER:
            g = i - lag
            if name in ("cost", "ca"):
                fn = cost_part if name == "cost" else cost_early
                pl.when(jnp.logical_and(g >= total_inst, g < total_inst + NB))(lambda: fn(g - total_inst))
            elif name == "kt":
                pl.when(i < 3)(lambda: kt(i))
            elif name != "kc":
                first = NB if name[0] == "s" or name == "t0" else 0
                pl.when(jnp.logical_and(g >= first, g < total_inst))(lambda: call(name, piece, g))
        return carry

    def full_tick(i):
        for name, piece, lag in ORDER:
            if name == "kc":
                kc(i - KC_FIRST)
            elif name not in ("cost", "ca", "kt"):
                call(name, piece, i - lag)

    full_end = KC_FIRST + n // 128
    lax.fori_loop(1, KC_FIRST, tick, 0)
    c_load.wait()
    for chip, cond in (("inner", inner), ("edge", edge)):
        @pl.when(cond)
        def _(chip=chip):
            def body(i, carry):
                mode.update(chip=chip, full=True)
                full_tick(i)
                mode.update(chip=None, full=False)
                return carry

            lax.fori_loop(KC_FIRST, full_end, body, 0)
    lax.fori_loop(full_end, total_inst + NB, tick, 0)

    tot = jnp.sum(jnp.transpose(ACC[...]), axis=0, keepdims=True)
    CPS[...] = jnp.broadcast_to(tot, CPS.shape)
    me = row * n_col + col
    cps = [rcopy(CPS, CPR.at[me], cp_sem.at[i], dev) for i, dev in enumerate(peers)]
    for cp in cps:
        cp.start()
    CPR[me] = CPS[...]
    for cp in cps:
        cp.wait()
    total = CPR[0]
    for i in range(1, n_row * n_col):
        total = total + CPR[i]
    cost_ref[...] = total[0:1, 0:cost_ref.shape[1]] / norm


def solution(mesh):
    n_row = mesh.shape["row"]
    n_col = mesh.shape["col"]

    def local_fn(kern, cost_mat, src_mass, tgt_mass):
        n = kern.shape[0]
        q = src_mass.shape[1]
        m = q // NB
        half = n // 2
        norm = float(n * n_row) * float(kern.shape[1] * n_col)
        dma = pltpu.SemaphoreType.DMA
        vmem = pltpu.VMEM
        any_spec = pl.BlockSpec(memory_space=pl.ANY)
        np_, ns = len(T_PIECES), len(S_PIECES)
        u, v, cost = pl.pallas_call(
            functools.partial(kernel, n_row, n_col, norm),
            out_shape=(vmem((NB, m, n), F32), vmem((NB, m, n), F32), vmem((1, q), F32)),
            in_specs=[any_spec] * 4,
            out_specs=(pl.BlockSpec(memory_space=vmem),) * 3,
            scratch_shapes=[
                vmem((n, n), BF16), vmem((n, n), BF16), vmem((n, n), BF16), vmem((n, n), BF16),
                vmem((NB, m, n), F32), vmem((NB, m, n), F32),
                vmem((NB, m, n), BF16), vmem((NB, m, n), BF16),
                vmem((m, n), F32),
                vmem((NB, m, half), F32), vmem((NB, m, half), F32),
                vmem((NB, m, half), F32), vmem((2, NB, m, half), F32),
                vmem((NB, m, n), F32), vmem((NB, m, n), F32),
                vmem((2, NB, m, n), F32),
                vmem((n_col, 1, n), F32),
                vmem((128, 128), F32), vmem((8, 128), F32), vmem((n_row * n_col, 8, 128), F32),
                dma((len(K_PIECES),)), dma((3,)), dma((n_col - 1, 2)),
                dma((NB, ns, 2)), dma((2, NB, ns, 2)), dma((NB, ns, 2)), dma((NB, 2)),
                dma((NB, np_, 2)), dma((2, NB, np_, 2)), dma((NB, np_, 2)), dma((NB, np_, 2)),
                dma((n_row * n_col - 1, 2)),
            ],
            compiler_params=pltpu.CompilerParams(collective_id=0, has_side_effects=True, vmem_limit_bytes=60 * 1024 * 1024),
        )(kern, cost_mat, src_mass.T.reshape(NB, m, n), tgt_mass.T.reshape(NB, m, n))
        return u.reshape(q, n).T, v.reshape(q, n).T, cost.reshape(q)

    return jax.shard_map(local_fn, mesh=mesh, in_specs=(P("row", "col"), P("row", "col"), P("row", "prob"), P("col", "prob")),
                         out_specs=(P("row", "prob"), P("col", "prob"), P("prob")), check_vma=False)
```

```python
import functools

import jax
import jax.numpy as jnp
from jax import lax
from jax.experimental import pallas as pl
from jax.experimental.pallas import tpu as pltpu
from jax.sharding import PartitionSpec as P

SWEEPS = 6
MESH = pl.DeviceIdType.MESH
F32 = jnp.float32
BF16 = jnp.bfloat16
NB = 4
T_PIECES = (512, 512, 512, 512, 256)
EARLY = ((0, 1, 2),)
TA_PIECES = (2304,)
S_PIECES = (512, 640)
K_PIECES = (256, 512, 768, 512, 256)
KC_FIRST = 5
ORDER = (
    ("e", 1, 4), ("e", 2, 4), ("sa", 0, 0), ("ca", None, 0), ("e", 3, 4), ("t3", 0, 3), ("s4", 0, 1),
    ("e", 4, 4), ("s1", None, 0), ("cost", None, 0), ("t3", 1, 3), ("s4", 1, 1), ("ta", 0, 1), ("s3", 0, 0),
    ("t2", 0, 2), ("s3", 1, 0), ("t3", 2, 3), ("t2", 1, 2), ("t0", None, 1), ("t1", None, 1), ("t3", 3, 3),
    ("t2", 2, 2), ("t3", 4, 3), ("e", 0, 3), ("kc", None, 0), ("t2", 3, 2), ("t2", 4, 2), ("kt", None, 0),
)


def dot_nn(x, y):
    return jnp.dot(x, y, preferred_element_type=F32)


def dot_nt(x, y):
    return lax.dot_general(x, y, (((1,), (1,)), ((), ())), preferred_element_type=F32)


def spans(sizes):
    out, o = [], 0
    for w in sizes:
        out.append((o, w))
        o += w
    return out


def tiles(size, tile=256):
    return [(o, min(tile, size - o)) for o in range(0, size, tile)]


def kernel(n_row, n_col, norm,
           k_hbm, c_hbm, a_hbm, b_hbm, UF, VF, cost_ref,
           K, KT, C, KCT, A, B, UB, VB, WP, DS, DR, SP, YR, TP, EI, XR, RX, ACC, CPS, CPR,
           k_sem, in_sem, r_sem,
           d_sem, y_sem, u_sem, uf_sem, e_sem, x_sem, v_sem, vf_sem, cp_sem):
    row = lax.axis_index("row")
    col = lax.axis_index("col")
    core = lax.rem(col, 2)
    n = K.shape[0]
    half = n // 2
    m = UB.shape[1]
    total_inst = SWEEPS * NB
    sib = {"col": col + 1 - 2 * core}
    ypeer = {"col": lax.rem(col + 2, n_col)}
    inner = jnp.logical_or(row == 1, row == 2)
    edge = jnp.logical_not(inner)
    zpair = {"row": row + 1 - 2 * lax.rem(row, 2)}
    zmid = {"row": n_row - 1 - row}
    own0 = pl.multiple_of(core * half, 128)
    sib0 = pl.multiple_of((1 - core) * half, 128)
    t_pieces = spans(T_PIECES)
    s_pieces = spans(S_PIECES)

    mode = {"chip": None, "full": False}

    def on_inner(fn):
        if mode["chip"] is None:
            pl.when(inner)(fn)
        elif mode["chip"] == "inner":
            fn()

    def on_edge(fn):
        if mode["chip"] is None:
            pl.when(edge)(fn)
        elif mode["chip"] == "edge":
            fn()

    def at(o, w):
        return pl.ds(pl.multiple_of(o, 128), w)

    def rcopy(src, dst, sem, dev):
        return pltpu.make_async_remote_copy(src_ref=src, dst_ref=dst, send_sem=sem.at[0], recv_sem=sem.at[1],
                                            device_id=dev, device_id_type=MESH)

    a_load = pltpu.make_async_copy(a_hbm, A, in_sem.at[0])
    b_load = pltpu.make_async_copy(b_hbm, B, in_sem.at[1])
    c_load = pltpu.make_async_copy(c_hbm, C, in_sem.at[2])
    k_loads = [pltpu.make_async_copy(k_hbm.at[o:o + w, :], K.at[o:o + w, :], k_sem.at[j])
               for j, (o, w) in enumerate(spans(K_PIECES))]
    for cp in k_loads:
        cp.start()
    a_load.start()

    barrier = pltpu.get_barrier_semaphore()
    rel = [(dr, dc) for dr in range(n_row) for dc in range(n_col) if (dr, dc) != (0, 0)]
    peers = [{"row": lax.rem(row + dr, n_row), "col": lax.rem(col + dc, n_col)} for dr, dc in rel]
    for dev in peers:
        pl.semaphore_signal(barrier, inc=1, device_id=dev, device_id_type=MESH)

    ACC[...] = jnp.zeros_like(ACC)

    def kt(t):
        rows = at(t * (n // 3), n // 3)

        def turn(q, carry):
            cols = at(q * 256, 256)
            KT[cols, rows] = jnp.transpose(K[rows, cols])
            return carry

        lax.fori_loop(0, n // 256, turn, 0)

    ones = jnp.ones((16, n), BF16)
    for cp, (o, w) in zip(k_loads, spans(K_PIECES)):
        cp.wait()
        RX[col, :, o:o + w] = dot_nt(ones, K[o:o + w, :])[:1]
    pl.semaphore_wait(barrier, len(peers))
    r_copies = [rcopy(RX.at[col], RX.at[col], r_sem.at[d - 1], {"col": lax.rem(col + d, n_col)}) for d in range(1, n_col)]
    for cp in r_copies:
        cp.start()
    b_load.start()
    c_load.start()
    a_load.wait()
    kt(0)
    for cp in r_copies:
        cp.wait()

    def first_u(b):
        s0 = RX[0] + RX[1]
        for d in range(2, n_col):
            s0 = s0 + RX[d]
        UB[b] = (A[b] / s0).astype(BF16)

    first_u(0)
    b_load.wait()

    def u_copy(b, j):
        o, w = s_pieces[j]
        ref = UB.at[b, :, at(own0 + o, w)]
        return rcopy(ref, ref, u_sem.at[b, j], sib)

    def uf_copy(b):
        ref = UF.at[b, :, at(own0, half)]
        return rcopy(ref, ref, uf_sem.at[b], sib)

    def d_copy(b, j):
        o, w = s_pieces[j]
        return rcopy(DS.at[b, :, pl.ds(o, w)], DR.at[b, :, pl.ds(o, w)], d_sem.at[b, j], sib)

    def y_copy(par, b, j):
        o, w = s_pieces[j]
        return rcopy(SP.at[b, :, pl.ds(o, w)], YR.at[par, b, :, pl.ds(o, w)], y_sem.at[par, b, j], ypeer)

    def e_copy(b, c):
        o, w = t_pieces[c]
        return rcopy(TP.at[b, :, pl.ds(o, w)], EI.at[b, :, pl.ds(o, w)], e_sem.at[b, c], zpair)

    def x_copy(par, b, c):
        o, w = t_pieces[c]
        return rcopy(TP.at[b, :, pl.ds(o, w)], XR.at[par, b, :, pl.ds(o, w)], x_sem.at[par, b, c], zmid)

    def v_copy(b, c):
        o, w = t_pieces[c]
        ref = VB.at[b, :, pl.ds(o, w)]
        return rcopy(ref, ref, v_sem.at[b, c], zpair)

    def vf_copy(b, c):
        o, w = t_pieces[c]
        ref = VF.at[b, :, pl.ds(o, w)]
        return rcopy(ref, ref, vf_sem.at[b, c], zpair)

    early_spans = spans([sum(T_PIECES[c] for c in group) for group in EARLY])
    early = sum(w for _, w in early_spans)

    def s_drain(b, par):
        for j in range(len(s_pieces)):
            d_copy(b, j).wait_send()
            y_copy(par, b, j).wait_send()

    def t_drain(b, par):
        @on_inner
        def _():
            for c in range(len(t_pieces)):
                x_copy(par, b, c).wait_send()

        @on_edge
        def _():
            for c in range(len(t_pieces)):
                e_copy(b, c).wait_send()

    def sa(q, b, par, sweep):
        if q == 0:
            pl.when(sweep > 1)(lambda: s_drain(b, 1 - par))
        k0, kw = early_spans[q]
        for dst, h0 in ((DS, sib0), (SP, own0)):
            for o, w in tiles(half):
                part = dot_nn(VB[b, :, k0:k0 + kw], KT[k0:k0 + kw, at(h0 + o, w)])
                dst[b, :, o:o + w] = part if q == 0 else dst[b, :, o:o + w] + part

    def s1(b, par, sweep):
        for j, (o0, width) in enumerate(s_pieces):
            for o, w in tiles(width):
                o += o0
                DS[b, :, o:o + w] += dot_nn(VB[b, :, early:], KT[early:, at(sib0 + o, w)])
            d_copy(b, j).start()
        for o, w in tiles(half):
            SP[b, :, o:o + w] += dot_nn(VB[b, :, early:], KT[early:, at(own0 + o, w)])

    def v_drain(b):
        @on_inner
        def _():
            for c in range(len(t_pieces)):
                v_copy(b, c).wait_send()

    def s3(j, b, par, sweep):
        o, w = s_pieces[j]
        d_copy(b, j).wait_recv()
        SP[b, :, o:o + w] = SP[b, :, o:o + w] + DR[b, :, o:o + w]
        y_copy(par, b, j).start()
        if j == len(s_pieces) - 1:
            v_drain(b)

    def s4(j, b, par, sweep):
        o, w = s_pieces[j]
        y_copy(par, b, j).wait_recv()
        sl = at(own0 + o, w)
        u = A[b, :, sl] / (SP[b, :, o:o + w] + YR[par, b, :, o:o + w])
        UB[b, :, sl] = u.astype(BF16)
        u_copy(b, j).start()
        UF[b, :, sl] = u
        if j == len(s_pieces) - 1:
            pl.when(sweep == SWEEPS - 1)(lambda: uf_copy(b).start())

    def t0(b, par, sweep):
        for j in range(len(s_pieces)):
            u_copy(b, j).wait()

    def ta(q, b, par, sweep):
        if q == 0:
            pl.when(sweep > 0)(lambda: t_drain(b, 1 - par))
        o0, width = spans(TA_PIECES)[q]
        for o, w in tiles(width):
            o += o0
            TP[b, :, o:o + w] = dot_nn(UB[b, :, at(own0, half)], K[at(own0, half), o:o + w])

    def t1(b, par, sweep):
        def products(send):
            for c, (o0, width) in enumerate(t_pieces):
                for o, w in tiles(width):
                    o += o0
                    TP[b, :, o:o + w] += dot_nn(UB[b, :, at(sib0, half)], K[at(sib0, half), o:o + w])
                if send:
                    e_copy(b, c).start()

        on_edge(lambda: products(True))
        on_inner(lambda: products(False))

    def t2(c, b, par, sweep):
        o, w = t_pieces[c]

        @on_inner
        def _():
            e_copy(b, c).wait_recv()
            TP[b, :, o:o + w] = TP[b, :, o:o + w] + EI[b, :, o:o + w]
            x_copy(par, b, c).start()

    def t3i(c, b, par, sweep):
        o, w = t_pieces[c]

        @on_inner
        def _():
            x_copy(par, b, c).wait_recv()
            v = B[b, :, o:o + w] / (TP[b, :, o:o + w] + XR[par, b, :, o:o + w])
            VB[b, :, o:o + w] = v.astype(BF16)
            if mode["full"]:
                v_copy(b, c).start()
            else:
                VF[b, :, o:o + w] = v
                pl.when(sweep == SWEEPS - 1)(lambda: vf_copy(b, c).start())
                pl.when(sweep < SWEEPS - 1)(lambda: v_copy(b, c).start())

    def t3e(c, b, par, sweep):
        o, w = t_pieces[c]

        def last():
            vf_copy(b, c).wait_recv()
            VB[b, :, o:o + w] = VF[b, :, o:o + w].astype(BF16)

        @on_edge
        def _():
            if mode["full"]:
                v_copy(b, c).wait_recv()
            else:
                pl.when(sweep < SWEEPS - 1)(lambda: v_copy(b, c).wait_recv())
                pl.when(sweep == SWEEPS - 1)(last)

    def cost_early(b):
        for o, w in tiles(n):
            WP[:, o:o + w] = dot_nn(VB[b, :, :early], KCT[:early, o:o + w])

    def cost_part(b):
        s_drain(b, (SWEEPS - 1) % 2)
        t_drain(b, (SWEEPS - 1) % 2)
        uf_copy(b).wait()
        acc = jnp.zeros((m, 128), F32)
        for o, w in tiles(n):
            p = UF[b, :, o:o + w] * (WP[:, o:o + w] + dot_nn(VB[b, :, early:], KCT[early:, o:o + w]))
            for q in range(0, w, 128):
                acc = acc + p[:, q:q + 128]
        ACC[pl.ds(pl.multiple_of(b * m, m), m), :] = acc
        for c in range(len(t_pieces)):
            on_inner(lambda c=c: vf_copy(b, c).wait_send())

    def kc(t):
        rows = at(t * 128, 128)

        def turn(q, carry):
            cols = at(q * 256, 256)
            KCT[cols, rows] = KT[cols, rows] * jnp.transpose(C[rows, cols])
            return carry

        lax.fori_loop(0, n // 256, turn, 0)

    steps = {"sa": sa, "s1": s1, "s3": s3, "s4": s4, "ta": ta, "t0": t0, "t1": t1, "t2": t2, "t3": t3i, "e": t3e}

    def call(name, piece, g):
        fn = steps[name] if piece is None else functools.partial(steps[name], piece)
        sweep = lax.div(g, NB)
        fn(lax.rem(g, NB), lax.rem(sweep, 2), sweep)

    def tick(i, carry):
        for name, piece, lag in ORDER:
            g = i - lag
            if name in ("cost", "ca"):
                fn = cost_part if name == "cost" else cost_early
                pl.when(jnp.logical_and(g >= total_inst, g < total_inst + NB))(lambda: fn(g - total_inst))
            elif name == "kt":
                pl.when(i < NB)(lambda: first_u(i))
                pl.when(i < 3)(lambda: kt(i))
            elif name != "kc":
                first = NB if name[0] == "s" or name == "t0" else 0
                pl.when(jnp.logical_and(g >= first, g < total_inst))(lambda: call(name, piece, g))
        return carry

    def full_tick(i):
        for name, piece, lag in ORDER:
            if name == "kc":
                kc(i - KC_FIRST)
            elif name not in ("cost", "ca", "kt"):
                call(name, piece, i - lag)

    full_end = KC_FIRST + n // 128
    lax.fori_loop(1, KC_FIRST, tick, 0)
    c_load.wait()
    for chip, cond in (("inner", inner), ("edge", edge)):
        @pl.when(cond)
        def _(chip=chip):
            def body(i, carry):
                mode.update(chip=chip, full=True)
                full_tick(i)
                mode.update(chip=None, full=False)
                return carry

            lax.fori_loop(KC_FIRST, full_end, body, 0)
    lax.fori_loop(full_end, total_inst + NB, tick, 0)

    tot = jnp.sum(jnp.transpose(ACC[...]), axis=0, keepdims=True)
    CPS[...] = jnp.broadcast_to(tot, CPS.shape)
    me = row * n_col + col
    cps = [rcopy(CPS, CPR.at[me], cp_sem.at[i], dev) for i, dev in enumerate(peers)]
    for cp in cps:
        cp.start()
    CPR[me] = CPS[...]
    for cp in cps:
        cp.wait()
    total = CPR[0]
    for i in range(1, n_row * n_col):
        total = total + CPR[i]
    cost_ref[...] = total[0:1, 0:cost_ref.shape[1]] / norm


def solution(mesh):
    n_row = mesh.shape["row"]
    n_col = mesh.shape["col"]

    def local_fn(kern, cost_mat, src_mass, tgt_mass):
        n = kern.shape[0]
        q = src_mass.shape[1]
        m = q // NB
        half = n // 2
        norm = float(n * n_row) * float(kern.shape[1] * n_col)
        dma = pltpu.SemaphoreType.DMA
        vmem = pltpu.VMEM
        any_spec = pl.BlockSpec(memory_space=pl.ANY)
        np_, ns = len(T_PIECES), len(S_PIECES)
        u, v, cost = pl.pallas_call(
            functools.partial(kernel, n_row, n_col, norm),
            out_shape=(vmem((NB, m, n), F32), vmem((NB, m, n), F32), vmem((1, q), F32)),
            in_specs=[any_spec] * 4,
            out_specs=(pl.BlockSpec(memory_space=vmem),) * 3,
            scratch_shapes=[
                vmem((n, n), BF16), vmem((n, n), BF16), vmem((n, n), BF16), vmem((n, n), BF16),
                vmem((NB, m, n), F32), vmem((NB, m, n), F32),
                vmem((NB, m, n), BF16), vmem((NB, m, n), BF16),
                vmem((m, n), F32),
                vmem((NB, m, half), F32), vmem((NB, m, half), F32),
                vmem((NB, m, half), F32), vmem((2, NB, m, half), F32),
                vmem((NB, m, n), F32), vmem((NB, m, n), F32),
                vmem((2, NB, m, n), F32),
                vmem((n_col, 1, n), F32),
                vmem((128, 128), F32), vmem((8, 128), F32), vmem((n_row * n_col, 8, 128), F32),
                dma((len(K_PIECES),)), dma((3,)), dma((n_col - 1, 2)),
                dma((NB, ns, 2)), dma((2, NB, ns, 2)), dma((NB, ns, 2)), dma((NB, 2)),
                dma((NB, np_, 2)), dma((2, NB, np_, 2)), dma((NB, np_, 2)), dma((NB, np_, 2)),
                dma((n_row * n_col - 1, 2)),
            ],
            compiler_params=pltpu.CompilerParams(collective_id=0, has_side_effects=True, vmem_limit_bytes=60 * 1024 * 1024),
        )(kern, cost_mat, src_mass.T.reshape(NB, m, n), tgt_mass.T.reshape(NB, m, n))
        return u.reshape(q, n).T, v.reshape(q, n).T, cost.reshape(q)

    return jax.shard_map(local_fn, mesh=mesh, in_specs=(P("row", "col"), P("row", "col"), P("row", "prob"), P("col", "prob")),
                         out_specs=(P("row", "prob"), P("col", "prob"), P("prob")), check_vma=False)
```

```python
import functools

import jax
import jax.numpy as jnp
from jax import lax
from jax.experimental import pallas as pl
from jax.experimental.pallas import tpu as pltpu
from jax.sharding import PartitionSpec as P

SWEEPS = 6
MESH = pl.DeviceIdType.MESH
F32 = jnp.float32
BF16 = jnp.bfloat16
NB = 4
T_PIECES = (512, 512, 512, 512, 256)
EARLY = ((0, 1, 2),)
TA_PIECES = (2304,)
S_PIECES = (512, 640)
K_PIECES = (256, 512, 768, 512, 256)
KC_FIRST = 5
ORDER = (
    ("e", 1, 4), ("e", 2, 4), ("sa", 0, 0), ("e", 3, 4), ("t3", 0, 3), ("s4", 0, 1),
    ("e", 4, 4), ("s1", None, 0), ("t3", 1, 3), ("s4", 1, 1), ("ta", 0, 1), ("s3", 0, 0),
    ("t2", 0, 2), ("s3", 1, 0), ("t3", 2, 3), ("t2", 1, 2), ("t0", None, 1), ("t1", None, 1), ("t3", 3, 3),
    ("t2", 2, 2), ("t3", 4, 3), ("e", 0, 3), ("kc", None, 0), ("t2", 3, 2), ("t2", 4, 2), ("ca", None, 0), ("cost", None, 0),
    ("kt", None, 0),
)


def dot_nn(x, y):
    return jnp.dot(x, y, preferred_element_type=F32)


def dot_nt(x, y):
    return lax.dot_general(x, y, (((1,), (1,)), ((), ())), preferred_element_type=F32)


def spans(sizes):
    out, o = [], 0
    for w in sizes:
        out.append((o, w))
        o += w
    return out


def tiles(size, tile=256):
    return [(o, min(tile, size - o)) for o in range(0, size, tile)]


def kernel(n_row, n_col, norm,
           k_hbm, c_hbm, a_hbm, b_hbm, UF, VF, cost_ref,
           K, KT, C, KCT, A, B, UB, VB, WP, DS, DR, SP, YR, TP, EI, XR, RX, ACC, CPS, CPR,
           k_sem, in_sem, r_sem,
           d_sem, y_sem, u_sem, uf_sem, e_sem, x_sem, v_sem, vf_sem, cp_sem):
    row = lax.axis_index("row")
    col = lax.axis_index("col")
    core = lax.rem(col, 2)
    n = K.shape[0]
    half = n // 2
    m = UB.shape[1]
    total_inst = SWEEPS * NB
    sib = {"col": col + 1 - 2 * core}
    ypeer = {"col": lax.rem(col + 2, n_col)}
    inner = jnp.logical_or(row == 1, row == 2)
    edge = jnp.logical_not(inner)
    zpair = {"row": row + 1 - 2 * lax.rem(row, 2)}
    zmid = {"row": n_row - 1 - row}
    own0 = pl.multiple_of(core * half, 128)
    sib0 = pl.multiple_of((1 - core) * half, 128)
    t_pieces = spans(T_PIECES)
    s_pieces = spans(S_PIECES)

    mode = {"chip": None, "full": False}

    def on_inner(fn):
        if mode["chip"] is None:
            pl.when(inner)(fn)
        elif mode["chip"] == "inner":
            fn()

    def on_edge(fn):
        if mode["chip"] is None:
            pl.when(edge)(fn)
        elif mode["chip"] == "edge":
            fn()

    def at(o, w):
        return pl.ds(pl.multiple_of(o, 128), w)

    def rcopy(src, dst, sem, dev):
        return pltpu.make_async_remote_copy(src_ref=src, dst_ref=dst, send_sem=sem.at[0], recv_sem=sem.at[1],
                                            device_id=dev, device_id_type=MESH)

    a_load = pltpu.make_async_copy(a_hbm, A, in_sem.at[0])
    b_load = pltpu.make_async_copy(b_hbm, B, in_sem.at[1])
    c_load = pltpu.make_async_copy(c_hbm, C, in_sem.at[2])
    k_loads = [pltpu.make_async_copy(k_hbm.at[o:o + w, :], K.at[o:o + w, :], k_sem.at[j])
               for j, (o, w) in enumerate(spans(K_PIECES))]
    for cp in k_loads:
        cp.start()
    a_load.start()

    barrier = pltpu.get_barrier_semaphore()
    rel = [(dr, dc) for dr in range(n_row) for dc in range(n_col) if (dr, dc) != (0, 0)]
    peers = [{"row": lax.rem(row + dr, n_row), "col": lax.rem(col + dc, n_col)} for dr, dc in rel]
    for dev in peers:
        pl.semaphore_signal(barrier, inc=1, device_id=dev, device_id_type=MESH)

    ACC[...] = jnp.zeros_like(ACC)

    def kt(t):
        rows = at(t * (n // 3), n // 3)

        def turn(q, carry):
            cols = at(q * 256, 256)
            KT[cols, rows] = jnp.transpose(K[rows, cols])
            return carry

        lax.fori_loop(0, n // 256, turn, 0)

    ones = jnp.ones((16, n), BF16)
    for cp, (o, w) in zip(k_loads, spans(K_PIECES)):
        cp.wait()
        RX[col, :, o:o + w] = dot_nt(ones, K[o:o + w, :])[:1]
    pl.semaphore_wait(barrier, len(peers))
    r_copies = [rcopy(RX.at[col], RX.at[col], r_sem.at[d - 1], {"col": lax.rem(col + d, n_col)}) for d in range(1, n_col)]
    for cp in r_copies:
        cp.start()
    b_load.start()
    c_load.start()
    a_load.wait()
    kt(0)
    for cp in r_copies:
        cp.wait()

    def first_u(b):
        s0 = RX[0] + RX[1]
        for d in range(2, n_col):
            s0 = s0 + RX[d]
        UB[b] = (A[b] / s0).astype(BF16)

    first_u(0)
    b_load.wait()

    def u_copy(b, j):
        o, w = s_pieces[j]
        ref = UB.at[b, :, at(own0 + o, w)]
        return rcopy(ref, ref, u_sem.at[b, j], sib)

    def uf_copy(b):
        ref = UF.at[b, :, at(own0, half)]
        return rcopy(ref, ref, uf_sem.at[b], sib)

    def d_copy(b, j):
        o, w = s_pieces[j]
        return rcopy(DS.at[b, :, pl.ds(o, w)], DR.at[b, :, pl.ds(o, w)], d_sem.at[b, j], sib)

    def y_copy(par, b, j):
        o, w = s_pieces[j]
        return rcopy(SP.at[b, :, pl.ds(o, w)], YR.at[par, b, :, pl.ds(o, w)], y_sem.at[par, b, j], ypeer)

    def e_copy(b, c):
        o, w = t_pieces[c]
        return rcopy(TP.at[b, :, pl.ds(o, w)], EI.at[b, :, pl.ds(o, w)], e_sem.at[b, c], zpair)

    def x_copy(par, b, c):
        o, w = t_pieces[c]
        return rcopy(TP.at[b, :, pl.ds(o, w)], XR.at[par, b, :, pl.ds(o, w)], x_sem.at[par, b, c], zmid)

    def v_copy(b, c):
        o, w = t_pieces[c]
        ref = VB.at[b, :, pl.ds(o, w)]
        return rcopy(ref, ref, v_sem.at[b, c], zpair)

    def vf_copy(b, c):
        o, w = t_pieces[c]
        ref = VF.at[b, :, pl.ds(o, w)]
        return rcopy(ref, ref, vf_sem.at[b, c], zpair)

    early_spans = spans([sum(T_PIECES[c] for c in group) for group in EARLY])
    early = sum(w for _, w in early_spans)

    def s_drain(b, par):
        for j in range(len(s_pieces)):
            d_copy(b, j).wait_send()
            y_copy(par, b, j).wait_send()

    def t_drain(b, par):
        @on_inner
        def _():
            for c in range(len(t_pieces)):
                x_copy(par, b, c).wait_send()

        @on_edge
        def _():
            for c in range(len(t_pieces)):
                e_copy(b, c).wait_send()

    def sa(q, b, par, sweep):
        if q == 0:
            pl.when(sweep > 1)(lambda: s_drain(b, 1 - par))
        k0, kw = early_spans[q]
        for dst, h0 in ((DS, sib0), (SP, own0)):
            for o, w in tiles(half):
                part = dot_nn(VB[b, :, k0:k0 + kw], KT[k0:k0 + kw, at(h0 + o, w)])
                dst[b, :, o:o + w] = part if q == 0 else dst[b, :, o:o + w] + part

    def s1(b, par, sweep):
        for j, (o0, width) in enumerate(s_pieces):
            for o, w in tiles(width):
                o += o0
                DS[b, :, o:o + w] += dot_nn(VB[b, :, early:], KT[early:, at(sib0 + o, w)])
            d_copy(b, j).start()
        for o, w in tiles(half):
            SP[b, :, o:o + w] += dot_nn(VB[b, :, early:], KT[early:, at(own0 + o, w)])

    def v_drain(b):
        @on_inner
        def _():
            for c in range(len(t_pieces)):
                v_copy(b, c).wait_send()

    def s3(j, b, par, sweep):
        o, w = s_pieces[j]
        d_copy(b, j).wait_recv()
        SP[b, :, o:o + w] = SP[b, :, o:o + w] + DR[b, :, o:o + w]
        y_copy(par, b, j).start()
        if j == len(s_pieces) - 1:
            v_drain(b)

    def s4(j, b, par, sweep):
        o, w = s_pieces[j]
        y_copy(par, b, j).wait_recv()
        sl = at(own0 + o, w)
        u = A[b, :, sl] / (SP[b, :, o:o + w] + YR[par, b, :, o:o + w])
        UB[b, :, sl] = u.astype(BF16)
        u_copy(b, j).start()
        UF[b, :, sl] = u
        if j == len(s_pieces) - 1:
            pl.when(sweep == SWEEPS - 1)(lambda: uf_copy(b).start())

    def t0(b, par, sweep):
        for j in range(len(s_pieces)):
            u_copy(b, j).wait()

    def ta(q, b, par, sweep):
        if q == 0:
            pl.when(sweep > 0)(lambda: t_drain(b, 1 - par))
        o0, width = spans(TA_PIECES)[q]
        for o, w in tiles(width):
            o += o0
            TP[b, :, o:o + w] = dot_nn(UB[b, :, at(own0, half)], K[at(own0, half), o:o + w])

    def t1(b, par, sweep):
        def products(send):
            for c, (o0, width) in enumerate(t_pieces):
                for o, w in tiles(width):
                    o += o0
                    TP[b, :, o:o + w] += dot_nn(UB[b, :, at(sib0, half)], K[at(sib0, half), o:o + w])
                if send:
                    e_copy(b, c).start()

        on_edge(lambda: products(True))
        on_inner(lambda: products(False))

    def t2(c, b, par, sweep):
        o, w = t_pieces[c]

        @on_inner
        def _():
            e_copy(b, c).wait_recv()
            TP[b, :, o:o + w] = TP[b, :, o:o + w] + EI[b, :, o:o + w]
            x_copy(par, b, c).start()

    def t3i(c, b, par, sweep):
        o, w = t_pieces[c]

        @on_inner
        def _():
            x_copy(par, b, c).wait_recv()
            v = B[b, :, o:o + w] / (TP[b, :, o:o + w] + XR[par, b, :, o:o + w])
            VB[b, :, o:o + w] = v.astype(BF16)
            if mode["full"]:
                v_copy(b, c).start()
            else:
                VF[b, :, o:o + w] = v
                pl.when(sweep == SWEEPS - 1)(lambda: vf_copy(b, c).start())
                pl.when(sweep < SWEEPS - 1)(lambda: v_copy(b, c).start())

    def t3e(c, b, par, sweep):
        o, w = t_pieces[c]

        def last():
            vf_copy(b, c).wait_recv()
            VB[b, :, o:o + w] = VF[b, :, o:o + w].astype(BF16)

        @on_edge
        def _():
            if mode["full"]:
                v_copy(b, c).wait_recv()
            else:
                pl.when(sweep < SWEEPS - 1)(lambda: v_copy(b, c).wait_recv())
                pl.when(sweep == SWEEPS - 1)(last)

    def cost_early(b):
        for o, w in tiles(n):
            WP[:, o:o + w] = dot_nn(VB[b, :, :early], KCT[:early, o:o + w])

    def cost_part(b):
        s_drain(b, (SWEEPS - 1) % 2)
        t_drain(b, (SWEEPS - 1) % 2)
        uf_copy(b).wait()
        acc = jnp.zeros((m, 128), F32)
        for o, w in tiles(n):
            p = UF[b, :, o:o + w] * (WP[:, o:o + w] + dot_nn(VB[b, :, early:], KCT[early:, o:o + w]))
            for q in range(0, w, 128):
                acc = acc + p[:, q:q + 128]
        ACC[pl.ds(pl.multiple_of(b * m, m), m), :] = acc
        for c in range(len(t_pieces)):
            on_inner(lambda c=c: vf_copy(b, c).wait_send())

    def kc(t):
        rows = at(t * 128, 128)

        def turn(q, carry):
            cols = at(q * 256, 256)
            KCT[cols, rows] = KT[cols, rows] * jnp.transpose(C[rows, cols])
            return carry

        lax.fori_loop(0, n // 256, turn, 0)

    steps = {"sa": sa, "s1": s1, "s3": s3, "s4": s4, "ta": ta, "t0": t0, "t1": t1, "t2": t2, "t3": t3i, "e": t3e}

    def call(name, piece, g):
        fn = steps[name] if piece is None else functools.partial(steps[name], piece)
        sweep = lax.div(g, NB)
        fn(lax.rem(g, NB), lax.rem(sweep, 2), sweep)

    def tick(i, carry):
        for name, piece, lag in ORDER:
            g = i - lag
            if name in ("cost", "ca"):
                fn = cost_part if name == "cost" else cost_early
                pl.when(jnp.logical_and(g >= total_inst, g < total_inst + NB))(lambda: fn(g - total_inst))
            elif name == "kt":
                pl.when(i < NB)(lambda: first_u(i))
                pl.when(i < 3)(lambda: kt(i))
            elif name != "kc":
                first = NB if name[0] == "s" or name == "t0" else 0
                pl.when(jnp.logical_and(g >= first, g < total_inst))(lambda: call(name, piece, g))
        return carry

    def full_tick(i):
        for name, piece, lag in ORDER:
            if name == "kc":
                kc(i - KC_FIRST)
            elif name not in ("cost", "ca", "kt"):
                call(name, piece, i - lag)

    full_end = KC_FIRST + n // 128
    lax.fori_loop(1, KC_FIRST, tick, 0)
    c_load.wait()
    for chip, cond in (("inner", inner), ("edge", edge)):
        @pl.when(cond)
        def _(chip=chip):
            def body(i, carry):
                mode.update(chip=chip, full=True)
                full_tick(i)
                mode.update(chip=None, full=False)
                return carry

            lax.fori_loop(KC_FIRST, full_end, body, 0)
    lax.fori_loop(full_end, total_inst + NB, tick, 0)

    tot = jnp.sum(jnp.transpose(ACC[...]), axis=0, keepdims=True)
    CPS[...] = jnp.broadcast_to(tot, CPS.shape)
    me = row * n_col + col
    cps = [rcopy(CPS, CPR.at[me], cp_sem.at[i], dev) for i, dev in enumerate(peers)]
    for cp in cps:
        cp.start()
    CPR[me] = CPS[...]
    for cp in cps:
        cp.wait()
    total = CPR[0]
    for i in range(1, n_row * n_col):
        total = total + CPR[i]
    cost_ref[...] = total[0:1, 0:cost_ref.shape[1]] / norm


def solution(mesh):
    n_row = mesh.shape["row"]
    n_col = mesh.shape["col"]

    def local_fn(kern, cost_mat, src_mass, tgt_mass):
        n = kern.shape[0]
        q = src_mass.shape[1]
        m = q // NB
        half = n // 2
        norm = float(n * n_row) * float(kern.shape[1] * n_col)
        dma = pltpu.SemaphoreType.DMA
        vmem = pltpu.VMEM
        any_spec = pl.BlockSpec(memory_space=pl.ANY)
        np_, ns = len(T_PIECES), len(S_PIECES)
        u, v, cost = pl.pallas_call(
            functools.partial(kernel, n_row, n_col, norm),
            out_shape=(vmem((NB, m, n), F32), vmem((NB, m, n), F32), vmem((1, q), F32)),
            in_specs=[any_spec] * 4,
            out_specs=(pl.BlockSpec(memory_space=vmem),) * 3,
            scratch_shapes=[
                vmem((n, n), BF16), vmem((n, n), BF16), vmem((n, n), BF16), vmem((n, n), BF16),
                vmem((NB, m, n), F32), vmem((NB, m, n), F32),
                vmem((NB, m, n), BF16), vmem((NB, m, n), BF16),
                vmem((m, n), F32),
                vmem((NB, m, half), F32), vmem((NB, m, half), F32),
                vmem((NB, m, half), F32), vmem((2, NB, m, half), F32),
                vmem((NB, m, n), F32), vmem((NB, m, n), F32),
                vmem((2, NB, m, n), F32),
                vmem((n_col, 1, n), F32),
                vmem((128, 128), F32), vmem((8, 128), F32), vmem((n_row * n_col, 8, 128), F32),
                dma((len(K_PIECES),)), dma((3,)), dma((n_col - 1, 2)),
                dma((NB, ns, 2)), dma((2, NB, ns, 2)), dma((NB, ns, 2)), dma((NB, 2)),
                dma((NB, np_, 2)), dma((2, NB, np_, 2)), dma((NB, np_, 2)), dma((NB, np_, 2)),
                dma((n_row * n_col - 1, 2)),
            ],
            compiler_params=pltpu.CompilerParams(collective_id=0, has_side_effects=True, vmem_limit_bytes=60 * 1024 * 1024),
        )(kern, cost_mat, src_mass.T.reshape(NB, m, n), tgt_mass.T.reshape(NB, m, n))
        return u.reshape(q, n).T, v.reshape(q, n).T, cost.reshape(q)

    return jax.shard_map(local_fn, mesh=mesh, in_specs=(P("row", "col"), P("row", "col"), P("row", "prob"), P("col", "prob")),
                         out_specs=(P("row", "prob"), P("col", "prob"), P("prob")), check_vma=False)
```
